128 devices in a mesh: seq: 16 (over y_lo, z, core), mp: 8 (over y_hi, x).
Axes of the slice: x: 4, y: 4 (y_hi: 2, y_lo: 2; y = y_hi * 2 + y_lo), z: 4, core: 2. Of those that a mesh axis runs over, the one named last changes fastest.
Arguments:
- hidden_in: bfloat16 [8192, 4096], P('seq', 'mp'), may hold values from -30 to 30
- norm_gain: float32 [4096], replicated, may hold values from 0.1 to 1.9
- w_z: bfloat16 [4096, 8192], P('seq', 'mp'), may hold values from -0.09375 to 0.09375
- w_x: bfloat16 [4096, 8192], P('seq', 'mp'), may hold values from -0.09375 to 0.09375
- w_b: bfloat16 [4096, 1024], P('seq', 'mp'), may hold values from -0.09375 to 0.09375
- w_c: bfloat16 [4096, 1024], P('seq', 'mp'), may hold values from -0.09375 to 0.09375
- w_dt: bfloat16 [4096, 128], P('seq', 'mp'), may hold values from -0.0625 to 0.0625
- conv_x: float32 [4, 8192], P(None, 'mp'), may hold values from -3 to 3
- conv_b: float32 [4, 1024], P(None, 'mp'), may hold values from -3 to 3
- conv_c: float32 [4, 1024], P(None, 'mp'), may hold values from -3 to 3
- dt_bias: float32 [128], P('mp'), may hold values from -9 to -5
- a_rate: float32 [128], P('mp'), may hold values from 0.5 to 16
- skip_gain: float32 [128], P('mp'), may hold values from -3 to 3
- group_gain: float32 [8192], P('mp'), may hold values from 0.1 to 1.9
- w_out: bfloat16 [8192, 4096], P('mp', 'seq'), may hold values from -0.0625 to 0.0625
- attn_gain: float32 [4096], replicated, may hold values from 0.1 to 1.9
- w_q: bfloat16 [4096, 4096], P(None, 'mp'), may hold values from -0.125 to 0.125
- w_k: bfloat16 [4096, 1024], P(None, 'mp'), may hold values from -0.125 to 0.125
- w_v: bfloat16 [4096, 1024], P(None, 'mp'), may hold values from -0.09375 to 0.09375
Outputs:
- mixed: float32 [8192, 4096], P('seq', 'mp')
- context: float32 [8192, 4096], P('seq', 'mp')
The draws below stay inside these ranges and needn't reach their ends.
All inputs are finite; a program needn't handle non-finite values.
Results may differ from the reference program's by a relative error of at most 0.017.
Values may be sent and summed in bfloat16 or wider, within the bound.
A program may use at most 128 MiB of HBM per device.

```python
import math
import jax
import jax.numpy as jnp
from jax import lax

D = 4096
DI = 8192
H = 128
P_SIZE = 64
N = 128
G = 8
KW = 4
HQ = 32
HK = 8
HD = 128
WINDOW = 4096
QB = 128
TOK_DEV = 512
TOKENS = 8192
N_SEQ = 16
N_MP = 8


def contiguous_spans(key):
    forward_sense = jnp.clip(jax.random.normal(jax.random.fold_in(key, 101), (D,), jnp.float32), -4.0, 4.0)
    processor_slots = jax.random.randint(jax.random.fold_in(key, 102), (TOKENS // TOK_DEV * 2,), 0, TOKENS)
    input_magnitude = jax.random.uniform(jax.random.fold_in(key, 103), (TOKENS // TOK_DEV * 2,), jnp.float32, 0.6, 1.0)
    return (forward_sense, processor_slots, input_magnitude)


def draw_hidden_in(key, part):
    forward_sense, processor_slots, input_magnitude = contiguous_spans(key)
    base = jnp.clip(jax.random.normal(jax.random.fold_in(key, 1), (TOKENS, D), jnp.float32), -6.0, 6.0)
    mixing = jnp.zeros((TOKENS,), jnp.float32).at[processor_slots].set(input_magnitude)
    values = base * (1.0 - mixing)[:, None] + forward_sense[None, :] * (4.0 * mixing)[:, None]
    return jnp.clip(values, -30.0, 30.0).astype(jnp.bfloat16)


def draw_w_dt(key, part):
    forward_sense, processor_slots, input_magnitude = contiguous_spans(key)
    noise = 0.3 * jnp.clip(jax.random.normal(jax.random.fold_in(key, 3), (D, H), jnp.float32), -6.0, 6.0) / math.sqrt(D)
    lifted = jax.random.uniform(jax.random.fold_in(key, 4), (H,), jnp.float32, 6.0, 10.0)
    limit = 4.0 / math.sqrt(D)
    return jnp.clip(noise + forward_sense[:, None] * lifted[None, :] / D, -limit, limit).astype(jnp.bfloat16)


def draw_w_q(key, part):
    base = jnp.clip(jax.random.normal(jax.random.fold_in(key, 5), (D, HQ * HD), jnp.float32), -6.0, 6.0) / math.sqrt(D)
    limit = 8.0 / math.sqrt(D)
    return jnp.clip(base, -limit, limit).astype(jnp.bfloat16)


def draw_w_k(key, part):
    base = jnp.clip(jax.random.normal(jax.random.fold_in(key, 6), (D, HK * HD), jnp.float32), -6.0, 6.0) / math.sqrt(D)
    limit = 8.0 / math.sqrt(D)
    return jnp.clip(base, -limit, limit).astype(jnp.bfloat16)


def block_levels(own_key, dims, split, smallest, largest):
    factor_of, own = 1.0, jax.random.fold_in(own_key, 6)
    for position, blocks in split:
        draws = jnp.exp(jax.random.uniform(jax.random.fold_in(own, position), (blocks,), jnp.float32, smallest / len(split), largest / len(split)))
        factor_of = factor_of * jnp.repeat(draws, dims[position] // blocks).reshape([-1 if axis == position else 1 for axis in range(len(dims))])
    return factor_of


def scatter_about(own_key, dims, scale, bound, split=(), kind=jnp.bfloat16):
    result = scale * jax.random.normal(own_key, dims, jnp.float32)
    if split:
        result = result * block_levels(own_key, dims, split, -0.22, 0.18)
    return jnp.clip(result, -bound, bound).astype(kind)


def setup_inputs(seed: int = 0) -> dict:
    key_list = jax.random.split(jax.random.key(seed), 20)
    return {
        "hidden_in": draw_hidden_in(jax.random.fold_in(key_list[19], 71), 0),
        "norm_gain": jnp.clip(1.0 + 0.18 * jax.random.normal(key_list[1], (D,), jnp.float32), 0.1, 1.9),
        "w_z": scatter_about(key_list[2], (D, DI), D ** -0.5, 0.09375, ((0, 16), (1, 8))),
        "w_x": scatter_about(key_list[3], (D, DI), D ** -0.5, 0.09375, ((0, 16), (1, 8))),
        "w_b": scatter_about(key_list[4], (D, G * N), D ** -0.5, 0.09375, ((0, 16), (1, 8))),
        "w_c": scatter_about(key_list[5], (D, G * N), D ** -0.5, 0.09375, ((0, 16), (1, 8))),
        "w_dt": draw_w_dt(jax.random.fold_in(key_list[19], 71), 0),
        "conv_x": scatter_about(key_list[7], (KW, DI), 0.5, 3.0, ((1, 8),), jnp.float32),
        "conv_b": scatter_about(key_list[8], (KW, G * N), 0.5, 3.0, ((1, 8),), jnp.float32),
        "conv_c": scatter_about(key_list[9], (KW, G * N), 0.5, 3.0, ((1, 8),), jnp.float32),
        "dt_bias": jnp.clip(-9.0 + 4.0 * jax.random.uniform(key_list[10], (H,), jnp.float32) ** block_levels(key_list[10], (H,), ((0, 8),), -0.2, 0.2), -9.0, -5.0),
        "a_rate": jnp.clip(jnp.exp(math.log(16.0) - 3.465736 * jax.random.uniform(key_list[11], (H,), jnp.float32) ** block_levels(key_list[11], (H,), ((0, 8),), -0.2, 0.2)), 0.5, 16.0),
        "skip_gain": scatter_about(key_list[12], (H,), 1.0, 3.0, ((0, 8),), jnp.float32),
        "group_gain": jnp.clip(1.0 + 0.18 * jax.random.normal(key_list[13], (DI,), jnp.float32), 0.1, 1.9),
        "w_out": scatter_about(key_list[14], (DI, D), DI ** -0.5, 0.0625, ((0, 8), (1, 16))),
        "attn_gain": jnp.clip(1.0 + 0.18 * jax.random.normal(key_list[15], (D,), jnp.float32), 0.1, 1.9),
        "w_q": draw_w_q(jax.random.fold_in(key_list[19], 71), 0),
        "w_k": draw_w_k(jax.random.fold_in(key_list[19], 71), 0),
        "w_v": scatter_about(key_list[18], (D, HK * HD), D ** -0.5, 0.09375, ((1, 8),)),
    }


HIGH = lax.Precision.HIGHEST

def rms_norm(values, gain):
    return values * lax.rsqrt(lax.optimization_barrier(jnp.mean(values * values, axis=-1, keepdims=True)) + 1e-05) * gain

def causal_conv(values, rim, device_routine):
    padded = jnp.concatenate([rim, values], axis=0)
    length = values.shape[0]
    summed = jnp.zeros(values.shape, jnp.float32)
    for offset in range(device_routine.shape[0]):
        summed = summed + device_routine[offset][None, :] * padded[offset:offset + length]
    return jax.nn.silu(summed)

def ssd_block(carry_state, pieces):
    inputs, step_sizes, decays, keys_b, reads_c = pieces
    per_group = inputs.shape[1] // keys_b.shape[1]
    b_heads = jnp.repeat(keys_b, per_group, axis=1)
    c_heads = jnp.repeat(reads_c, per_group, axis=1)
    cumulative = jnp.cumsum(decays, axis=0)
    length = inputs.shape[0]
    causal_mask = jnp.arange(length)[:, None] >= jnp.arange(length)[None, :]
    spread = cumulative[:, None, :] - cumulative[None, :, :]
    within = jnp.exp(jnp.where(causal_mask[:, :, None], spread, -jnp.inf))
    affinity = jnp.einsum('tgn,sgn->gts', reads_c, keys_b, precision=HIGH)
    affinity = jnp.repeat(affinity, per_group, axis=0)
    mixing = affinity * jnp.transpose(within, (2, 0, 1)) * jnp.transpose(step_sizes)[:, None, :]
    inside = jnp.einsum('hts,shp->thp', mixing, inputs, precision=HIGH)
    carried = jnp.exp(cumulative)[:, :, None] * jnp.einsum('thn,hpn->thp', c_heads, carry_state, precision=HIGH)
    tail_weight = jnp.exp(cumulative[-1][None, :] - cumulative) * step_sizes
    fresh_state = jnp.einsum('sh,shp,shn->hpn', tail_weight, inputs, b_heads, precision=HIGH)
    updated = jnp.exp(cumulative[-1])[:, None, None] * carry_state + fresh_state
    return (updated, inside + carried)

def run_ssd(inputs, step_sizes, decays, keys_b, reads_c, block, carry_state):
    total_rows = inputs.shape[0]
    block_count = total_rows // block

    def blocked(values):
        return values.reshape((block_count, block) + values.shape[1:])
    final_state, outputs = lax.scan(ssd_block, carry_state, (blocked(inputs), blocked(step_sizes), blocked(decays), blocked(keys_b), blocked(reads_c)))
    return (final_state, outputs.reshape((total_rows,) + outputs.shape[2:]))

def window_attention(asking_vectors, keys, values, shift_rows, first_key):
    per_kv = asking_vectors.shape[1] // keys.shape[1]
    keys_all = jnp.repeat(keys, per_kv, axis=1)
    values_all = jnp.repeat(values, per_kv, axis=1)
    query_rows = asking_vectors.shape[0]
    key_count = keys.shape[0]
    scale = asking_vectors.shape[2] ** (-0.5)
    index_offsets = jnp.arange(key_count)[None, :] - shift_rows - jnp.arange(query_rows)[:, None]
    allowed = (index_offsets <= 0) & (index_offsets > -WINDOW) & (first_key + jnp.arange(key_count) >= 0)[None, :]

    def one_head(operands):
        query_h, key_h, value_h = operands
        scores = lax.dot_general(query_h, key_h, (((1,), (1,)), ((), ())), preferred_element_type=jnp.float32) * scale
        scores = jnp.where(allowed, scores, -jnp.inf)
        row_peak = lax.optimization_barrier(jnp.max(scores, axis=1, keepdims=True))
        exp_scores = jnp.exp(scores - row_peak)
        weights = (exp_scores / lax.optimization_barrier(jnp.sum(exp_scores, axis=1, keepdims=True))).astype(jnp.bfloat16)
        return jnp.dot(weights, value_h, preferred_element_type=jnp.float32)
    outputs = lax.map(one_head, (jnp.transpose(asking_vectors, (1, 0, 2)), jnp.transpose(keys_all, (1, 0, 2)), jnp.transpose(values_all, (1, 0, 2))))
    return jnp.transpose(outputs, (1, 0, 2)).reshape(query_rows, -1)

def reference(hidden_in, norm_gain, w_z, w_x, w_b, w_c, w_dt, conv_x, conv_b, conv_c, dt_bias, a_rate, skip_gain, group_gain, w_out, attn_gain, w_q, w_k, w_v):
    stream = hidden_in.astype(jnp.float32)
    normed = rms_norm(stream, norm_gain).astype(jnp.bfloat16)
    gate_proj = jnp.dot(normed, w_z, preferred_element_type=jnp.float32)
    input_mapped = jnp.dot(normed, w_x, preferred_element_type=jnp.float32)
    b_proj = jnp.dot(normed, w_b, preferred_element_type=jnp.float32)
    c_proj = jnp.dot(normed, w_c, preferred_element_type=jnp.float32)
    delta_time_unscaled = jnp.dot(normed, w_dt, preferred_element_type=jnp.float32)
    conv_in = causal_conv(input_mapped, jnp.zeros((KW - 1, DI), jnp.float32), conv_x)
    conv_bv = causal_conv(b_proj, jnp.zeros((KW - 1, G * N), jnp.float32), conv_b)
    conv_cv = causal_conv(c_proj, jnp.zeros((KW - 1, G * N), jnp.float32), conv_c)
    step_sizes = jax.nn.softplus(delta_time_unscaled + dt_bias[None, :])
    decays = -a_rate[None, :] * step_sizes
    inputs = conv_in.reshape(TOKENS, H, P_SIZE)
    final_state, ssd_out = run_ssd(inputs, step_sizes, decays, conv_bv.reshape(TOKENS, G, N), conv_cv.reshape(TOKENS, G, N), QB, jnp.zeros((H, P_SIZE, N), jnp.float32))
    full = ssd_out + skip_gain[None, :, None] * inputs
    gated = full.reshape(TOKENS, DI) * jax.nn.silu(gate_proj)
    grouped = gated.reshape(TOKENS, G, DI // G)
    y_normed = rms_norm(grouped, group_gain.reshape(G, DI // G)).reshape(TOKENS, DI).astype(jnp.bfloat16)
    width = DI // N_MP
    summed = jnp.zeros((TOKENS, D), jnp.float32)
    for member in range(N_MP):
        term = jnp.dot(y_normed[:, member * width:(member + 1) * width], w_out[member * width:(member + 1) * width], preferred_element_type=jnp.float32)
        summed = summed + lax.optimization_barrier(term.astype(jnp.bfloat16)).astype(jnp.float32)
    mixed = stream + summed
    mixed_low = lax.optimization_barrier(mixed.astype(jnp.bfloat16)).astype(jnp.float32)
    normed_two = rms_norm(mixed_low, attn_gain).astype(jnp.bfloat16)
    asking_vectors = jnp.dot(normed_two, w_q, preferred_element_type=jnp.float32).astype(jnp.bfloat16).reshape(TOKENS, HQ, HD)
    keys = jnp.dot(normed_two, w_k, preferred_element_type=jnp.float32).astype(jnp.bfloat16).reshape(TOKENS, HK, HD)
    values = jnp.dot(normed_two, w_v, preferred_element_type=jnp.float32).astype(jnp.bfloat16).reshape(TOKENS, HK, HD)
    keys_pad = jnp.concatenate([jnp.zeros((WINDOW, HK, HD), jnp.bfloat16), keys], axis=0)
    values_pad = jnp.concatenate([jnp.zeros((WINDOW, HK, HD), jnp.bfloat16), values], axis=0)

    def one_block(block_index):
        start = (block_index * TOK_DEV).astype(jnp.int32)
        asking_tile = lax.dynamic_slice_in_dim(asking_vectors, start, TOK_DEV, 0)
        key_blk = lax.dynamic_slice_in_dim(keys_pad, start, WINDOW + TOK_DEV, 0)
        value_blk = lax.dynamic_slice_in_dim(values_pad, start, WINDOW + TOK_DEV, 0)
        return window_attention(asking_tile, key_blk, value_blk, WINDOW, start - WINDOW)
    blocks = lax.map(one_block, jnp.arange(N_SEQ, dtype=jnp.int32))
    context = blocks.reshape(TOKENS, HQ * HD)
    return (mixed, context)
```

```python
import functools
import jax
import jax.numpy as jnp
from jax import lax
from jax.experimental import pallas as pl
from jax.experimental.pallas import tpu as pltpu
from jax.sharding import PartitionSpec as P

MESH = pl.DeviceIdType.MESH
P_SIZE = 64
N = 128
HD = 128
WINDOW = 4096
QB = 128
VM = pl.BlockSpec(memory_space=pltpu.VMEM)


def rows(start, size):
    return pl.ds(start, size)


def mp_places():
    me = lax.axis_index("mp")
    high, low = me // 4, me % 4
    return high, low


def mp_greet(others):
    barrier = pltpu.get_barrier_semaphore()
    for other in others:
        pl.semaphore_signal(barrier, inc=1, device_id={"mp": other}, device_id_type=MESH)
    pl.semaphore_wait(barrier, len(others))


def gather_kernel(chunks, x_ref, gain_ref, normed_ref, out_ref, own_sem, ysend, yrecv, xsend, xrecv, fsend, frecv):
    high, low = mp_places()
    right, left = (low + 1) % 4, (low + 3) % 4
    me, partner = high * 4 + low, (1 - high) * 4 + low
    mp_greet((high * 4 + right, high * 4 + left, partner))
    count = x_ref.shape[0] // chunks
    half = x_ref.shape[0] // 2

    def send(src, block, piece, target, ssem, rsem):
        copy = pltpu.make_async_remote_copy(
            src_ref=src, dst_ref=out_ref.at[block, piece], send_sem=ssem, recv_sem=rsem,
            device_id={"mp": target}, device_id_type=MESH)
        copy.start()
        return copy

    sides = ((right, left), (left, right))
    started = []
    ycopies, own = [], []
    for c in range(chunks):
        piece = rows(c * count, count)
        ycopies.append(send(x_ref.at[piece], me, piece, partner, ysend.at[c], yrecv.at[c]))
        own.append([
            send(x_ref.at[piece], me, piece, high * 4 + to, xsend.at[0, d, c], xrecv.at[0, d, c])
            for d, (to, _) in enumerate(sides)])
    local = pltpu.make_async_copy(x_ref, out_ref.at[me], own_sem)
    local.start()
    other = []
    for c in range(chunks):
        piece = rows(c * count, count)
        ycopies[c].wait_recv()
        other.append([
            send(out_ref.at[partner, piece], partner, piece, high * 4 + to, xsend.at[1, d, c], xrecv.at[1, d, c])
            for d, (to, _) in enumerate(sides)])
    forwards = []
    for k, copies in enumerate((own, other)):
        for c in range(chunks):
            for d, (to, origin) in enumerate(sides):
                copies[c][d].wait_recv()
                if (c * count < half) == (d == 0):
                    block = (high if k == 0 else 1 - high) * 4 + origin
                    piece = rows(c * count, count)
                    forwards.append(send(out_ref.at[block, piece], block, piece, high * 4 + to,
                                         fsend.at[k, c], frecv.at[k, c]))
    for copy in forwards:
        copy.wait()
    local.wait()
    for c in range(chunks):
        ycopies[c].wait_send()
        for copies in (own, other):
            for d in range(2):
                copies[c][d].wait_send()
    wide = x_ref.shape[1]

    def norm(c, _):
        piece = rows(pl.multiple_of(c * 32, 32), 32)
        square = jnp.zeros((32, wide), jnp.float32)
        for b in range(8):
            value = out_ref[b, piece, :].astype(jnp.float32)
            square = square + value * value
        scale = lax.rsqrt(jnp.sum(square, axis=1, keepdims=True) / (8 * wide) + 1e-05)
        for b in range(8):
            lanes = slice(b * wide, (b + 1) * wide)
            normed_ref[piece, lanes] = (out_ref[b, piece, :].astype(jnp.float32) * scale
                                        * gain_ref[:, lanes]).astype(normed_ref.dtype)
        return 0

    lax.fori_loop(0, x_ref.shape[0] // 32, norm, 0)


def mp_gather_norm(x, gain, cid, chunks=4):
    n, w = x.shape
    D = pltpu.SemaphoreType.DMA
    return pl.pallas_call(
        functools.partial(gather_kernel, chunks),
        out_shape=jax.ShapeDtypeStruct((n, 8 * w), x.dtype),
        in_specs=[VM, VM], out_specs=VM,
        scratch_shapes=[pltpu.VMEM((8, n, w), x.dtype), D, D((chunks,)), D((chunks,)), D((2, 2, chunks)), D((2, 2, chunks)), D((2, chunks)), D((2, chunks))],
        compiler_params=pltpu.CompilerParams(collective_id=cid, has_side_effects=True, vmem_limit_bytes=24 << 20),
    )(x, gain)


def reduce_kernel(p_ref, out_ref, tmp, d1, d2, ysrc, ydst, s1, r1, s2, r2, sy, ry, sraw, rraw):
    high, low = mp_places()
    right, left = (low + 1) % 4, (low + 3) % 4
    far = (low + 2) % 4
    partner = (1 - high) * 4 + low
    mp_greet((high * 4 + right, high * 4 + left, partner))
    n = p_ref.shape[1]
    half = n // 2
    order = (1 - high, high)
    sides = ((right, left), (left, right))

    def send(src, dst, target, ssem, rsem):
        copy = pltpu.make_async_remote_copy(src_ref=src, dst_ref=dst, send_sem=ssem, recv_sem=rsem,
                                            device_id={"mp": target}, device_id_type=MESH)
        copy.start()
        return copy

    first = [[send(p_ref.at[order[k] * 4 + far, rows(d * half, half)], d1.at[k, d], high * 4 + sides[d][0],
                   s1.at[k, d], r1.at[k, d]) for d in range(2)] for k in range(2)]
    raw = [[send(p_ref.at[order[k] * 4 + sides[d][0], rows((1 - d) * half, half)],
                 d2.at[k, d, rows((1 - d) * half, half)], high * 4 + sides[d][0],
                 sraw.at[k, d], rraw.at[k, d]) for d in range(2)] for k in range(2)]
    second = []
    for k in range(2):
        for d in range(2):
            first[k][d].wait_recv()
            tmp[k, d] = (d1[k, d].astype(jnp.float32)
                         + p_ref[order[k] * 4 + sides[d][0], d * half:(d + 1) * half].astype(jnp.float32)).astype(tmp.dtype)
            second.append(send(tmp.at[k, d], d2.at[k, d, rows(d * half, half)], high * 4 + sides[d][0],
                               s2.at[k, d], r2.at[k, d]))
    totals = None
    for k in range(2):
        for d in range(2):
            raw[k][d].wait_recv()
            second[k * 2 + d].wait_recv()
        total = (p_ref[order[k] * 4 + low].astype(jnp.float32) + d2[k, 0].astype(jnp.float32)
                 + d2[k, 1].astype(jnp.float32))
        if k == 0:
            ysrc[...] = total.astype(ysrc.dtype)
            ycopy = send(ysrc, ydst, partner, sy, ry)
        else:
            ycopy.wait_recv()
            out_ref[...] = total + ydst[...].astype(jnp.float32)
    ycopy.wait_send()
    for k in range(2):
        for d in range(2):
            first[k][d].wait_send()
            raw[k][d].wait_send()
            second[k * 2 + d].wait_send()


def mp_reduce(p, cid):
    _, n, w = p.shape
    D = pltpu.SemaphoreType.DMA
    half = n // 2
    return pl.pallas_call(
        reduce_kernel,
        out_shape=jax.ShapeDtypeStruct((n, w), jnp.float32),
        in_specs=[VM], out_specs=VM,
        scratch_shapes=[pltpu.VMEM((2, 2, half, w), p.dtype), pltpu.VMEM((2, 2, half, w), p.dtype),
                        pltpu.VMEM((2, 2, n, w), p.dtype), pltpu.VMEM((n, w), p.dtype), pltpu.VMEM((n, w), p.dtype),
                        D((2, 2)), D((2, 2)), D((2, 2)), D((2, 2)), D, D, D((2, 2)), D((2, 2))],
        compiler_params=pltpu.CompilerParams(collective_id=cid, has_side_effects=True, vmem_limit_bytes=32 << 20),
    )(p)


def ssd_kernel(xp_ref, bcd_ref, rimx_ref, rimbc_ref, cx_ref, cbc_ref, bias_ref, rate_ref, skip_ref,
               y_ref, cc_ref, cum_ref, send_ref, padx, padbc, state):
    n = xp_ref.shape[0]
    count = n // QB
    padx[pl.ds(0, 8), :] = rimx_ref[...]
    padbc[pl.ds(0, 8), :] = rimbc_ref[...]
    padx[pl.ds(8, n), :] = xp_ref[...]
    padbc[pl.ds(8, n), :] = bcd_ref[:, 0:2 * N]
    state[...] = jnp.zeros_like(state)
    row = lax.broadcasted_iota(jnp.int32, (QB, QB), 0)
    col = lax.broadcasted_iota(jnp.int32, (QB, QB), 1)
    causal = row >= col
    tri = jnp.where(causal, 1.0, 0.0).astype(jnp.float32)
    low = col < P_SIZE
    bf = jnp.bfloat16

    def silu(v):
        return v / (1.0 + jnp.exp(-v))

    def conv(pad, taps, start, lanes):
        whole = pad[pl.ds(start, QB + 8), lanes]
        total = taps[0:1, lanes] * whole[5:5 + QB]
        for j in range(1, 4):
            total = total + taps[j:j + 1, lanes] * whole[5 + j:5 + j + QB]
        return silu(total)

    def one(c, before):
        start = pl.multiple_of(c * QB, QB)
        here = pl.ds(start, QB)
        bv = conv(padbc, cbc_ref, start, slice(0, N))
        cv = conv(padbc, cbc_ref, start, slice(N, 2 * N)).astype(bf)
        cc_ref[here, :] = cv
        raw = bcd_ref[here, 2 * N:3 * N] + bias_ref[...]
        step = jnp.maximum(raw, 0.0) + jnp.log1p(jnp.exp(-jnp.abs(raw)))
        decay = -rate_ref[...] * step
        cum = jnp.dot(tri, decay, precision=lax.Precision.HIGHEST, preferred_element_type=jnp.float32)
        cum_ref[here, :] = cum + before
        cum_t, step_t = cum.T, step.T
        last = cum[QB - 1:QB, :]
        bt = bv.T.astype(bf)
        affinity = jnp.dot(cv, bt, preferred_element_type=jnp.float32)
        for p in range(xp_ref.shape[1] // 128):
            lanes = slice(p * 128, (p + 1) * 128)
            xv = conv(padx, cx_ref, start, lanes)
            mixes, grown, tails, ends = [], [], [], []
            for h in (2 * p, 2 * p + 1):
                ct = jnp.broadcast_to(cum[:, h:h + 1], (QB, QB))
                st = jnp.broadcast_to(step[:, h:h + 1], (QB, QB))
                end = jnp.broadcast_to(last[:, h:h + 1], (1, QB))
                spread = jnp.where(causal, ct - cum_t[h:h + 1, :], -jnp.inf)
                mixes.append((affinity * jnp.exp(spread) * step_t[h:h + 1, :]).astype(bf))
                grown.append(ct)
                tails.append(jnp.exp(end - ct) * st)
                ends.append(end)
            lowhalf = low[0:1]
            mixed = jnp.concatenate(mixes, axis=1)
            xs = jnp.concatenate([jnp.where(low, xv, 0.0).astype(bf), jnp.where(low, 0.0, xv).astype(bf)], axis=0)
            out = jnp.dot(mixed, xs, preferred_element_type=jnp.float32)
            old = state[:, lanes]
            carried = jnp.dot(cv, old.astype(bf), preferred_element_type=jnp.float32)
            out = out + jnp.exp(jnp.where(low, grown[0], grown[1])) * carried
            y_ref[here, lanes] = out + skip_ref[0:1, lanes] * xv
            weighted = (xv * jnp.where(low, tails[0], tails[1])).astype(bf)
            fresh = jnp.dot(bt, weighted, preferred_element_type=jnp.float32)
            state[:, lanes] = jnp.exp(jnp.where(lowhalf, ends[0], ends[1])) * old + fresh
        return before + last

    total = lax.fori_loop(0, count, one, jnp.zeros((1, 128), jnp.float32))
    send_ref[0:N, :] = state[...].astype(bf)
    for p in range(xp_ref.shape[1] // 128):
        lanes = slice(p * 128, (p + 1) * 128)
        ends = [jnp.broadcast_to(total[:, h:h + 1], (16, 128)) for h in (2 * p, 2 * p + 1)]
        decay = jnp.exp(jnp.where(low[0:16], ends[0], ends[1]))
        big = decay.astype(bf)
        rest = decay - big.astype(jnp.float32)
        middle = rest.astype(bf)
        small = (rest - middle.astype(jnp.float32)).astype(bf)
        which = row[0:16]
        send_ref[N:N + 16, lanes] = jnp.where(which == 0, big.astype(jnp.float32), jnp.where(
            which == 1, middle.astype(jnp.float32), small.astype(jnp.float32))).astype(bf)


def run_ssd(xp, bcd, rimx, rimbc, conv_x, conv_bc, bias, rate, skip):
    n, width = xp.shape
    f32, bf = jnp.float32, jnp.bfloat16
    return pl.pallas_call(
        ssd_kernel,
        out_shape=(jax.ShapeDtypeStruct((n, width), f32), jax.ShapeDtypeStruct((n, N), bf),
                   jax.ShapeDtypeStruct((n, 128), f32), jax.ShapeDtypeStruct((N + 16, width), bf)),
        in_specs=[VM] * 9, out_specs=(VM,) * 4,
        scratch_shapes=[pltpu.VMEM((n + 8, width), f32), pltpu.VMEM((n + 8, 2 * N), f32), pltpu.VMEM((N, width), f32)],
        compiler_params=pltpu.CompilerParams(vmem_limit_bytes=32 << 20),
        cost_estimate=pl.CostEstimate(flops=4_000_000_000, bytes_accessed=8 << 20, transcendentals=0),
    )(xp, bcd, rimx, rimbc, conv_x, conv_bc, bias, rate, skip)


def gate_kernel(y_ref, cc_ref, cum_ref, states_ref, gate_ref, gain_ref, out_ref, incoming, full):
    place = lax.axis_index("seq")
    n, width = y_ref.shape
    bf, f32 = jnp.bfloat16, jnp.float32
    incoming[...] = jnp.zeros_like(incoming)

    def add(k, _):
        tail = states_ref[k, N:N + 16, :].astype(f32)
        decay = tail[0:1] + (tail[1:2] + tail[2:3])
        incoming[...] = decay * incoming[...] + states_ref[k, 0:N, :].astype(f32)
        return 0

    lax.fori_loop(0, place, add, 0)
    low = lax.broadcasted_iota(jnp.int32, (QB, 128), 1) < P_SIZE

    def one(c, _):
        here = pl.ds(pl.multiple_of(c * QB, QB), QB)
        cv = cc_ref[here, :]
        cum = cum_ref[here, :]
        square = jnp.zeros((QB, 128), f32)
        for p in range(width // 128):
            lanes = slice(p * 128, (p + 1) * 128)
            ct = jnp.where(low, jnp.broadcast_to(cum[:, 2 * p:2 * p + 1], (QB, 128)),
                           jnp.broadcast_to(cum[:, 2 * p + 1:2 * p + 2], (QB, 128)))
            carried = jnp.dot(cv, incoming[:, lanes].astype(bf), preferred_element_type=f32)
            g = gate_ref[here, lanes]
            value = (y_ref[here, lanes] + jnp.exp(ct) * carried) * (g / (1.0 + jnp.exp(-g)))
            full[:, lanes] = value
            square = square + value * value
        scale = lax.rsqrt(jnp.sum(square, axis=1, keepdims=True) / width + 1e-05)
        out_ref[here, :] = (full[...] * scale * gain_ref[...]).astype(bf)
        return 0

    lax.fori_loop(0, n // QB, one, 0)


def run_gate(y, cc, cum, states, gate, gain):
    n, width = y.shape
    return pl.pallas_call(
        gate_kernel,
        out_shape=jax.ShapeDtypeStruct((n, width), jnp.bfloat16),
        in_specs=[VM] * 6, out_specs=VM,
        scratch_shapes=[pltpu.VMEM((N, width), jnp.float32), pltpu.VMEM((QB, width), jnp.float32)],
        compiler_params=pltpu.CompilerParams(vmem_limit_bytes=32 << 20),
        cost_estimate=pl.CostEstimate(flops=2_000_000_000, bytes_accessed=8 << 20, transcendentals=0),
    )(y, cc, cum, states, gate, gain)


def out_kernel(y_ref, w_ref, out_ref):
    out_ref[0] = jnp.dot(y_ref[...], w_ref[0], preferred_element_type=jnp.float32).astype(out_ref.dtype)


def run_out(y, w):
    n, width = y.shape
    cols = w.shape[2]
    return pl.pallas_call(
        out_kernel,
        out_shape=jax.ShapeDtypeStruct((8, n, 2 * cols), jnp.bfloat16),
        grid=(w.shape[0],),
        in_specs=[pl.BlockSpec((n, width), lambda j: (0, 0)), pl.BlockSpec((1, width, cols), lambda j: (j, 0, 0))],
        out_specs=pl.BlockSpec((1, n, cols), lambda j: (j // 2, 0, j % 2)),
        compiler_params=pltpu.CompilerParams(vmem_limit_bytes=16 << 20),
        cost_estimate=pl.CostEstimate(flops=2 * n * width * 4096, bytes_accessed=16 << 20, transcendentals=0),
    )(y, w)


def attention_kernel(q_ref, kv_ref, out_ref, peak, total):
    place = lax.axis_index("seq")
    j = pl.program_id(0)
    reach = pl.num_programs(0) - 1
    n = q_ref.shape[0]
    heads = q_ref.shape[1] // HD
    scale = HD ** -0.5 * 1.4426950408889634

    @pl.when(j == 0)
    def _():
        peak[...] = jnp.full_like(peak, -1e30)
        total[...] = jnp.zeros_like(total)

    def work(edge):
        keys = kv_ref[0, :, 0:HD]
        both = jnp.concatenate([kv_ref[0, :, HD:2 * HD], jnp.ones((n, HD), jnp.bfloat16)], axis=1)
        for h in range(heads):
            scores = lax.dot_general(q_ref[:, h * HD:(h + 1) * HD], keys, (((1,), (1,)), ((), ())),
                                     preferred_element_type=jnp.float32) * scale
            if edge is not None:
                t = lax.broadcasted_iota(jnp.int32, (n, n), 0)
                s = lax.broadcasted_iota(jnp.int32, (n, n), 1)
                scores = jnp.where(s > t if edge == 0 else s <= t, scores, -1e30)
            old = peak[h]
            new = jnp.maximum(old, jnp.max(scores, axis=1, keepdims=True))
            weights = jnp.exp2(scores - new[:, 0:1])
            if edge == 0:
                weights = jnp.where(s > t, weights, 0.0)
            shrink = jnp.exp2(old - new)
            peak[h] = new
            total[h] = jnp.concatenate([shrink, shrink], axis=1) * total[h] + jnp.dot(
                weights.astype(jnp.bfloat16), both, preferred_element_type=jnp.float32)

    @pl.when((j == 0) & (place >= reach))
    def _():
        work(0)

    @pl.when((j > 0) & (j < reach) & (place + j >= reach))
    def _():
        work(None)

    @pl.when(j == reach)
    def _():
        work(1)
        for h in range(heads):
            out_ref[:, h * HD:(h + 1) * HD] = total[h, :, 0:HD] / total[h, :, HD:2 * HD]


def run_attention(q, kv):
    n, width = q.shape
    reach = WINDOW // n
    heads = width // HD
    return pl.pallas_call(
        attention_kernel,
        out_shape=jax.ShapeDtypeStruct((n, width), jnp.float32),
        grid=(reach + 1,),
        in_specs=[pl.BlockSpec((n, width), lambda j: (0, 0)),
                  pl.BlockSpec((1, n, 2 * HD), lambda j: (jnp.maximum(lax.axis_index("seq") + j - reach, 0), 0, 0))],
        out_specs=pl.BlockSpec((n, width), lambda j: (0, 0)),
        scratch_shapes=[pltpu.VMEM((heads, n, HD), jnp.float32), pltpu.VMEM((heads, n, 2 * HD), jnp.float32)],
        compiler_params=pltpu.CompilerParams(vmem_limit_bytes=32 << 20),
        cost_estimate=pl.CostEstimate(flops=8 * n * width * WINDOW, bytes_accessed=8 << 20, transcendentals=0),
    )(q, kv)


def rms_norm(values, gain):
    return values * lax.rsqrt(jnp.mean(values * values, axis=-1, keepdims=True) + 1e-05) * gain


def padded(vector):
    return jnp.pad(vector, (0, 128 - vector.shape[0]))[None, :]


def on_device(hidden_in, norm_gain, w_z, w_x, w_b, w_c, w_dt, conv_x, conv_b, conv_c, dt_bias, a_rate,
              skip_gain, group_gain, w_out, attn_gain, w_q, w_k, w_v):
    f32, bf = jnp.float32, jnp.bfloat16
    n = hidden_in.shape[0]
    w_bcd = jnp.concatenate([w_b, w_c, jnp.pad(w_dt, ((0, 0), (0, 128 - w_dt.shape[1])))], axis=1)
    w_x_all = lax.all_gather(w_x, "seq", axis=0, tiled=True)
    w_bcd_all = lax.all_gather(w_bcd, "seq", axis=0, tiled=True)
    w_z_all = lax.all_gather(w_z, "seq", axis=0, tiled=True)
    w_out_all = lax.all_gather(w_out, "seq")
    normed = mp_gather_norm(hidden_in, norm_gain[None, :], 0)
    bcd = jnp.dot(normed, w_bcd_all, preferred_element_type=f32)
    xp = jnp.dot(normed, w_x_all, preferred_element_type=f32)
    route = [(i, i + 1) for i in range(lax.axis_size("seq") - 1)]
    rims = lax.ppermute(jnp.concatenate([xp[n - 8:], bcd[n - 8:, 0:2 * N]], axis=1), "seq", route)
    width = xp.shape[1]
    y, cc, cum, send = run_ssd(
        xp, bcd, rims[:, 0:width], rims[:, width:], conv_x, jnp.concatenate([conv_b, conv_c], axis=1),
        padded(dt_bias), padded(a_rate), jnp.repeat(skip_gain, P_SIZE)[None, :])
    states = lax.all_gather(send, "seq")
    gate = jnp.dot(normed, w_z_all, preferred_element_type=f32)
    y_normed = run_gate(y, cc, cum, states, gate, group_gain[None, :])
    parts = run_out(y_normed, w_out_all)
    mixed = hidden_in.astype(f32) + mp_reduce(parts, 1)
    normed_two = mp_gather_norm(mixed.astype(bf), attn_gain[None, :], 2)
    keys = jnp.dot(normed_two, w_k, preferred_element_type=f32).astype(bf)
    values = jnp.dot(normed_two, w_v, preferred_element_type=f32).astype(bf)
    kv = lax.all_gather(jnp.concatenate([keys, values], axis=1), "seq")
    queries = jnp.dot(normed_two, w_q, preferred_element_type=f32).astype(bf)
    return (mixed, run_attention(queries, kv))


def solution(mesh):
    tile, cols = P("seq", "mp"), P(None, "mp")
    placed = (tile, P(), tile, tile, tile, tile, tile, cols, cols, cols, P("mp"), P("mp"), P("mp"), P("mp"),
              P("mp", "seq"), P(), cols, cols, cols)
    return jax.shard_map(on_device, mesh=mesh, in_specs=placed, out_specs=(tile, tile), check_vma=False)
```

```python
import jax
import jax.numpy as jnp
from jax import lax
from jax.experimental import pallas as pl
from jax.experimental.pallas import tpu as pltpu
from jax.sharding import PartitionSpec as P

MESH = pl.DeviceIdType.MESH
VM = pl.BlockSpec(memory_space=pltpu.VMEM)
P_SIZE = 64
N = 128
HD = 128
WINDOW = 4096
QB = 128


def rows(start, size):
    return pl.ds(start, size)


class Gather:
    def __init__(self, view, own, names, pair, ring, core, sends, recvs, base, pieces, fan):
        self.view, self.own, self.names = view, own, names
        self.pair, self.ring, self.core = pair, ring, core
        self.sends, self.recvs, self.next, self.pieces, self.fan = sends, recvs, base, pieces, fan
        self.right, self.left, self.far = (ring + 1) % 4, (ring + 3) % 4, (ring + 2) % 4
        self.started, self.across = [], []
        self.y, self.a, self.b, self.f = {}, {}, {}, []

    def send(self, src, block, piece, pair, ring, core):
        copy = pltpu.make_async_remote_copy(
            src_ref=src, dst_ref=self.view(*block, piece), send_sem=self.sends.at[self.next], recv_sem=self.recvs.at[self.next],
            device_id=self.names(pair, ring, core), device_id_type=MESH)
        self.next += 1
        copy.start()
        self.started.append(copy)
        return copy

    def over(self, src, block, piece):
        if self.fan:
            self.across.append(self.send(src, block, piece, self.pair, self.ring, 1 - self.core))

    def begin(self):
        me = (self.pair, self.ring, self.core)
        for k, piece in enumerate(self.pieces):
            src = self.own(piece)
            self.y[k] = self.send(src, me, piece, 1 - self.pair, self.ring, self.core)
            self.a[k] = [self.send(src, me, piece, self.pair, to, self.core) for to in (self.right, self.left)]
            self.over(src, me, piece)

    def second(self, k):
        piece, block = self.pieces[k], (1 - self.pair, self.ring, self.core)
        self.y[k].wait_recv()
        src = self.view(*block, piece)
        self.b[k] = [self.send(src, block, piece, self.pair, to, self.core) for to in (self.right, self.left)]
        self.over(src, block, piece)

    def forward(self, which, k):
        pair = self.pair if which == 0 else 1 - self.pair
        piece, first = self.pieces[k], k < len(self.pieces) // 2
        for d, (to, origin) in enumerate(((self.right, self.left), (self.left, self.right))):
            (self.a, self.b)[which][k][d].wait_recv()
            block = (pair, origin, self.core)
            src = self.view(*block, piece)
            if first == (d == 0):
                self.f.append((self.send(src, block, piece, self.pair, to, self.core), (pair, self.far, self.core), piece))
            self.over(src, block, piece)

    def last(self):
        for copy, block, piece in self.f:
            copy.wait_recv()
            self.over(self.view(*block, piece), block, piece)

    def finish(self):
        for copy in self.across:
            copy.wait_recv()
        for copy in self.started:
            copy.wait_send()


def copies_of(pieces, fan):
    return pieces * (7 + (8 if fan else 0))


def seq_names(pair, ring, core):
    return {"seq": (pair * 4 + ring) * 2 + core}


def mp_names(pair, ring, core):
    return {"mp": pair * 4 + ring}


def greet(ids):
    barrier = pltpu.get_barrier_semaphore()
    for other in ids:
        pl.semaphore_signal(barrier, inc=1, device_id=other, device_id_type=MESH)
    pl.semaphore_wait(barrier, len(ids))


def seq_place():
    me = lax.axis_index("seq")
    return me // 8, (me // 2) % 4, me % 2


def mp_place():
    me = lax.axis_index("mp")
    return me // 4, me % 4


def neighbours(names, pair, ring, core, fan):
    ids = [names(1 - pair, ring, core), names(pair, (ring + 1) % 4, core), names(pair, (ring + 3) % 4, core)]
    return ids + ([names(pair, ring, 1 - core)] if fan else [])


def cut(total, count):
    return [pl.ds(k * (total // count), total // count) for k in range(count)]


def write_normed(whole, gain_ref, normed_ref):
    blocks, n, wide = whole.shape

    def norm(c, _):
        piece = rows(pl.multiple_of(c * 32, 32), 32)
        square = jnp.zeros((32, wide), jnp.float32)
        for b in range(blocks):
            value = whole[b, piece, :].astype(jnp.float32)
            square = square + value * value
        scale = lax.rsqrt(jnp.sum(square, axis=1, keepdims=True) / (blocks * wide) + 1e-05)
        for b in range(blocks):
            lanes = slice(b * wide, (b + 1) * wide)
            normed_ref[piece, lanes] = (whole[b, piece, :].astype(jnp.float32) * scale * gain_ref[:, lanes]).astype(normed_ref.dtype)
        return 0

    lax.fori_loop(0, n // 32, norm, 0)


def first_kernel(x_ref, wx_ref, wb_ref, gain_ref, normed_ref, wxa_ref, wba_ref, whole, local, ms, mr, bs, br, xs, xr):
    mpair, mring = mp_place()
    spair, sring, score = seq_place()
    greet(neighbours(mp_names, mpair, mring, 0, False) + neighbours(seq_names, spair, sring, score, True))
    depth = wx_ref.shape[0]

    def wide_view(ref):
        return lambda pair, ring, core, piece: ref.at[pl.ds(((pair * 4 + ring) * 2 + core) * depth + piece.start, piece.size), :]

    hidden = Gather(lambda pair, ring, core, piece: whole.at[pair * 4 + ring, piece], lambda piece: x_ref.at[piece], mp_names,
                    mpair, mring, 0, ms, mr, 0, cut(x_ref.shape[0], 2), False)
    small = Gather(wide_view(wba_ref), lambda piece: wb_ref.at[piece], seq_names, spair, sring, score, bs, br, 0, cut(depth, 2), True)
    big = Gather(wide_view(wxa_ref), lambda piece: wx_ref.at[piece], seq_names, spair, sring, score, xs, xr, 0, cut(depth, 2), True)
    here = (spair * 4 + sring) * 2 + score
    mine = [pltpu.make_async_copy(x_ref, whole.at[mpair * 4 + mring], local.at[0]),
            pltpu.make_async_copy(wx_ref, wxa_ref.at[pl.ds(here * depth, depth), :], local.at[1]),
            pltpu.make_async_copy(wb_ref, wba_ref.at[pl.ds(here * depth, depth), :], local.at[2])]
    everything = (hidden, small, big)
    for g in everything:
        g.begin()
    for copy in mine:
        copy.start()
    for k in range(2):
        for g in (small, hidden, big):
            g.second(k)
    for which in range(2):
        for k in range(2):
            for g in (small, hidden, big):
                g.forward(which, k)
    hidden.last()
    mine[0].wait()
    write_normed(whole, gain_ref, normed_ref)
    small.last()
    big.last()
    for g in everything:
        g.finish()
    for copy in mine[1:]:
        copy.wait()


def run_first(x, wx, wb, gain, cid):
    n, w = x.shape
    depth = wx.shape[0]
    D = pltpu.SemaphoreType.DMA
    few, many = copies_of(2, False), copies_of(2, True)
    bf = jnp.bfloat16
    return pl.pallas_call(
        first_kernel,
        out_shape=(jax.ShapeDtypeStruct((n, 8 * w), bf), jax.ShapeDtypeStruct((16 * depth, wx.shape[1]), bf),
                   jax.ShapeDtypeStruct((16 * depth, wb.shape[1]), bf)),
        in_specs=[VM] * 4, out_specs=(VM,) * 3,
        scratch_shapes=[pltpu.VMEM((8, n, w), bf), D((3,)), D((few,)), D((few,)), D((many,)), D((many,)), D((many,)), D((many,))],
        compiler_params=pltpu.CompilerParams(collective_id=cid, has_side_effects=True, vmem_limit_bytes=40 << 20),
    )(x, wx, wb, gain)


def norm_kernel(x_ref, gain_ref, normed_ref, whole, local, ms, mr):
    pair, ring = mp_place()
    greet(neighbours(mp_names, pair, ring, 0, False))
    hidden = Gather(lambda pair, ring, core, piece: whole.at[pair * 4 + ring, piece], lambda piece: x_ref.at[piece], mp_names,
                    pair, ring, 0, ms, mr, 0, cut(x_ref.shape[0], 4), False)
    mine = pltpu.make_async_copy(x_ref, whole.at[pair * 4 + ring], local)
    hidden.begin()
    mine.start()
    for k in range(4):
        hidden.second(k)
    for which in range(2):
        for k in range(4):
            hidden.forward(which, k)
    hidden.last()
    hidden.finish()
    mine.wait()
    write_normed(whole, gain_ref, normed_ref)


def run_norm(x, gain, cid):
    n, w = x.shape
    D = pltpu.SemaphoreType.DMA
    few = copies_of(4, False)
    return pl.pallas_call(
        norm_kernel,
        out_shape=jax.ShapeDtypeStruct((n, 8 * w), x.dtype),
        in_specs=[VM, VM], out_specs=VM,
        scratch_shapes=[pltpu.VMEM((8, n, w), x.dtype), D, D((few,)), D((few,))],
        compiler_params=pltpu.CompilerParams(collective_id=cid, has_side_effects=True, vmem_limit_bytes=24 << 20),
    )(x, gain)


def reduce_kernel(p_ref, out_ref, tmp, d1, d2, ysrc, ydst, s1, r1, s2, r2, sy, ry, sraw, rraw):
    high, low = mp_place()
    right, left = (low + 1) % 4, (low + 3) % 4
    far = (low + 2) % 4
    partner = (1 - high) * 4 + low
    greet(neighbours(mp_names, high, low, 0, False))
    n = p_ref.shape[1]
    half = n // 2
    order = (1 - high, high)
    sides = ((right, left), (left, right))

    def send(src, dst, target, ssem, rsem):
        copy = pltpu.make_async_remote_copy(src_ref=src, dst_ref=dst, send_sem=ssem, recv_sem=rsem,
                                            device_id={"mp": target}, device_id_type=MESH)
        copy.start()
        return copy

    first = [[send(p_ref.at[order[k] * 4 + far, rows(d * half, half)], d1.at[k, d], high * 4 + sides[d][0],
                   s1.at[k, d], r1.at[k, d]) for d in range(2)] for k in range(2)]
    raw = [[send(p_ref.at[order[k] * 4 + sides[d][0], rows((1 - d) * half, half)],
                 d2.at[k, d, rows((1 - d) * half, half)], high * 4 + sides[d][0],
                 sraw.at[k, d], rraw.at[k, d]) for d in range(2)] for k in range(2)]
    second = []
    for k in range(2):
        for d in range(2):
            first[k][d].wait_recv()
            tmp[k, d] = (d1[k, d].astype(jnp.float32)
                         + p_ref[order[k] * 4 + sides[d][0], d * half:(d + 1) * half].astype(jnp.float32)).astype(tmp.dtype)
            second.append(send(tmp.at[k, d], d2.at[k, d, rows(d * half, half)], high * 4 + sides[d][0],
                               s2.at[k, d], r2.at[k, d]))
    totals = None
    for k in range(2):
        for d in range(2):
            raw[k][d].wait_recv()
            second[k * 2 + d].wait_recv()
        total = (p_ref[order[k] * 4 + low].astype(jnp.float32) + d2[k, 0].astype(jnp.float32)
                 + d2[k, 1].astype(jnp.float32))
        if k == 0:
            ysrc[...] = total.astype(ysrc.dtype)
            ycopy = send(ysrc, ydst, partner, sy, ry)
        else:
            ycopy.wait_recv()
            out_ref[...] = total + ydst[...].astype(jnp.float32)
    ycopy.wait_send()
    for k in range(2):
        for d in range(2):
            first[k][d].wait_send()
            raw[k][d].wait_send()
            second[k * 2 + d].wait_send()


def mp_reduce(p, cid):
    _, n, w = p.shape
    D = pltpu.SemaphoreType.DMA
    half = n // 2
    return pl.pallas_call(
        reduce_kernel,
        out_shape=jax.ShapeDtypeStruct((n, w), jnp.float32),
        in_specs=[VM], out_specs=VM,
        scratch_shapes=[pltpu.VMEM((2, 2, half, w), p.dtype), pltpu.VMEM((2, 2, half, w), p.dtype),
                        pltpu.VMEM((2, 2, n, w), p.dtype), pltpu.VMEM((n, w), p.dtype), pltpu.VMEM((n, w), p.dtype),
                        D((2, 2)), D((2, 2)), D((2, 2)), D((2, 2)), D, D, D((2, 2)), D((2, 2))],
        compiler_params=pltpu.CompilerParams(collective_id=cid, has_side_effects=True, vmem_limit_bytes=32 << 20),
    )(p)


def ssd_kernel(xp_ref, bcd_ref, rimx_ref, rimbc_ref, cx_ref, cbc_ref, bias_ref, rate_ref, skip_ref,
               y_ref, cc_ref, cum_ref, send_ref, padx, padbc, state):
    n = xp_ref.shape[0]
    count = n // QB
    padx[pl.ds(0, 8), :] = rimx_ref[...]
    padbc[pl.ds(0, 8), :] = rimbc_ref[...]
    padx[pl.ds(8, n), :] = xp_ref[...]
    padbc[pl.ds(8, n), :] = bcd_ref[:, 0:2 * N]
    state[...] = jnp.zeros_like(state)
    row = lax.broadcasted_iota(jnp.int32, (QB, QB), 0)
    col = lax.broadcasted_iota(jnp.int32, (QB, QB), 1)
    causal = row >= col
    tri = jnp.where(causal, 1.0, 0.0).astype(jnp.float32)
    low = col < P_SIZE
    bf = jnp.bfloat16

    def silu(v):
        return v / (1.0 + jnp.exp(-v))

    def conv(pad, taps, start, lanes):
        whole = pad[pl.ds(start, QB + 8), lanes]
        total = taps[0:1, lanes] * whole[5:5 + QB]
        for j in range(1, 4):
            total = total + taps[j:j + 1, lanes] * whole[5 + j:5 + j + QB]
        return silu(total)

    def one(c, before):
        start = pl.multiple_of(c * QB, QB)
        here = pl.ds(start, QB)
        bv = conv(padbc, cbc_ref, start, slice(0, N))
        cv = conv(padbc, cbc_ref, start, slice(N, 2 * N)).astype(bf)
        cc_ref[here, :] = cv
        raw = bcd_ref[here, 2 * N:3 * N] + bias_ref[...]
        step = jnp.maximum(raw, 0.0) + jnp.log1p(jnp.exp(-jnp.abs(raw)))
        decay = -rate_ref[...] * step
        cum = jnp.dot(tri, decay, precision=lax.Precision.HIGHEST, preferred_element_type=jnp.float32)
        cum_ref[here, :] = cum + before
        cum_t, step_t = cum.T, step.T
        last = cum[QB - 1:QB, :]
        bt = bv.T.astype(bf)
        affinity = jnp.dot(cv, bt, preferred_element_type=jnp.float32)
        for p in range(xp_ref.shape[1] // 128):
            lanes = slice(p * 128, (p + 1) * 128)
            xv = conv(padx, cx_ref, start, lanes)
            mixes, grown, tails, ends = [], [], [], []
            for h in (2 * p, 2 * p + 1):
                ct = jnp.broadcast_to(cum[:, h:h + 1], (QB, QB))
                st = jnp.broadcast_to(step[:, h:h + 1], (QB, QB))
                end = jnp.broadcast_to(last[:, h:h + 1], (1, QB))
                spread = jnp.where(causal, ct - cum_t[h:h + 1, :], -jnp.inf)
                mixes.append((affinity * jnp.exp(spread) * step_t[h:h + 1, :]).astype(bf))
                grown.append(ct)
                tails.append(jnp.exp(end - ct) * st)
                ends.append(end)
            lowhalf = low[0:1]
            mixed = jnp.concatenate(mixes, axis=1)
            xs = jnp.concatenate([jnp.where(low, xv, 0.0).astype(bf), jnp.where(low, 0.0, xv).astype(bf)], axis=0)
            out = jnp.dot(mixed, xs, preferred_element_type=jnp.float32)
            old = state[:, lanes]
            carried = jnp.dot(cv, old.astype(bf), preferred_element_type=jnp.float32)
            out = out + jnp.exp(jnp.where(low, grown[0], grown[1])) * carried
            y_ref[here, lanes] = out + skip_ref[0:1, lanes] * xv
            weighted = (xv * jnp.where(low, tails[0], tails[1])).astype(bf)
            fresh = jnp.dot(bt, weighted, preferred_element_type=jnp.float32)
            state[:, lanes] = jnp.exp(jnp.where(lowhalf, ends[0], ends[1])) * old + fresh
        return before + last

    total = lax.fori_loop(0, count, one, jnp.zeros((1, 128), jnp.float32))
    send_ref[0:N, :] = state[...].astype(bf)
    for p in range(xp_ref.shape[1] // 128):
        lanes = slice(p * 128, (p + 1) * 128)
        ends = [jnp.broadcast_to(total[:, h:h + 1], (16, 128)) for h in (2 * p, 2 * p + 1)]
        decay = jnp.exp(jnp.where(low[0:16], ends[0], ends[1]))
        big = decay.astype(bf)
        rest = decay - big.astype(jnp.float32)
        middle = rest.astype(bf)
        small = (rest - middle.astype(jnp.float32)).astype(bf)
        which = row[0:16]
        send_ref[N:N + 16, lanes] = jnp.where(which == 0, big.astype(jnp.float32), jnp.where(
            which == 1, middle.astype(jnp.float32), small.astype(jnp.float32))).astype(bf)


def run_ssd(xp, bcd, rimx, rimbc, conv_x, conv_bc, bias, rate, skip):
    n, width = xp.shape
    f32, bf = jnp.float32, jnp.bfloat16
    return pl.pallas_call(
        ssd_kernel,
        out_shape=(jax.ShapeDtypeStruct((n, width), f32), jax.ShapeDtypeStruct((n, N), bf),
                   jax.ShapeDtypeStruct((n, 128), f32), jax.ShapeDtypeStruct((N + 16, width), bf)),
        in_specs=[VM] * 9, out_specs=(VM,) * 4,
        scratch_shapes=[pltpu.VMEM((n + 8, width), f32), pltpu.VMEM((n + 8, 2 * N), f32), pltpu.VMEM((N, width), f32)],
        compiler_params=pltpu.CompilerParams(vmem_limit_bytes=32 << 20),
        cost_estimate=pl.CostEstimate(flops=4_000_000_000, bytes_accessed=8 << 20, transcendentals=0),
    )(xp, bcd, rimx, rimbc, conv_x, conv_bc, bias, rate, skip)


def gate_kernel(normed_ref, wz_ref, send_ref, y_ref, cc_ref, cum_ref, gain_ref, out_ref, states, incoming, gate, local, ss, sr):
    place = lax.axis_index("seq")
    pair, ring, core = seq_place()
    greet(neighbours(seq_names, pair, ring, core, True))
    n, width = y_ref.shape
    bf, f32 = jnp.bfloat16, jnp.float32
    tall = send_ref.shape[0]
    every = Gather(lambda pair, ring, core, piece: states.at[(pair * 4 + ring) * 2 + core, piece], lambda piece: send_ref.at[piece],
                   seq_names, pair, ring, core, ss, sr, 0, [pl.ds(0, 80), pl.ds(80, tall - 80)], True)
    mine = pltpu.make_async_copy(send_ref, states.at[place], local)
    every.begin()
    mine.start()

    def matmul(part):
        lanes = slice(part * 128, (part + 1) * 128)
        gate[:, lanes] = jnp.dot(normed_ref[...], wz_ref[:, lanes], preferred_element_type=f32)

    matmul(0)
    matmul(1)
    every.second(0)
    every.second(1)
    matmul(2)
    every.forward(0, 0)
    every.forward(0, 1)
    matmul(3)
    matmul(4)
    every.forward(1, 0)
    every.forward(1, 1)
    matmul(5)
    matmul(6)
    matmul(7)
    every.last()
    every.finish()
    mine.wait()
    incoming[...] = jnp.zeros_like(incoming)

    def add(k, _):
        tail = states[k, N:N + 16, :].astype(f32)
        decay = tail[0:1] + (tail[1:2] + tail[2:3])
        incoming[...] = decay * incoming[...] + states[k, 0:N, :].astype(f32)
        return 0

    lax.fori_loop(0, place, add, 0)
    low = lax.broadcasted_iota(jnp.int32, (QB, 128), 1) < P_SIZE

    def one(c, _):
        here = pl.ds(pl.multiple_of(c * QB, QB), QB)
        cv = cc_ref[here, :]
        cum = cum_ref[here, :]
        square = jnp.zeros((QB, 128), f32)
        for p in range(width // 128):
            lanes = slice(p * 128, (p + 1) * 128)
            ct = jnp.where(low, jnp.broadcast_to(cum[:, 2 * p:2 * p + 1], (QB, 128)),
                           jnp.broadcast_to(cum[:, 2 * p + 1:2 * p + 2], (QB, 128)))
            carried = jnp.dot(cv, incoming[:, lanes].astype(bf), preferred_element_type=f32)
            g = gate[here, lanes]
            value = (y_ref[here, lanes] + jnp.exp(ct) * carried) * (g / (1.0 + jnp.exp(-g)))
            gate[here, lanes] = value
            square = square + value * value
        scale = lax.rsqrt(jnp.sum(square, axis=1, keepdims=True) / width + 1e-05)
        out_ref[here, :] = (gate[here, :] * scale * gain_ref[...]).astype(bf)
        return 0

    lax.fori_loop(0, n // QB, one, 0)


def run_gate(normed, wz, send, y, cc, cum, gain, cid):
    n, width = y.shape
    D = pltpu.SemaphoreType.DMA
    many = copies_of(2, True)
    return pl.pallas_call(
        gate_kernel,
        out_shape=jax.ShapeDtypeStruct((n, width), jnp.bfloat16),
        in_specs=[VM] * 7, out_specs=VM,
        scratch_shapes=[pltpu.VMEM((16,) + send.shape, jnp.bfloat16), pltpu.VMEM((N, width), jnp.float32),
                        pltpu.VMEM((n, width), jnp.float32), D, D((many,)), D((many,))],
        compiler_params=pltpu.CompilerParams(collective_id=cid, has_side_effects=True, vmem_limit_bytes=40 << 20),
    )(normed, wz, send, y, cc, cum, gain)


def out_kernel(y_ref, w_ref, out_ref):
    out_ref[0] = jnp.dot(y_ref[...], w_ref[0], preferred_element_type=jnp.float32).astype(out_ref.dtype)


def run_out(y, w):
    n, width = y.shape
    cols = w.shape[2]
    return pl.pallas_call(
        out_kernel,
        out_shape=jax.ShapeDtypeStruct((8, n, 2 * cols), jnp.bfloat16),
        grid=(w.shape[0],),
        in_specs=[pl.BlockSpec((n, width), lambda j: (0, 0)), pl.BlockSpec((1, width, cols), lambda j: (j, 0, 0))],
        out_specs=pl.BlockSpec((1, n, cols), lambda j: (j // 2, 0, j % 2)),
        compiler_params=pltpu.CompilerParams(vmem_limit_bytes=16 << 20),
        cost_estimate=pl.CostEstimate(flops=2 * n * width * 4096, bytes_accessed=16 << 20, transcendentals=0),
    )(y, w)


def attention_kernel(q_ref, kv_ref, out_ref, peak, total):
    place = lax.axis_index("seq")
    j = pl.program_id(0)
    reach = pl.num_programs(0) - 1
    n = q_ref.shape[0]
    heads = q_ref.shape[1] // HD
    scale = HD ** -0.5 * 1.4426950408889634

    @pl.when(j == 0)
    def _():
        peak[...] = jnp.full_like(peak, -1e30)
        total[...] = jnp.zeros_like(total)

    def work(edge):
        keys = kv_ref[0, :, 0:HD]
        both = jnp.concatenate([kv_ref[0, :, HD:2 * HD], jnp.ones((n, HD), jnp.bfloat16)], axis=1)
        for h in range(heads):
            scores = lax.dot_general(q_ref[:, h * HD:(h + 1) * HD], keys, (((1,), (1,)), ((), ())),
                                     preferred_element_type=jnp.float32) * scale
            if edge is not None:
                t = lax.broadcasted_iota(jnp.int32, (n, n), 0)
                s = lax.broadcasted_iota(jnp.int32, (n, n), 1)
                scores = jnp.where(s > t if edge == 0 else s <= t, scores, -1e30)
            old = peak[h]
            new = jnp.maximum(old, jnp.max(scores, axis=1, keepdims=True))
            weights = jnp.exp2(scores - new[:, 0:1])
            if edge == 0:
                weights = jnp.where(s > t, weights, 0.0)
            shrink = jnp.exp2(old - new)
            peak[h] = new
            total[h] = jnp.concatenate([shrink, shrink], axis=1) * total[h] + jnp.dot(
                weights.astype(jnp.bfloat16), both, preferred_element_type=jnp.float32)

    @pl.when((j == 0) & (place >= reach))
    def _():
        work(0)

    @pl.when((j > 0) & (j < reach) & (place + j >= reach))
    def _():
        work(None)

    @pl.when(j == reach)
    def _():
        work(1)
        for h in range(heads):
            out_ref[:, h * HD:(h + 1) * HD] = total[h, :, 0:HD] / total[h, :, HD:2 * HD]


def run_attention(q, kv):
    n, width = q.shape
    reach = WINDOW // n
    heads = width // HD
    return pl.pallas_call(
        attention_kernel,
        out_shape=jax.ShapeDtypeStruct((n, width), jnp.float32),
        grid=(reach + 1,),
        in_specs=[pl.BlockSpec((n, width), lambda j: (0, 0)),
                  pl.BlockSpec((1, n, 2 * HD), lambda j: (jnp.maximum(lax.axis_index("seq") + j - reach, 0), 0, 0))],
        out_specs=pl.BlockSpec((n, width), lambda j: (0, 0)),
        scratch_shapes=[pltpu.VMEM((heads, n, HD), jnp.float32), pltpu.VMEM((heads, n, 2 * HD), jnp.float32)],
        compiler_params=pltpu.CompilerParams(vmem_limit_bytes=32 << 20),
        cost_estimate=pl.CostEstimate(flops=8 * n * width * WINDOW, bytes_accessed=8 << 20, transcendentals=0),
    )(q, kv)


def padded(vector):
    return jnp.pad(vector, (0, 128 - vector.shape[0]))[None, :]


def on_device(hidden_in, norm_gain, w_z, w_x, w_b, w_c, w_dt, conv_x, conv_b, conv_c, dt_bias, a_rate,
              skip_gain, group_gain, w_out, attn_gain, w_q, w_k, w_v):
    f32, bf = jnp.float32, jnp.bfloat16
    n = hidden_in.shape[0]
    w_bcd = jnp.concatenate([w_b, w_c, jnp.pad(w_dt, ((0, 0), (0, 128 - w_dt.shape[1])))], axis=1)
    w_z_all = lax.all_gather(w_z, "seq", axis=0, tiled=True)
    w_out_all = lax.all_gather(w_out, "seq")
    normed, w_x_all, w_bcd_all = run_first(hidden_in, w_x, w_bcd, norm_gain[None, :], 0)
    bcd = jnp.dot(normed, w_bcd_all, preferred_element_type=f32)
    xp = jnp.dot(normed, w_x_all, preferred_element_type=f32)
    route = [(i, i + 1) for i in range(lax.axis_size("seq") - 1)]
    rims = lax.ppermute(jnp.concatenate([xp[n - 8:], bcd[n - 8:, 0:2 * N]], axis=1), "seq", route)
    width = xp.shape[1]
    y, cc, cum, send = run_ssd(
        xp, bcd, rims[:, 0:width], rims[:, width:], conv_x, jnp.concatenate([conv_b, conv_c], axis=1),
        padded(dt_bias), padded(a_rate), jnp.repeat(skip_gain, P_SIZE)[None, :])
    y_normed = run_gate(normed, w_z_all, send, y, cc, cum, group_gain[None, :], 3)
    parts = run_out(y_normed, w_out_all)
    mixed = hidden_in.astype(f32) + mp_reduce(parts, 1)
    normed_two = run_norm(mixed.astype(bf), attn_gain[None, :], 2)
    keys = jnp.dot(normed_two, w_k, preferred_element_type=f32).astype(bf)
    values = jnp.dot(normed_two, w_v, preferred_element_type=f32).astype(bf)
    kv = lax.all_gather(jnp.concatenate([keys, values], axis=1), "seq")
    queries = jnp.dot(normed_two, w_q, preferred_element_type=f32).astype(bf)
    return (mixed, run_attention(queries, kv))


def solution(mesh):
    tile, cols = P("seq", "mp"), P(None, "mp")
    placed = (tile, P(), tile, tile, tile, tile, tile, cols, cols, cols, P("mp"), P("mp"), P("mp"), P("mp"),
              P("mp", "seq"), P(), cols, cols, cols)
    return jax.shard_map(on_device, mesh=mesh, in_specs=placed, out_specs=(tile, tile), check_vma=False)
```

```python
import jax
import jax.numpy as jnp
from jax import lax
from jax.experimental import pallas as pl
from jax.experimental.pallas import tpu as pltpu
from jax.sharding import PartitionSpec as P

MESH = pl.DeviceIdType.MESH
VM = pl.BlockSpec(memory_space=pltpu.VMEM)
P_SIZE = 64
N = 128
HD = 128
WINDOW = 4096
QB = 128


def rows(start, size):
    return pl.ds(start, size)


class Gather:
    def __init__(self, view, own, names, pair, ring, core, sends, recvs, base, pieces, fan):
        self.view, self.own, self.names = view, own, names
        self.pair, self.ring, self.core = pair, ring, core
        self.sends, self.recvs, self.next, self.pieces, self.fan = sends, recvs, base, pieces, fan
        self.right, self.left, self.far = (ring + 1) % 4, (ring + 3) % 4, (ring + 2) % 4
        self.started, self.across = [], []
        self.y, self.a, self.b, self.f = {}, {}, {}, []

    def send(self, src, block, piece, pair, ring, core):
        copy = pltpu.make_async_remote_copy(
            src_ref=src, dst_ref=self.view(*block, piece), send_sem=self.sends.at[self.next], recv_sem=self.recvs.at[self.next],
            device_id=self.names(pair, ring, core), device_id_type=MESH)
        self.next += 1
        copy.start()
        self.started.append(copy)
        return copy

    def over(self, src, block, piece):
        if self.fan:
            self.across.append(self.send(src, block, piece, self.pair, self.ring, 1 - self.core))

    def begin(self):
        me = (self.pair, self.ring, self.core)
        for k, piece in enumerate(self.pieces):
            src = self.own(piece)
            self.y[k] = self.send(src, me, piece, 1 - self.pair, self.ring, self.core)
            self.a[k] = [self.send(src, me, piece, self.pair, to, self.core) for to in (self.right, self.left)]
            self.over(src, me, piece)

    def second(self, k):
        piece, block = self.pieces[k], (1 - self.pair, self.ring, self.core)
        self.y[k].wait_recv()
        src = self.view(*block, piece)
        self.b[k] = [self.send(src, block, piece, self.pair, to, self.core) for to in (self.right, self.left)]
        self.over(src, block, piece)

    def forward(self, which, k):
        pair = self.pair if which == 0 else 1 - self.pair
        piece, first = self.pieces[k], k < len(self.pieces) // 2
        for d, (to, origin) in enumerate(((self.right, self.left), (self.left, self.right))):
            (self.a, self.b)[which][k][d].wait_recv()
            block = (pair, origin, self.core)
            src = self.view(*block, piece)
            if first == (d == 0):
                self.f.append((self.send(src, block, piece, self.pair, to, self.core), (pair, self.far, self.core), piece))
            self.over(src, block, piece)

    def last(self):
        for copy, block, piece in self.f:
            copy.wait_recv()
            self.over(self.view(*block, piece), block, piece)

    def finish(self):
        for copy in self.across:
            copy.wait_recv()
        for copy in self.started:
            copy.wait_send()


def copies_of(pieces, fan):
    return pieces * (7 + (8 if fan else 0))


def seq_names(pair, ring, core):
    return {"seq": (pair * 4 + ring) * 2 + core}


def mp_names(pair, ring, core):
    return {"mp": pair * 4 + ring}


def greet(ids):
    barrier = pltpu.get_barrier_semaphore()
    for other in ids:
        pl.semaphore_signal(barrier, inc=1, device_id=other, device_id_type=MESH)
    pl.semaphore_wait(barrier, len(ids))


def seq_place():
    me = lax.axis_index("seq")
    return me // 8, (me // 2) % 4, me % 2


def mp_place():
    me = lax.axis_index("mp")
    return me // 4, me % 4


def neighbours(names, pair, ring, core, fan):
    ids = [names(1 - pair, ring, core), names(pair, (ring + 1) % 4, core), names(pair, (ring + 3) % 4, core)]
    return ids + ([names(pair, ring, 1 - core)] if fan else [])


def cut(total, count):
    return [pl.ds(k * (total // count), total // count) for k in range(count)]


def write_normed(whole, gain_ref, normed_ref):
    blocks, n, wide = whole.shape

    def norm(c, _):
        piece = rows(pl.multiple_of(c * 32, 32), 32)
        square = jnp.zeros((32, wide), jnp.float32)
        for b in range(blocks):
            value = whole[b, piece, :].astype(jnp.float32)
            square = square + value * value
        scale = lax.rsqrt(jnp.sum(square, axis=1, keepdims=True) / (blocks * wide) + 1e-05)
        for b in range(blocks):
            lanes = slice(b * wide, (b + 1) * wide)
            normed_ref[piece, lanes] = (whole[b, piece, :].astype(jnp.float32) * scale * gain_ref[:, lanes]).astype(normed_ref.dtype)
        return 0

    lax.fori_loop(0, n // 32, norm, 0)


def first_kernel(x_ref, wx_ref, wb_ref, gain_ref, normed_ref, wxa_ref, wba_ref, whole, local, ms, mr, bs, br, xs, xr):
    mpair, mring = mp_place()
    spair, sring, score = seq_place()
    greet(neighbours(mp_names, mpair, mring, 0, False) + neighbours(seq_names, spair, sring, score, True))
    depth = wx_ref.shape[0]

    def wide_view(ref):
        return lambda pair, ring, core, piece: ref.at[pl.ds(((pair * 4 + ring) * 2 + core) * depth + piece.start, piece.size), :]

    hidden = Gather(lambda pair, ring, core, piece: whole.at[pair * 4 + ring, piece], lambda piece: x_ref.at[piece], mp_names,
                    mpair, mring, 0, ms, mr, 0, cut(x_ref.shape[0], 2), False)
    small = Gather(wide_view(wba_ref), lambda piece: wb_ref.at[piece], seq_names, spair, sring, score, bs, br, 0, cut(depth, 2), True)
    big = Gather(wide_view(wxa_ref), lambda piece: wx_ref.at[piece], seq_names, spair, sring, score, xs, xr, 0, cut(depth, 2), True)
    here = (spair * 4 + sring) * 2 + score
    mine = [pltpu.make_async_copy(x_ref, whole.at[mpair * 4 + mring], local.at[0]),
            pltpu.make_async_copy(wx_ref, wxa_ref.at[pl.ds(here * depth, depth), :], local.at[1]),
            pltpu.make_async_copy(wb_ref, wba_ref.at[pl.ds(here * depth, depth), :], local.at[2])]
    everything = (hidden, small, big)
    for g in everything:
        g.begin()
    for copy in mine:
        copy.start()
    for k in range(2):
        for g in (small, hidden, big):
            g.second(k)
    for which in range(2):
        for k in range(2):
            for g in (small, hidden, big):
                g.forward(which, k)
    hidden.last()
    mine[0].wait()
    write_normed(whole, gain_ref, normed_ref)
    small.last()
    big.last()
    for g in everything:
        g.finish()
    for copy in mine[1:]:
        copy.wait()


def run_first(x, wx, wb, gain, cid):
    n, w = x.shape
    depth = wx.shape[0]
    D = pltpu.SemaphoreType.DMA
    few, many = copies_of(2, False), copies_of(2, True)
    bf = jnp.bfloat16
    return pl.pallas_call(
        first_kernel,
        out_shape=(jax.ShapeDtypeStruct((n, 8 * w), bf), jax.ShapeDtypeStruct((16 * depth, wx.shape[1]), bf),
                   jax.ShapeDtypeStruct((16 * depth, wb.shape[1]), bf)),
        in_specs=[VM] * 4, out_specs=(VM,) * 3,
        scratch_shapes=[pltpu.VMEM((8, n, w), bf), D((3,)), D((few,)), D((few,)), D((many,)), D((many,)), D((many,)), D((many,))],
        compiler_params=pltpu.CompilerParams(collective_id=cid, has_side_effects=True, vmem_limit_bytes=40 << 20),
    )(x, wx, wb, gain)


def norm_kernel(x_ref, gain_ref, normed_ref, whole, local, ms, mr):
    pair, ring = mp_place()
    greet(neighbours(mp_names, pair, ring, 0, False))
    hidden = Gather(lambda pair, ring, core, piece: whole.at[pair * 4 + ring, piece], lambda piece: x_ref.at[piece], mp_names,
                    pair, ring, 0, ms, mr, 0, cut(x_ref.shape[0], 4), False)
    mine = pltpu.make_async_copy(x_ref, whole.at[pair * 4 + ring], local)
    hidden.begin()
    mine.start()
    for k in range(4):
        hidden.second(k)
    for which in range(2):
        for k in range(4):
            hidden.forward(which, k)
    hidden.last()
    hidden.finish()
    mine.wait()
    write_normed(whole, gain_ref, normed_ref)


def run_norm(x, gain, cid):
    n, w = x.shape
    D = pltpu.SemaphoreType.DMA
    few = copies_of(4, False)
    return pl.pallas_call(
        norm_kernel,
        out_shape=jax.ShapeDtypeStruct((n, 8 * w), x.dtype),
        in_specs=[VM, VM], out_specs=VM,
        scratch_shapes=[pltpu.VMEM((8, n, w), x.dtype), D, D((few,)), D((few,))],
        compiler_params=pltpu.CompilerParams(collective_id=cid, has_side_effects=True, vmem_limit_bytes=24 << 20),
    )(x, gain)


def reduce_kernel(p_ref, out_ref, tmp, d1, d2, ysrc, ydst, s1, r1, s2, r2, sy, ry, sraw, rraw):
    high, low = mp_place()
    right, left = (low + 1) % 4, (low + 3) % 4
    far = (low + 2) % 4
    partner = (1 - high) * 4 + low
    greet(neighbours(mp_names, high, low, 0, False))
    n = p_ref.shape[1]
    half = n // 2
    order = (1 - high, high)
    sides = ((right, left), (left, right))

    def send(src, dst, target, ssem, rsem):
        copy = pltpu.make_async_remote_copy(src_ref=src, dst_ref=dst, send_sem=ssem, recv_sem=rsem,
                                            device_id={"mp": target}, device_id_type=MESH)
        copy.start()
        return copy

    first = [[send(p_ref.at[order[k] * 4 + far, rows(d * half, half)], d1.at[k, d], high * 4 + sides[d][0],
                   s1.at[k, d], r1.at[k, d]) for d in range(2)] for k in range(2)]
    raw = [[send(p_ref.at[order[k] * 4 + sides[d][0], rows((1 - d) * half, half)],
                 d2.at[k, d, rows((1 - d) * half, half)], high * 4 + sides[d][0],
                 sraw.at[k, d], rraw.at[k, d]) for d in range(2)] for k in range(2)]
    second = []
    for k in range(2):
        for d in range(2):
            first[k][d].wait_recv()
            tmp[k, d] = (d1[k, d].astype(jnp.float32)
                         + p_ref[order[k] * 4 + sides[d][0], d * half:(d + 1) * half].astype(jnp.float32)).astype(tmp.dtype)
            second.append(send(tmp.at[k, d], d2.at[k, d, rows(d * half, half)], high * 4 + sides[d][0],
                               s2.at[k, d], r2.at[k, d]))
    totals = None
    for k in range(2):
        for d in range(2):
            raw[k][d].wait_recv()
            second[k * 2 + d].wait_recv()
        total = (p_ref[order[k] * 4 + low].astype(jnp.float32) + d2[k, 0].astype(jnp.float32)
                 + d2[k, 1].astype(jnp.float32))
        if k == 0:
            ysrc[...] = total.astype(ysrc.dtype)
            ycopy = send(ysrc, ydst, partner, sy, ry)
        else:
            ycopy.wait_recv()
            out_ref[...] = total + ydst[...].astype(jnp.float32)
    ycopy.wait_send()
    for k in range(2):
        for d in range(2):
            first[k][d].wait_send()
            raw[k][d].wait_send()
            second[k * 2 + d].wait_send()


def mp_reduce(p, cid):
    _, n, w = p.shape
    D = pltpu.SemaphoreType.DMA
    half = n // 2
    return pl.pallas_call(
        reduce_kernel,
        out_shape=jax.ShapeDtypeStruct((n, w), jnp.float32),
        in_specs=[VM], out_specs=VM,
        scratch_shapes=[pltpu.VMEM((2, 2, half, w), p.dtype), pltpu.VMEM((2, 2, half, w), p.dtype),
                        pltpu.VMEM((2, 2, n, w), p.dtype), pltpu.VMEM((n, w), p.dtype), pltpu.VMEM((n, w), p.dtype),
                        D((2, 2)), D((2, 2)), D((2, 2)), D((2, 2)), D, D, D((2, 2)), D((2, 2))],
        compiler_params=pltpu.CompilerParams(collective_id=cid, has_side_effects=True, vmem_limit_bytes=32 << 20),
    )(p)


def ssd_kernel(xp_ref, bcd_ref, rimx_ref, rimbc_ref, cx_ref, cbc_ref, bias_ref, rate_ref, skip_ref,
               y_ref, cc_ref, cum_ref, send_ref, padx, padbc, state):
    n = xp_ref.shape[0]
    count = n // QB
    padx[pl.ds(0, 8), :] = rimx_ref[...]
    padbc[pl.ds(0, 8), :] = rimbc_ref[...]
    padx[pl.ds(8, n), :] = xp_ref[...]
    padbc[pl.ds(8, n), :] = bcd_ref[:, 0:2 * N]
    state[...] = jnp.zeros_like(state)
    row = lax.broadcasted_iota(jnp.int32, (QB, QB), 0)
    col = lax.broadcasted_iota(jnp.int32, (QB, QB), 1)
    causal = row >= col
    tri = jnp.where(causal, 1.0, 0.0).astype(jnp.float32)
    low = col < P_SIZE
    bf = jnp.bfloat16

    def silu(v):
        return v / (1.0 + jnp.exp(-v))

    def conv(pad, taps, start, lanes):
        whole = pad[pl.ds(start, QB + 8), lanes]
        total = taps[0:1, lanes] * whole[5:5 + QB]
        for j in range(1, 4):
            total = total + taps[j:j + 1, lanes] * whole[5 + j:5 + j + QB]
        return silu(total)

    def one(c, before):
        start = pl.multiple_of(c * QB, QB)
        here = pl.ds(start, QB)
        bv = conv(padbc, cbc_ref, start, slice(0, N))
        cv = conv(padbc, cbc_ref, start, slice(N, 2 * N)).astype(bf)
        cc_ref[here, :] = cv
        raw = bcd_ref[here, 2 * N:3 * N] + bias_ref[...]
        step = jnp.maximum(raw, 0.0) + jnp.log1p(jnp.exp(-jnp.abs(raw)))
        decay = -rate_ref[...] * step
        cum = jnp.dot(tri, decay, precision=lax.Precision.HIGHEST, preferred_element_type=jnp.float32)
        cum_ref[here, :] = cum + before
        cum_t, step_t = cum.T, step.T
        last = cum[QB - 1:QB, :]
        bt = bv.T.astype(bf)
        affinity = jnp.dot(cv, bt, preferred_element_type=jnp.float32)
        for p in range(xp_ref.shape[1] // 128):
            lanes = slice(p * 128, (p + 1) * 128)
            xv = conv(padx, cx_ref, start, lanes)
            mixes, grown, tails, ends = [], [], [], []
            for h in (2 * p, 2 * p + 1):
                ct = jnp.broadcast_to(cum[:, h:h + 1], (QB, QB))
                st = jnp.broadcast_to(step[:, h:h + 1], (QB, QB))
                end = jnp.broadcast_to(last[:, h:h + 1], (1, QB))
                spread = jnp.where(causal, ct - cum_t[h:h + 1, :], -jnp.inf)
                mixes.append((affinity * jnp.exp(spread) * step_t[h:h + 1, :]).astype(bf))
                grown.append(ct)
                tails.append(jnp.exp(end - ct) * st)
                ends.append(end)
            lowhalf = low[0:1]
            mixed = jnp.concatenate(mixes, axis=1)
            xs = jnp.concatenate([jnp.where(low, xv, 0.0).astype(bf), jnp.where(low, 0.0, xv).astype(bf)], axis=0)
            out = jnp.dot(mixed, xs, preferred_element_type=jnp.float32)
            old = state[:, lanes]
            carried = jnp.dot(cv, old.astype(bf), preferred_element_type=jnp.float32)
            out = out + jnp.exp(jnp.where(low, grown[0], grown[1])) * carried
            y_ref[here, lanes] = out + skip_ref[0:1, lanes] * xv
            weighted = (xv * jnp.where(low, tails[0], tails[1])).astype(bf)
            fresh = jnp.dot(bt, weighted, preferred_element_type=jnp.float32)
            state[:, lanes] = jnp.exp(jnp.where(lowhalf, ends[0], ends[1])) * old + fresh
        return before + last

    total = lax.fori_loop(0, count, one, jnp.zeros((1, 128), jnp.float32))
    send_ref[0:N, :] = state[...].astype(bf)
    for p in range(xp_ref.shape[1] // 128):
        lanes = slice(p * 128, (p + 1) * 128)
        ends = [jnp.broadcast_to(total[:, h:h + 1], (16, 128)) for h in (2 * p, 2 * p + 1)]
        decay = jnp.exp(jnp.where(low[0:16], ends[0], ends[1]))
        big = decay.astype(bf)
        rest = decay - big.astype(jnp.float32)
        middle = rest.astype(bf)
        small = (rest - middle.astype(jnp.float32)).astype(bf)
        which = row[0:16]
        send_ref[N:N + 16, lanes] = jnp.where(which == 0, big.astype(jnp.float32), jnp.where(
            which == 1, middle.astype(jnp.float32), small.astype(jnp.float32))).astype(bf)


def run_ssd(xp, bcd, rimx, rimbc, conv_x, conv_bc, bias, rate, skip):
    n, width = xp.shape
    f32, bf = jnp.float32, jnp.bfloat16
    return pl.pallas_call(
        ssd_kernel,
        out_shape=(jax.ShapeDtypeStruct((n, width), f32), jax.ShapeDtypeStruct((n, N), bf),
                   jax.ShapeDtypeStruct((n, 128), f32), jax.ShapeDtypeStruct((N + 16, width), bf)),
        in_specs=[VM] * 9, out_specs=(VM,) * 4,
        scratch_shapes=[pltpu.VMEM((n + 8, width), f32), pltpu.VMEM((n + 8, 2 * N), f32), pltpu.VMEM((N, width), f32)],
        compiler_params=pltpu.CompilerParams(vmem_limit_bytes=32 << 20),
        cost_estimate=pl.CostEstimate(flops=4_000_000_000, bytes_accessed=8 << 20, transcendentals=0),
    )(xp, bcd, rimx, rimbc, conv_x, conv_bc, bias, rate, skip)


def gate_kernel(normed_ref, wz_ref, send_ref, y_ref, cc_ref, cum_ref, gain_ref, out_ref, states, incoming, gate, local, ss, sr):
    place = lax.axis_index("seq")
    pair, ring, core = seq_place()
    greet(neighbours(seq_names, pair, ring, core, True))
    n, width = y_ref.shape
    bf, f32 = jnp.bfloat16, jnp.float32
    tall = send_ref.shape[0]
    every = Gather(lambda pair, ring, core, piece: states.at[(pair * 4 + ring) * 2 + core, piece], lambda piece: send_ref.at[piece],
                   seq_names, pair, ring, core, ss, sr, 0, [pl.ds(0, 80), pl.ds(80, tall - 80)], True)
    mine = pltpu.make_async_copy(send_ref, states.at[place], local)
    every.begin()
    mine.start()

    def matmul(part):
        lanes = slice(part * 128, (part + 1) * 128)
        gate[:, lanes] = jnp.dot(normed_ref[...], wz_ref[:, lanes], preferred_element_type=f32)

    matmul(0)
    matmul(1)
    every.second(0)
    every.second(1)
    matmul(2)
    every.forward(0, 0)
    every.forward(0, 1)
    matmul(3)
    matmul(4)
    every.forward(1, 0)
    every.forward(1, 1)
    matmul(5)
    matmul(6)
    matmul(7)
    every.last()
    every.finish()
    mine.wait()
    incoming[...] = jnp.zeros_like(incoming)

    def add(k, _):
        tail = states[k, N:N + 16, :].astype(f32)
        decay = tail[0:1] + (tail[1:2] + tail[2:3])
        incoming[...] = decay * incoming[...] + states[k, 0:N, :].astype(f32)
        return 0

    lax.fori_loop(0, place, add, 0)
    low = lax.broadcasted_iota(jnp.int32, (QB, 128), 1) < P_SIZE

    def one(c, _):
        here = pl.ds(pl.multiple_of(c * QB, QB), QB)
        cv = cc_ref[here, :]
        cum = cum_ref[here, :]
        square = jnp.zeros((QB, 128), f32)
        for p in range(width // 128):
            lanes = slice(p * 128, (p + 1) * 128)
            ct = jnp.where(low, jnp.broadcast_to(cum[:, 2 * p:2 * p + 1], (QB, 128)),
                           jnp.broadcast_to(cum[:, 2 * p + 1:2 * p + 2], (QB, 128)))
            carried = jnp.dot(cv, incoming[:, lanes].astype(bf), preferred_element_type=f32)
            g = gate[here, lanes]
            value = (y_ref[here, lanes] + jnp.exp(ct) * carried) * (g / (1.0 + jnp.exp(-g)))
            gate[here, lanes] = value
            square = square + value * value
        scale = lax.rsqrt(jnp.sum(square, axis=1, keepdims=True) / width + 1e-05)
        out_ref[here, :] = (gate[here, :] * scale * gain_ref[...]).astype(bf)
        return 0

    lax.fori_loop(0, n // QB, one, 0)


def run_gate(normed, wz, send, y, cc, cum, gain, cid):
    n, width = y.shape
    D = pltpu.SemaphoreType.DMA
    many = copies_of(2, True)
    return pl.pallas_call(
        gate_kernel,
        out_shape=jax.ShapeDtypeStruct((n, width), jnp.bfloat16),
        in_specs=[VM] * 7, out_specs=VM,
        scratch_shapes=[pltpu.VMEM((16,) + send.shape, jnp.bfloat16), pltpu.VMEM((N, width), jnp.float32),
                        pltpu.VMEM((n, width), jnp.float32), D, D((many,)), D((many,))],
        compiler_params=pltpu.CompilerParams(collective_id=cid, has_side_effects=True, vmem_limit_bytes=40 << 20),
    )(normed, wz, send, y, cc, cum, gain)


def out_kernel(y_ref, w_ref, out_ref):
    out_ref[0] = jnp.dot(y_ref[...], w_ref[0], preferred_element_type=jnp.float32).astype(out_ref.dtype)


def run_out(y, w):
    n, width = y.shape
    cols = w.shape[2]
    return pl.pallas_call(
        out_kernel,
        out_shape=jax.ShapeDtypeStruct((8, n, 2 * cols), jnp.bfloat16),
        grid=(w.shape[0],),
        in_specs=[pl.BlockSpec((n, width), lambda j: (0, 0)), pl.BlockSpec((1, width, cols), lambda j: (j, 0, 0))],
        out_specs=pl.BlockSpec((1, n, cols), lambda j: (j // 2, 0, j % 2)),
        compiler_params=pltpu.CompilerParams(vmem_limit_bytes=16 << 20),
        cost_estimate=pl.CostEstimate(flops=2 * n * width * 4096, bytes_accessed=16 << 20, transcendentals=0),
    )(y, w)


def attention_kernel(x_ref, wq_ref, wk_ref, wv_ref, out_ref, own, kv, q, peak, total, local, ss, sr):
    place = lax.axis_index("seq")
    pair, ring, core = seq_place()
    greet(neighbours(seq_names, pair, ring, core, True))
    n = x_ref.shape[0]
    heads = q.shape[0]
    bf, f32 = jnp.bfloat16, jnp.float32
    scale = HD ** -0.5 * 1.4426950408889634
    own[:, 0:HD] = jnp.dot(x_ref[...], wk_ref[...], preferred_element_type=f32).astype(bf)
    own[:, HD:2 * HD] = jnp.dot(x_ref[...], wv_ref[...], preferred_element_type=f32).astype(bf)
    every = Gather(lambda pair, ring, core, piece: kv.at[(pair * 4 + ring) * 2 + core, piece], lambda piece: own.at[piece],
                   seq_names, pair, ring, core, ss, sr, 0, cut(n, 2), True)
    every.begin()
    for h in range(heads):
        q[h] = jnp.dot(x_ref[...], wq_ref[:, h * HD:(h + 1) * HD], preferred_element_type=f32).astype(bf)
    peak[...] = jnp.full_like(peak, -1e30)
    total[...] = jnp.zeros_like(total)

    def work(block, edge):
        def head(h, _):
            keys = block[:, 0:HD]
            both = jnp.concatenate([block[:, HD:2 * HD], jnp.ones((n, HD), bf)], axis=1)
            if edge is not None:
                t = lax.broadcasted_iota(jnp.int32, (n, n), 0)
                s = lax.broadcasted_iota(jnp.int32, (n, n), 1)
                allowed = s > t if edge == 0 else s <= t
            scores = lax.dot_general(q[h], keys, (((1,), (1,)), ((), ())), preferred_element_type=f32) * scale
            if edge is not None:
                scores = jnp.where(allowed, scores, -1e30)
            old = peak[h]
            new = jnp.maximum(old, jnp.max(scores, axis=1, keepdims=True))
            weights = jnp.exp2(scores - new[:, 0:1])
            if edge == 0:
                weights = jnp.where(allowed, weights, 0.0)
            shrink = jnp.exp2(old - new)
            peak[h] = new
            total[h] = jnp.concatenate([shrink, shrink], axis=1) * total[h] + jnp.dot(
                weights.astype(bf), both, preferred_element_type=f32)
            return 0

        lax.fori_loop(0, heads, head, 0)

    def visit(first, count, chip):
        def one(j, _):
            other_pair, other_ring = chip(j // 2)
            which = (other_pair * 4 + other_ring) * 2 + j % 2
            away = place - which

            @pl.when((away >= 1) & (away < WINDOW // n))
            def _():
                work(kv.at[which], None)
            return 0

        lax.fori_loop(first, count, one, 0)

    work(own, 1)
    every.second(0)
    every.second(1)

    @pl.when(pair == 1)
    def _():
        work(kv.at[ring * 2 + core], 0)

    every.forward(0, 0)
    every.forward(0, 1)
    for copy in every.across[0:4]:
        copy.wait_recv()
    mine = pltpu.make_async_copy(own, kv.at[place], local)
    mine.start()
    mine.wait()
    visit(0, 4, lambda g: (jnp.where(g == 0, pair, 1 - pair), ring))
    every.forward(1, 0)
    every.forward(1, 1)
    for copy in every.across[4:12]:
        copy.wait_recv()
    visit(0, 8, lambda g: (jnp.where(g < 2, pair, 1 - pair), (ring + 1 + 2 * (g % 2)) % 4))
    every.last()
    for copy in every.across[12:]:
        copy.wait_recv()
    visit(0, 4, lambda g: (jnp.where(g == 0, pair, 1 - pair), (ring + 2) % 4))
    for copy in every.started:
        copy.wait_send()
    for h in range(heads):
        out_ref[:, h * HD:(h + 1) * HD] = total[h, :, 0:HD] / total[h, :, HD:2 * HD]


def run_attention(x, wq, wk, wv, cid):
    n = x.shape[0]
    width = wq.shape[1]
    heads = width // HD
    D = pltpu.SemaphoreType.DMA
    many = copies_of(2, True)
    bf, f32 = jnp.bfloat16, jnp.float32
    return pl.pallas_call(
        attention_kernel,
        out_shape=jax.ShapeDtypeStruct((n, width), f32),
        in_specs=[VM] * 4, out_specs=VM,
        scratch_shapes=[pltpu.VMEM((n, 2 * HD), bf), pltpu.VMEM((16, n, 2 * HD), bf), pltpu.VMEM((heads, n, HD), bf),
                        pltpu.VMEM((heads, n, HD), f32), pltpu.VMEM((heads, n, 2 * HD), f32), D, D((many,)), D((many,))],
        compiler_params=pltpu.CompilerParams(collective_id=cid, has_side_effects=True, vmem_limit_bytes=40 << 20),
    )(x, wq, wk, wv)


def padded(vector):
    return jnp.pad(vector, (0, 128 - vector.shape[0]))[None, :]


def on_device(hidden_in, norm_gain, w_z, w_x, w_b, w_c, w_dt, conv_x, conv_b, conv_c, dt_bias, a_rate,
              skip_gain, group_gain, w_out, attn_gain, w_q, w_k, w_v):
    f32, bf = jnp.float32, jnp.bfloat16
    n = hidden_in.shape[0]
    w_bcd = jnp.concatenate([w_b, w_c, jnp.pad(w_dt, ((0, 0), (0, 128 - w_dt.shape[1])))], axis=1)
    w_z_all = lax.all_gather(w_z, "seq", axis=0, tiled=True)
    w_out_all = lax.all_gather(w_out, "seq")
    normed, w_x_all, w_bcd_all = run_first(hidden_in, w_x, w_bcd, norm_gain[None, :], 0)
    bcd = jnp.dot(normed, w_bcd_all, preferred_element_type=f32)
    xp = jnp.dot(normed, w_x_all, preferred_element_type=f32)
    route = [(i, i + 1) for i in range(lax.axis_size("seq") - 1)]
    rims = lax.ppermute(jnp.concatenate([xp[n - 8:], bcd[n - 8:, 0:2 * N]], axis=1), "seq", route)
    width = xp.shape[1]
    y, cc, cum, send = run_ssd(
        xp, bcd, rims[:, 0:width], rims[:, width:], conv_x, jnp.concatenate([conv_b, conv_c], axis=1),
        padded(dt_bias), padded(a_rate), jnp.repeat(skip_gain, P_SIZE)[None, :])
    y_normed = run_gate(normed, w_z_all, send, y, cc, cum, group_gain[None, :], 3)
    parts = run_out(y_normed, w_out_all)
    mixed = hidden_in.astype(f32) + mp_reduce(parts, 1)
    normed_two = run_norm(mixed.astype(bf), attn_gain[None, :], 2)
    return (mixed, run_attention(normed_two, w_q, w_k, w_v, 4))


def solution(mesh):
    tile, cols = P("seq", "mp"), P(None, "mp")
    placed = (tile, P(), tile, tile, tile, tile, tile, cols, cols, cols, P("mp"), P("mp"), P("mp"), P("mp"),
              P("mp", "seq"), P(), cols, cols, cols)
    return jax.shard_map(on_device, mesh=mesh, in_specs=placed, out_specs=(tile, tile), check_vma=False)
```

```python
import jax
import jax.numpy as jnp
from jax import lax
from jax.experimental import pallas as pl
from jax.experimental.pallas import tpu as pltpu
from jax.sharding import PartitionSpec as P

MESH = pl.DeviceIdType.MESH
VM = pl.BlockSpec(memory_space=pltpu.VMEM)
P_SIZE = 64
N = 128
HD = 128
WINDOW = 4096
QB = 128


def rows(start, size):
    return pl.ds(start, size)


class Gather:
    def __init__(self, view, own, names, pair, ring, core, sends, recvs, base, pieces, fan):
        self.view, self.own, self.names = view, own, names
        self.pair, self.ring, self.core = pair, ring, core
        self.sends, self.recvs, self.next, self.pieces, self.fan = sends, recvs, base, pieces, fan
        self.right, self.left, self.far = (ring + 1) % 4, (ring + 3) % 4, (ring + 2) % 4
        self.started, self.across = [], []
        self.y, self.a, self.b, self.f = {}, {}, {}, []

    def send(self, src, block, piece, pair, ring, core):
        copy = pltpu.make_async_remote_copy(
            src_ref=src, dst_ref=self.view(*block, piece), send_sem=self.sends.at[self.next], recv_sem=self.recvs.at[self.next],
            device_id=self.names(pair, ring, core), device_id_type=MESH)
        self.next += 1
        copy.start()
        self.started.append(copy)
        return copy

    def over(self, src, block, piece):
        if self.fan:
            self.across.append(self.send(src, block, piece, self.pair, self.ring, 1 - self.core))

    def begin(self):
        me = (self.pair, self.ring, self.core)
        for k, piece in enumerate(self.pieces):
            src = self.own(piece)
            self.y[k] = self.send(src, me, piece, 1 - self.pair, self.ring, self.core)
            self.a[k] = [self.send(src, me, piece, self.pair, to, self.core) for to in (self.right, self.left)]
            self.over(src, me, piece)

    def second(self, k):
        piece, block = self.pieces[k], (1 - self.pair, self.ring, self.core)
        self.y[k].wait_recv()
        src = self.view(*block, piece)
        self.b[k] = [self.send(src, block, piece, self.pair, to, self.core) for to in (self.right, self.left)]
        self.over(src, block, piece)

    def forward(self, which, k):
        pair = self.pair if which == 0 else 1 - self.pair
        piece, first = self.pieces[k], k < len(self.pieces) // 2
        for d, (to, origin) in enumerate(((self.right, self.left), (self.left, self.right))):
            (self.a, self.b)[which][k][d].wait_recv()
            block = (pair, origin, self.core)
            src = self.view(*block, piece)
            if first == (d == 0):
                self.f.append((self.send(src, block, piece, self.pair, to, self.core), (pair, self.far, self.core), piece))
            self.over(src, block, piece)

    def last(self):
        for copy, block, piece in self.f:
            copy.wait_recv()
            self.over(self.view(*block, piece), block, piece)

    def finish(self):
        for copy in self.across:
            copy.wait_recv()
        for copy in self.started:
            copy.wait_send()


def copies_of(pieces, fan):
    return pieces * (7 + (8 if fan else 0))


def seq_names(pair, ring, core):
    return {"seq": (pair * 4 + ring) * 2 + core}


def mp_names(pair, ring, core):
    return {"mp": pair * 4 + ring}


def greet(ids):
    barrier = pltpu.get_barrier_semaphore()
    for other in ids:
        pl.semaphore_signal(barrier, inc=1, device_id=other, device_id_type=MESH)
    pl.semaphore_wait(barrier, len(ids))


def seq_place():
    me = lax.axis_index("seq")
    return me // 8, (me // 2) % 4, me % 2


def mp_place():
    me = lax.axis_index("mp")
    return me // 4, me % 4


def neighbours(names, pair, ring, core, fan):
    ids = [names(1 - pair, ring, core), names(pair, (ring + 1) % 4, core), names(pair, (ring + 3) % 4, core)]
    return ids + ([names(pair, ring, 1 - core)] if fan else [])


def cut(total, count):
    return [pl.ds(k * (total // count), total // count) for k in range(count)]


def write_normed(whole, gain_ref, normed_ref, start, count):
    blocks, _, wide = whole.shape

    def norm(c, _):
        piece = rows(pl.multiple_of(start + c * 32, 32), 32)
        square = jnp.zeros((32, wide), jnp.float32)
        for b in range(blocks):
            value = whole[b, piece, :].astype(jnp.float32)
            square = square + value * value
        scale = lax.rsqrt(jnp.sum(square, axis=1, keepdims=True) / (blocks * wide) + 1e-05)
        for b in range(blocks):
            lanes = slice(b * wide, (b + 1) * wide)
            normed_ref[piece, lanes] = (whole[b, piece, :].astype(jnp.float32) * scale * gain_ref[:, lanes]).astype(normed_ref.dtype)
        return 0

    lax.fori_loop(0, count // 32, norm, 0)


def first_kernel(x_ref, wx_ref, wb_ref, gain_ref, normed_ref, wxa_ref, wba_ref, whole, local, ms, mr, bs, br, xs, xr):
    mpair, mring = mp_place()
    spair, sring, score = seq_place()
    greet(neighbours(mp_names, mpair, mring, 0, False) + neighbours(seq_names, spair, sring, score, True))
    depth = wx_ref.shape[0]

    def wide_view(ref):
        return lambda pair, ring, core, piece: ref.at[pl.ds(((pair * 4 + ring) * 2 + core) * depth + piece.start, piece.size), :]

    hidden = Gather(lambda pair, ring, core, piece: whole.at[pair * 4 + ring, piece], lambda piece: x_ref.at[piece], mp_names,
                    mpair, mring, 0, ms, mr, 0, cut(x_ref.shape[0], 2), False)
    small = Gather(wide_view(wba_ref), lambda piece: wb_ref.at[piece], seq_names, spair, sring, score, bs, br, 0, cut(depth, 2), True)
    big = Gather(wide_view(wxa_ref), lambda piece: wx_ref.at[piece], seq_names, spair, sring, score, xs, xr, 0, cut(depth, 2), True)
    here = (spair * 4 + sring) * 2 + score
    mine = [pltpu.make_async_copy(x_ref, whole.at[mpair * 4 + mring], local.at[0]),
            pltpu.make_async_copy(wx_ref, wxa_ref.at[pl.ds(here * depth, depth), :], local.at[1]),
            pltpu.make_async_copy(wb_ref, wba_ref.at[pl.ds(here * depth, depth), :], local.at[2])]
    everything = (hidden, small, big)
    for g in everything:
        g.begin()
    for copy in mine:
        copy.start()
    for k in range(2):
        for g in (small, hidden, big):
            g.second(k)
    for which in range(2):
        for k in range(2):
            for g in (small, hidden, big):
                g.forward(which, k)
    hidden.last()
    mine[0].wait()
    write_normed(whole, gain_ref, normed_ref, 0, whole.shape[1])
    small.last()
    big.last()
    for g in everything:
        g.finish()
    for copy in mine[1:]:
        copy.wait()


def run_first(x, wx, wb, gain, cid):
    n, w = x.shape
    depth = wx.shape[0]
    D = pltpu.SemaphoreType.DMA
    few, many = copies_of(2, False), copies_of(2, True)
    bf = jnp.bfloat16
    return pl.pallas_call(
        first_kernel,
        out_shape=(jax.ShapeDtypeStruct((n, 8 * w), bf), jax.ShapeDtypeStruct((16 * depth, wx.shape[1]), bf),
                   jax.ShapeDtypeStruct((16 * depth, wb.shape[1]), bf)),
        in_specs=[VM] * 4, out_specs=(VM,) * 3,
        scratch_shapes=[pltpu.VMEM((8, n, w), bf), D((3,)), D((few,)), D((few,)), D((many,)), D((many,)), D((many,)), D((many,))],
        compiler_params=pltpu.CompilerParams(collective_id=cid, has_side_effects=True, vmem_limit_bytes=40 << 20),
    )(x, wx, wb, gain)


def mix_kernel(y_ref, w_hbm, hidden_ref, gain_ref, mixed_ref, normed_ref, w, p, tmp, d1, d2, ysrc, ydst, whole, wsem,
               s1, r1, s2, r2, sraw, rraw, sy, ry, gs, gr):
    high, low = mp_place()
    right, left, far = (low + 1) % 4, (low + 3) % 4, (low + 2) % 4
    me = high * 4 + low
    order = (1 - high, high)
    sides = ((right, left), (left, right))
    n = y_ref.shape[0]
    half, quarter = n // 2, n // 4
    f32 = jnp.float32
    blocks = [pair * 4 + ring for ring in (far, right, left, low) for pair in order]
    loads = [pltpu.make_async_copy(w_hbm.at[pl.ds(2 * b, 2)], w.at[pl.ds(2 * b, 2)], wsem.at[i]) for i, b in enumerate(blocks)]
    for load in loads:
        load.start()
    greet(neighbours(mp_names, high, low, 0, False))

    def send(src, dst, pair, ring, ssem, rsem):
        copy = pltpu.make_async_remote_copy(src_ref=src, dst_ref=dst, send_sem=ssem, recv_sem=rsem,
                                            device_id=mp_names(pair, ring, 0), device_id_type=MESH)
        copy.start()
        sent.append(copy)
        return copy

    def product(h, b):
        here = slice(h * half, (h + 1) * half)
        cols = w.shape[2]
        for c in range(2):
            p[b, here, c * cols:(c + 1) * cols] = jnp.dot(
                y_ref[here, :], w[2 * b + c], preferred_element_type=f32).astype(p.dtype)

    def start_first(h, k):
        return [send(p.at[order[k] * 4 + far, rows(h * half + d * quarter, quarter)], d1.at[h, k, d], high, sides[d][0],
                     s1.at[h, k, d], r1.at[h, k, d]) for d in range(2)]

    def start_raw(h, k, d):
        return send(p.at[order[k] * 4 + sides[d][0], rows(h * half + (1 - d) * quarter, quarter)],
                    d2.at[h, k, d, rows((1 - d) * quarter, quarter)], high, sides[d][0], sraw.at[h, k, d], rraw.at[h, k, d])

    def pass_on(h, k):
        result = []
        for d in range(2):
            first[h][k][d].wait_recv()
            here = slice(h * half + d * quarter, h * half + (d + 1) * quarter)
            tmp[h, k, d] = (d1[h, k, d].astype(f32) + p[order[k] * 4 + sides[d][0], here, :].astype(f32)).astype(tmp.dtype)
            result.append(send(tmp.at[h, k, d], d2.at[h, k, d, rows(d * quarter, quarter)], high, sides[d][0],
                               s2.at[h, k, d], r2.at[h, k, d]))
        second[h][k] = result

    def total(h, k):
        for d in range(2):
            raw[h][k][d].wait_recv()
            second[h][k][d].wait_recv()
        here = slice(h * half, (h + 1) * half)
        return p[order[k] * 4 + low, here, :].astype(f32) + d2[h, k, 0].astype(f32) + d2[h, k, 1].astype(f32)

    def give(h):
        ysrc[h] = total(h, 0).astype(ysrc.dtype)
        across[h] = send(ysrc.at[h], ydst.at[h], 1 - high, low, sy.at[h], ry.at[h])

    def close(h):
        here = slice(h * half, (h + 1) * half)
        own = total(h, 1)
        across[h].wait_recv()
        result = hidden_ref[here, :].astype(f32) + (own + ydst[h].astype(f32))
        mixed_ref[here, :] = result
        whole[me, here, :] = result.astype(whole.dtype)
        gathers[h].begin()

    sent = []
    first, raw, second = [[None, None] for _ in range(2)], [[None, None] for _ in range(2)], [[None, None] for _ in range(2)]
    across = [None, None]

    def view(pair, ring, core, piece):
        return whole.at[pair * 4 + ring, piece]

    gathers = [Gather(view, lambda piece: whole.at[me, piece], mp_names, high, low, 0, gs, gr, h * copies_of(2, False),
                      [pl.ds(h * half, quarter), pl.ds(h * half + quarter, quarter)], False) for h in range(2)]
    for h in range(2):
        raw[h] = [[None, None], [None, None]]
        for i, b in enumerate(blocks):
            if h == 0:
                loads[i].wait()
            product(h, b)
            if h == 0 and i < 2:
                first[0][i] = start_first(0, i)
            if h == 0 and 2 <= i < 6:
                raw[0][i % 2][i // 2 - 1] = start_raw(0, i % 2, i // 2 - 1)
    pass_on(0, 0)
    pass_on(0, 1)
    for k in range(2):
        first[1][k] = start_first(1, k)
    for k in range(2):
        for d in range(2):
            raw[1][k][d] = start_raw(1, k, d)
    give(0)
    pass_on(1, 0)
    pass_on(1, 1)
    close(0)
    give(1)
    early, late = gathers
    early.second(0)
    early.second(1)
    early.forward(0, 0)
    early.forward(0, 1)
    close(1)
    early.forward(1, 0)
    early.forward(1, 1)
    late.second(0)
    late.second(1)
    late.forward(0, 0)
    late.forward(0, 1)
    early.last()
    late.forward(1, 0)
    late.forward(1, 1)
    write_normed(whole, gain_ref, normed_ref, 0, half)
    late.last()
    write_normed(whole, gain_ref, normed_ref, half, half)
    early.finish()
    late.finish()
    for copy in sent:
        copy.wait_send()


def run_mix(y, w, hidden, gain, cid):
    n, width = hidden.shape
    D = pltpu.SemaphoreType.DMA
    bf = jnp.bfloat16
    V = pltpu.VMEM
    few = 2 * copies_of(2, False)
    return pl.pallas_call(
        mix_kernel,
        out_shape=(jax.ShapeDtypeStruct((n, width), jnp.float32), jax.ShapeDtypeStruct((n, 8 * width), bf)),
        in_specs=[VM, pl.BlockSpec(memory_space=pl.ANY), VM, VM], out_specs=(VM, VM),
        scratch_shapes=[V(w.shape, bf), V((8, n, width), bf), V((2, 2, 2, n // 4, width), bf), V((2, 2, 2, n // 4, width), bf),
                        V((2, 2, 2, n // 2, width), bf), V((2, n // 2, width), bf), V((2, n // 2, width), bf), V((8, n, width), bf),
                        D((8,))] + [D((2, 2, 2))] * 6 + [D((2,))] * 2 + [D((few,))] * 2,
        compiler_params=pltpu.CompilerParams(collective_id=cid, has_side_effects=True, vmem_limit_bytes=48 << 20),
    )(y, w, hidden, gain)


def ssd_kernel(xp_ref, bcd_ref, rimx_ref, rimbc_ref, cx_ref, cbc_ref, bias_ref, rate_ref, skip_ref,
               y_ref, cc_ref, cum_ref, send_ref, padx, padbc, state):
    n = xp_ref.shape[0]
    count = n // QB
    padx[pl.ds(0, 8), :] = rimx_ref[...]
    padbc[pl.ds(0, 8), :] = rimbc_ref[...]
    padx[pl.ds(8, n), :] = xp_ref[...]
    padbc[pl.ds(8, n), :] = bcd_ref[:, 0:2 * N]
    state[...] = jnp.zeros_like(state)
    row = lax.broadcasted_iota(jnp.int32, (QB, QB), 0)
    col = lax.broadcasted_iota(jnp.int32, (QB, QB), 1)
    causal = row >= col
    tri = jnp.where(causal, 1.0, 0.0).astype(jnp.float32)
    low = col < P_SIZE
    bf = jnp.bfloat16

    def silu(v):
        return v / (1.0 + jnp.exp(-v))

    def conv(pad, taps, start, lanes):
        whole = pad[pl.ds(start, QB + 8), lanes]
        total = taps[0:1, lanes] * whole[5:5 + QB]
        for j in range(1, 4):
            total = total + taps[j:j + 1, lanes] * whole[5 + j:5 + j + QB]
        return silu(total)

    def one(c, before):
        start = pl.multiple_of(c * QB, QB)
        here = pl.ds(start, QB)
        bv = conv(padbc, cbc_ref, start, slice(0, N))
        cv = conv(padbc, cbc_ref, start, slice(N, 2 * N)).astype(bf)
        cc_ref[here, :] = cv
        raw = bcd_ref[here, 2 * N:3 * N] + bias_ref[...]
        step = jnp.maximum(raw, 0.0) + jnp.log1p(jnp.exp(-jnp.abs(raw)))
        decay = -rate_ref[...] * step
        cum = jnp.dot(tri, decay, precision=lax.Precision.HIGHEST, preferred_element_type=jnp.float32)
        cum_ref[here, :] = cum + before
        cum_t, step_t = cum.T, step.T
        last = cum[QB - 1:QB, :]
        bt = bv.T.astype(bf)
        affinity = jnp.dot(cv, bt, preferred_element_type=jnp.float32)
        for p in range(xp_ref.shape[1] // 128):
            lanes = slice(p * 128, (p + 1) * 128)
            xv = conv(padx, cx_ref, start, lanes)
            mixes, grown, tails, ends = [], [], [], []
            for h in (2 * p, 2 * p + 1):
                ct = jnp.broadcast_to(cum[:, h:h + 1], (QB, QB))
                st = jnp.broadcast_to(step[:, h:h + 1], (QB, QB))
                end = jnp.broadcast_to(last[:, h:h + 1], (1, QB))
                spread = jnp.where(causal, ct - cum_t[h:h + 1, :], -jnp.inf)
                mixes.append((affinity * jnp.exp(spread) * step_t[h:h + 1, :]).astype(bf))
                grown.append(ct)
                tails.append(jnp.exp(end - ct) * st)
                ends.append(end)
            lowhalf = low[0:1]
            mixed = jnp.concatenate(mixes, axis=1)
            xs = jnp.concatenate([jnp.where(low, xv, 0.0).astype(bf), jnp.where(low, 0.0, xv).astype(bf)], axis=0)
            out = jnp.dot(mixed, xs, preferred_element_type=jnp.float32)
            old = state[:, lanes]
            carried = jnp.dot(cv, old.astype(bf), preferred_element_type=jnp.float32)
            out = out + jnp.exp(jnp.where(low, grown[0], grown[1])) * carried
            y_ref[here, lanes] = out + skip_ref[0:1, lanes] * xv
            weighted = (xv * jnp.where(low, tails[0], tails[1])).astype(bf)
            fresh = jnp.dot(bt, weighted, preferred_element_type=jnp.float32)
            state[:, lanes] = jnp.exp(jnp.where(lowhalf, ends[0], ends[1])) * old + fresh
        return before + last

    total = lax.fori_loop(0, count, one, jnp.zeros((1, 128), jnp.float32))
    send_ref[0:N, :] = state[...].astype(bf)
    for p in range(xp_ref.shape[1] // 128):
        lanes = slice(p * 128, (p + 1) * 128)
        ends = [jnp.broadcast_to(total[:, h:h + 1], (16, 128)) for h in (2 * p, 2 * p + 1)]
        decay = jnp.exp(jnp.where(low[0:16], ends[0], ends[1]))
        big = decay.astype(bf)
        rest = decay - big.astype(jnp.float32)
        middle = rest.astype(bf)
        small = (rest - middle.astype(jnp.float32)).astype(bf)
        which = row[0:16]
        send_ref[N:N + 16, lanes] = jnp.where(which == 0, big.astype(jnp.float32), jnp.where(
            which == 1, middle.astype(jnp.float32), small.astype(jnp.float32))).astype(bf)


def run_ssd(xp, bcd, rimx, rimbc, conv_x, conv_bc, bias, rate, skip):
    n, width = xp.shape
    f32, bf = jnp.float32, jnp.bfloat16
    return pl.pallas_call(
        ssd_kernel,
        out_shape=(jax.ShapeDtypeStruct((n, width), f32), jax.ShapeDtypeStruct((n, N), bf),
                   jax.ShapeDtypeStruct((n, 128), f32), jax.ShapeDtypeStruct((N + 16, width), bf)),
        in_specs=[VM] * 9, out_specs=(VM,) * 4,
        scratch_shapes=[pltpu.VMEM((n + 8, width), f32), pltpu.VMEM((n + 8, 2 * N), f32), pltpu.VMEM((N, width), f32)],
        compiler_params=pltpu.CompilerParams(vmem_limit_bytes=32 << 20),
        cost_estimate=pl.CostEstimate(flops=4_000_000_000, bytes_accessed=8 << 20, transcendentals=0),
    )(xp, bcd, rimx, rimbc, conv_x, conv_bc, bias, rate, skip)


def gate_kernel(normed_ref, wz_ref, send_ref, y_ref, cc_ref, cum_ref, gain_ref, out_ref, states, incoming, gate, local, ss, sr):
    place = lax.axis_index("seq")
    pair, ring, core = seq_place()
    greet(neighbours(seq_names, pair, ring, core, True))
    n, width = y_ref.shape
    bf, f32 = jnp.bfloat16, jnp.float32
    tall = send_ref.shape[0]
    every = Gather(lambda pair, ring, core, piece: states.at[(pair * 4 + ring) * 2 + core, piece], lambda piece: send_ref.at[piece],
                   seq_names, pair, ring, core, ss, sr, 0, [pl.ds(0, 80), pl.ds(80, tall - 80)], True)
    mine = pltpu.make_async_copy(send_ref, states.at[place], local)
    every.begin()
    mine.start()

    def matmul(part):
        lanes = slice(part * 128, (part + 1) * 128)
        gate[:, lanes] = jnp.dot(normed_ref[...], wz_ref[:, lanes], preferred_element_type=f32)

    matmul(0)
    matmul(1)
    every.second(0)
    every.second(1)
    matmul(2)
    every.forward(0, 0)
    every.forward(0, 1)
    matmul(3)
    matmul(4)
    every.forward(1, 0)
    every.forward(1, 1)
    matmul(5)
    matmul(6)
    matmul(7)
    every.last()
    every.finish()
    mine.wait()
    incoming[...] = jnp.zeros_like(incoming)

    def add(k, _):
        tail = states[k, N:N + 16, :].astype(f32)
        decay = tail[0:1] + (tail[1:2] + tail[2:3])
        incoming[...] = decay * incoming[...] + states[k, 0:N, :].astype(f32)
        return 0

    lax.fori_loop(0, place, add, 0)
    low = lax.broadcasted_iota(jnp.int32, (QB, 128), 1) < P_SIZE

    def one(c, _):
        here = pl.ds(pl.multiple_of(c * QB, QB), QB)
        cv = cc_ref[here, :]
        cum = cum_ref[here, :]
        square = jnp.zeros((QB, 128), f32)
        for p in range(width // 128):
            lanes = slice(p * 128, (p + 1) * 128)
            ct = jnp.where(low, jnp.broadcast_to(cum[:, 2 * p:2 * p + 1], (QB, 128)),
                           jnp.broadcast_to(cum[:, 2 * p + 1:2 * p + 2], (QB, 128)))
            carried = jnp.dot(cv, incoming[:, lanes].astype(bf), preferred_element_type=f32)
            g = gate[here, lanes]
            value = (y_ref[here, lanes] + jnp.exp(ct) * carried) * (g / (1.0 + jnp.exp(-g)))
            gate[here, lanes] = value
            square = square + value * value
        scale = lax.rsqrt(jnp.sum(square, axis=1, keepdims=True) / width + 1e-05)
        out_ref[here, :] = (gate[here, :] * scale * gain_ref[...]).astype(bf)
        return 0

    lax.fori_loop(0, n // QB, one, 0)


def run_gate(normed, wz, send, y, cc, cum, gain, cid):
    n, width = y.shape
    D = pltpu.SemaphoreType.DMA
    many = copies_of(2, True)
    return pl.pallas_call(
        gate_kernel,
        out_shape=jax.ShapeDtypeStruct((n, width), jnp.bfloat16),
        in_specs=[VM] * 7, out_specs=VM,
        scratch_shapes=[pltpu.VMEM((16,) + send.shape, jnp.bfloat16), pltpu.VMEM((N, width), jnp.float32),
                        pltpu.VMEM((n, width), jnp.float32), D, D((many,)), D((many,))],
        compiler_params=pltpu.CompilerParams(collective_id=cid, has_side_effects=True, vmem_limit_bytes=40 << 20),
    )(normed, wz, send, y, cc, cum, gain)


def attention_kernel(x_ref, wq_ref, wk_ref, wv_ref, out_ref, own, kv, q, peak, total, local, ss, sr):
    place = lax.axis_index("seq")
    pair, ring, core = seq_place()
    greet(neighbours(seq_names, pair, ring, core, True))
    n = x_ref.shape[0]
    heads = q.shape[0]
    bf, f32 = jnp.bfloat16, jnp.float32
    scale = HD ** -0.5 * 1.4426950408889634
    own[:, 0:HD] = jnp.dot(x_ref[...], wk_ref[...], preferred_element_type=f32).astype(bf)
    own[:, HD:2 * HD] = jnp.dot(x_ref[...], wv_ref[...], preferred_element_type=f32).astype(bf)
    every = Gather(lambda pair, ring, core, piece: kv.at[(pair * 4 + ring) * 2 + core, piece], lambda piece: own.at[piece],
                   seq_names, pair, ring, core, ss, sr, 0, cut(n, 2), True)
    every.begin()
    for h in range(heads):
        q[h] = jnp.dot(x_ref[...], wq_ref[:, h * HD:(h + 1) * HD], preferred_element_type=f32).astype(bf)
    peak[...] = jnp.full_like(peak, -1e30)
    total[...] = jnp.zeros_like(total)

    def work(block, edge):
        def head(h, _):
            keys = block[:, 0:HD]
            both = jnp.concatenate([block[:, HD:2 * HD], jnp.ones((n, HD), bf)], axis=1)
            if edge is not None:
                t = lax.broadcasted_iota(jnp.int32, (n, n), 0)
                s = lax.broadcasted_iota(jnp.int32, (n, n), 1)
                allowed = s > t if edge == 0 else s <= t
            scores = lax.dot_general(q[h], keys, (((1,), (1,)), ((), ())), preferred_element_type=f32) * scale
            if edge is not None:
                scores = jnp.where(allowed, scores, -1e30)
            old = peak[h]
            new = jnp.maximum(old, jnp.max(scores, axis=1, keepdims=True))
            weights = jnp.exp2(scores - new[:, 0:1])
            if edge == 0:
                weights = jnp.where(allowed, weights, 0.0)
            shrink = jnp.exp2(old - new)
            peak[h] = new
            total[h] = jnp.concatenate([shrink, shrink], axis=1) * total[h] + jnp.dot(
                weights.astype(bf), both, preferred_element_type=f32)
            return 0

        lax.fori_loop(0, heads, head, 0)

    def visit(first, count, chip):
        def one(j, _):
            other_pair, other_ring = chip(j // 2)
            which = (other_pair * 4 + other_ring) * 2 + j % 2
            away = place - which

            @pl.when((away >= 1) & (away < WINDOW // n))
            def _():
                work(kv.at[which], None)
            return 0

        lax.fori_loop(first, count, one, 0)

    work(own, 1)
    every.second(0)
    every.second(1)

    @pl.when(pair == 1)
    def _():
        work(kv.at[ring * 2 + core], 0)

    every.forward(0, 0)
    every.forward(0, 1)
    for copy in every.across[0:4]:
        copy.wait_recv()
    mine = pltpu.make_async_copy(own, kv.at[place], local)
    mine.start()
    mine.wait()
    visit(0, 4, lambda g: (jnp.where(g == 0, pair, 1 - pair), ring))
    every.forward(1, 0)
    every.forward(1, 1)
    for copy in every.across[4:12]:
        copy.wait_recv()
    visit(0, 8, lambda g: (jnp.where(g < 2, pair, 1 - pair), (ring + 1 + 2 * (g % 2)) % 4))
    every.last()
    for copy in every.across[12:]:
        copy.wait_recv()
    visit(0, 4, lambda g: (jnp.where(g == 0, pair, 1 - pair), (ring + 2) % 4))
    for copy in every.started:
        copy.wait_send()
    for h in range(heads):
        out_ref[:, h * HD:(h + 1) * HD] = total[h, :, 0:HD] / total[h, :, HD:2 * HD]


def run_attention(x, wq, wk, wv, cid):
    n = x.shape[0]
    width = wq.shape[1]
    heads = width // HD
    D = pltpu.SemaphoreType.DMA
    many = copies_of(2, True)
    bf, f32 = jnp.bfloat16, jnp.float32
    return pl.pallas_call(
        attention_kernel,
        out_shape=jax.ShapeDtypeStruct((n, width), f32),
        in_specs=[VM] * 4, out_specs=VM,
        scratch_shapes=[pltpu.VMEM((n, 2 * HD), bf), pltpu.VMEM((16, n, 2 * HD), bf), pltpu.VMEM((heads, n, HD), bf),
                        pltpu.VMEM((heads, n, HD), f32), pltpu.VMEM((heads, n, 2 * HD), f32), D, D((many,)), D((many,))],
        compiler_params=pltpu.CompilerParams(collective_id=cid, has_side_effects=True, vmem_limit_bytes=40 << 20),
    )(x, wq, wk, wv)


def padded(vector):
    return jnp.pad(vector, (0, 128 - vector.shape[0]))[None, :]


def on_device(hidden_in, norm_gain, w_z, w_x, w_b, w_c, w_dt, conv_x, conv_b, conv_c, dt_bias, a_rate,
              skip_gain, group_gain, w_out, attn_gain, w_q, w_k, w_v):
    f32, bf = jnp.float32, jnp.bfloat16
    n = hidden_in.shape[0]
    w_bcd = jnp.concatenate([w_b, w_c, jnp.pad(w_dt, ((0, 0), (0, 128 - w_dt.shape[1])))], axis=1)
    w_z_all = lax.all_gather(w_z, "seq", axis=0, tiled=True)
    w_out_all = lax.all_gather(w_out, "seq")
    normed, w_x_all, w_bcd_all = run_first(hidden_in, w_x, w_bcd, norm_gain[None, :], 0)
    bcd = jnp.dot(normed, w_bcd_all, preferred_element_type=f32)
    xp = jnp.dot(normed, w_x_all, preferred_element_type=f32)
    route = [(i, i + 1) for i in range(lax.axis_size("seq") - 1)]
    rims = lax.ppermute(jnp.concatenate([xp[n - 8:], bcd[n - 8:, 0:2 * N]], axis=1), "seq", route)
    width = xp.shape[1]
    y, cc, cum, send = run_ssd(
        xp, bcd, rims[:, 0:width], rims[:, width:], conv_x, jnp.concatenate([conv_b, conv_c], axis=1),
        padded(dt_bias), padded(a_rate), jnp.repeat(skip_gain, P_SIZE)[None, :])
    y_normed = run_gate(normed, w_z_all, send, y, cc, cum, group_gain[None, :], 3)
    mixed, normed_two = run_mix(y_normed, w_out_all, hidden_in, attn_gain[None, :], 1)
    return (mixed, run_attention(normed_two, w_q, w_k, w_v, 4))


def solution(mesh):
    tile, cols = P("seq", "mp"), P(None, "mp")
    placed = (tile, P(), tile, tile, tile, tile, tile, cols, cols, cols, P("mp"), P("mp"), P("mp"), P("mp"),
              P("mp", "seq"), P(), cols, cols, cols)
    return jax.shard_map(on_device, mesh=mesh, in_specs=placed, out_specs=(tile, tile), check_vma=False)
```

```python
import jax
import jax.numpy as jnp
from jax import lax
from jax.experimental import pallas as pl
from jax.experimental.pallas import tpu as pltpu
from jax.sharding import PartitionSpec as P

MESH = pl.DeviceIdType.MESH
VM = pl.BlockSpec(memory_space=pltpu.VMEM)
P_SIZE = 64
N = 128
HD = 128
WINDOW = 4096
QB = 128


def rows(start, size):
    return pl.ds(start, size)


class Gather:
    def __init__(self, view, own, names, pair, ring, core, sends, recvs, base, pieces, fan):
        self.view, self.own, self.names = view, own, names
        self.pair, self.ring, self.core = pair, ring, core
        self.sends, self.recvs, self.next, self.pieces, self.fan = sends, recvs, base, pieces, fan
        self.right, self.left, self.far = (ring + 1) % 4, (ring + 3) % 4, (ring + 2) % 4
        self.started, self.across = [], []
        self.y, self.a, self.b, self.f = {}, {}, {}, []

    def send(self, src, block, piece, pair, ring, core):
        copy = pltpu.make_async_remote_copy(
            src_ref=src, dst_ref=self.view(*block, piece), send_sem=self.sends.at[self.next], recv_sem=self.recvs.at[self.next],
            device_id=self.names(pair, ring, core), device_id_type=MESH)
        self.next += 1
        copy.start()
        self.started.append(copy)
        return copy

    def over(self, src, block, piece):
        if self.fan:
            self.across.append(self.send(src, block, piece, self.pair, self.ring, 1 - self.core))

    def begin(self):
        me = (self.pair, self.ring, self.core)
        for k, piece in enumerate(self.pieces):
            src = self.own(piece)
            self.y[k] = self.send(src, me, piece, 1 - self.pair, self.ring, self.core)
            self.a[k] = [self.send(src, me, piece, self.pair, to, self.core) for to in (self.right, self.left)]
            self.over(src, me, piece)

    def second(self, k):
        piece, block = self.pieces[k], (1 - self.pair, self.ring, self.core)
        self.y[k].wait_recv()
        src = self.view(*block, piece)
        self.b[k] = [self.send(src, block, piece, self.pair, to, self.core) for to in (self.right, self.left)]
        self.over(src, block, piece)

    def forward(self, which, k):
        pair = self.pair if which == 0 else 1 - self.pair
        piece, first = self.pieces[k], k < len(self.pieces) // 2
        for d, (to, origin) in enumerate(((self.right, self.left), (self.left, self.right))):
            (self.a, self.b)[which][k][d].wait_recv()
            block = (pair, origin, self.core)
            src = self.view(*block, piece)
            if first == (d == 0):
                self.f.append((self.send(src, block, piece, self.pair, to, self.core), (pair, self.far, self.core), piece))
            self.over(src, block, piece)

    def last(self):
        for copy, block, piece in self.f:
            copy.wait_recv()
            self.over(self.view(*block, piece), block, piece)

    def finish(self):
        for copy in self.across:
            copy.wait_recv()
        for copy in self.started:
            copy.wait_send()


def copies_of(pieces, fan):
    return pieces * (7 + (8 if fan else 0))


def seq_names(pair, ring, core):
    return {"seq": (pair * 4 + ring) * 2 + core}


def mp_names(pair, ring, core):
    return {"mp": pair * 4 + ring}


def greet(ids):
    barrier = pltpu.get_barrier_semaphore()
    for other in ids:
        pl.semaphore_signal(barrier, inc=1, device_id=other, device_id_type=MESH)
    pl.semaphore_wait(barrier, len(ids))


def seq_place():
    me = lax.axis_index("seq")
    return me // 8, (me // 2) % 4, me % 2


def mp_place():
    me = lax.axis_index("mp")
    return me // 4, me % 4


def neighbours(names, pair, ring, core, fan):
    ids = [names(1 - pair, ring, core), names(pair, (ring + 1) % 4, core), names(pair, (ring + 3) % 4, core)]
    return ids + ([names(pair, ring, 1 - core)] if fan else [])


def cut(total, count):
    return [pl.ds(k * (total // count), total // count) for k in range(count)]


def write_normed(whole, gain_ref, normed_ref, start, count, size):
    blocks, _, wide = whole.shape

    def norm(c, _):
        piece = rows(pl.multiple_of(start + c * size, 16), size)
        square = jnp.zeros((size, wide), jnp.float32)
        for b in range(blocks):
            value = whole[b, piece, :].astype(jnp.float32)
            square = square + value * value
        scale = lax.rsqrt(jnp.sum(square, axis=1, keepdims=True) / (blocks * wide) + 1e-05)
        for b in range(blocks):
            lanes = slice(b * wide, (b + 1) * wide)
            normed_ref[piece, lanes] = (whole[b, piece, :].astype(jnp.float32) * scale * gain_ref[:, lanes]).astype(normed_ref.dtype)
        return 0

    lax.fori_loop(0, count // size, norm, 0)


class RingFirst(Gather):
    def begin(self):
        me = (self.pair, self.ring, self.core)
        self.pairs_open = []
        for k, piece in enumerate(self.pieces):
            src = self.own(piece)
            self.a[k] = [self.send(src, me, piece, self.pair, to, self.core) for to in (self.right, self.left)]
            self.pairs_open.append((self.send(src, me, piece, 1 - self.pair, self.ring, self.core), self.ring, piece))
            self.over(src, me, piece)

    def beside(self, src, block, piece):
        self.pairs_open.append((self.send(src, block, piece, 1 - self.pair, self.ring, self.core), block[1], piece))
        self.over(src, block, piece)

    def forward(self, k):
        piece, first = self.pieces[k], k < len(self.pieces) // 2
        for d, (to, origin) in enumerate(((self.right, self.left), (self.left, self.right))):
            self.a[k][d].wait_recv()
            block = (self.pair, origin, self.core)
            src = self.view(*block, piece)
            if first == (d == 0):
                self.f.append((self.send(src, block, piece, self.pair, to, self.core), (self.pair, self.far, self.core), piece))
            self.beside(src, block, piece)

    def last(self):
        for copy, block, piece in self.f:
            copy.wait_recv()
            self.beside(self.view(*block, piece), block, piece)

    def pairs(self):
        for copy, ring, piece in self.pairs_open:
            copy.wait_recv()
            block = (1 - self.pair, ring, self.core)
            self.over(self.view(*block, piece), block, piece)


def three_terms(decay):
    bf, f32 = jnp.bfloat16, jnp.float32
    big = decay.astype(bf).astype(f32)
    middle = (decay - big).astype(bf).astype(f32)
    small = (decay - big - middle).astype(bf).astype(f32)
    which = lax.broadcasted_iota(jnp.int32, decay.shape, 0)
    return jnp.where(which == 0, big, jnp.where(which == 1, middle, small)).astype(bf)


def decay_of(block):
    tail = block.astype(jnp.float32)
    return tail[0:1] + (tail[1:2] + tail[2:3])


def mixer_kernel(x_ref, wx_ref, wb_ref, wz_ref, wo_ref, norm_ref, cx_ref, cbc_ref, bias_ref, rate_ref, skip_ref, gain_ref,
                 out_ref, woa, whole, normed, wxa, wba, wza, padx, padbc, bcd, y, gate, state, cc, cumul, tail, mine, theirs,
                 agg, aggs, turn, half_in, half_out, incoming, local, ts, tr, hs, hr, es, er, bs, br, xs, xr, zs, zr, os, orr, gs, gr):
    bf, f32 = jnp.bfloat16, jnp.float32
    mpair, mring = mp_place()
    pair, ring, core = seq_place()
    place = lax.axis_index("seq")
    following, previous = (place + 1) % 16, (place + 15) % 16
    greet(neighbours(mp_names, mpair, mring, 0, False) + neighbours(seq_names, pair, ring, core, True)
          + [{"seq": following}, {"seq": previous}])
    n = x_ref.shape[0]
    depth, tall = wx_ref.shape[0], wo_ref.shape[0]
    count = n // QB
    width = wx_ref.shape[1]

    def wide_view(ref):
        return lambda pair, ring, core, piece: ref.at[pl.ds(((pair * 4 + ring) * 2 + core) * depth + piece.start, piece.size), :]

    def seq_gather(kind, view, own, sends, recvs, base, pieces, fan=True):
        return kind(view, lambda piece: own.at[piece], seq_names, pair, ring, core, sends, recvs, base, pieces, fan)

    def mp_view(pair, ring, core, piece):
        return whole.at[pair * 4 + ring, piece]

    hidden = Gather(mp_view, lambda piece: x_ref.at[piece], mp_names, mpair, mring, 0, hs, hr, 0, cut(n, 2), False)
    edge = Gather(mp_view, lambda piece: tail, mp_names, mpair, mring, 0, es, er, 0, [pl.ds(n, 16)], False)
    small = seq_gather(Gather, wide_view(wba), wb_ref, bs, br, 0, cut(depth, 2))
    big = seq_gather(Gather, wide_view(wxa), wx_ref, xs, xr, 0, cut(depth, 2))
    fan2 = copies_of(2, True)
    quarters, parts = cut(depth, 4), cut(tall, 4)
    z_pair = seq_gather(Gather, wide_view(wza), wz_ref, zs, zr, 0, quarters[0:2])
    z_ring = seq_gather(RingFirst, wide_view(wza), wz_ref, zs, zr, fan2, quarters[2:4])

    def out_view(pair, ring, core, piece):
        return woa.at[(pair * 4 + ring) * 2 + core, piece]

    o_pair = seq_gather(Gather, out_view, wo_ref, os, orr, 0, parts[0:2])
    o_ring = seq_gather(RingFirst, out_view, wo_ref, os, orr, fan2, parts[2:4])
    own_rows = pl.ds(place * depth, depth)
    at_home = [pltpu.make_async_copy(x_ref, whole.at[mpair * 4 + mring, pl.ds(0, n)], local.at[0]),
               pltpu.make_async_copy(wx_ref, wxa.at[own_rows, :], local.at[1]),
               pltpu.make_async_copy(wb_ref, wba.at[own_rows, :], local.at[2]),
               pltpu.make_async_copy(wz_ref, wza.at[own_rows, :], local.at[3]),
               pltpu.make_async_copy(wo_ref, woa.at[place], local.at[4])]

    def to_device(src, dst, index, device):
        copy = pltpu.make_async_remote_copy(src_ref=src, dst_ref=dst, send_sem=ts.at[index], recv_sem=tr.at[index],
                                            device_id=device, device_id_type=MESH)
        copy.start()
        return copy

    shifted = to_device(x_ref.at[pl.ds(n - 16, 16)], tail, 0, {"seq": following})
    small.begin()
    hidden.begin()
    big.begin()
    for copy in at_home:
        copy.start()
    shifted.wait_recv()
    edge.begin()
    home_tail = pltpu.make_async_copy(tail, whole.at[mpair * 4 + mring, pl.ds(n, 16)], local.at[5])
    home_tail.start()
    for k in range(2):
        small.second(k)
        hidden.second(k)
        big.second(k)
    edge.second(0)
    for which in range(2):
        for k in range(2):
            for g in (small, hidden, big):
                g.forward(which, k)
        edge.forward(which, 0)
    z_ring.begin()
    z_pair.begin()
    hidden.last()
    edge.last()
    at_home[0].wait()
    home_tail.wait()
    write_normed(whole, norm_ref, normed, 0, n, 32)
    write_normed(whole, norm_ref, normed, n, 16, 16)
    small.last()
    small.finish()
    at_home[2].wait()
    inside = jnp.where(place > 0, 1.0, 0.0)
    product = jnp.dot(normed[...], wba[...], preferred_element_type=f32)
    bcd[...] = product[0:n, 2 * N:3 * N]
    padbc[pl.ds(8, n), :] = product[0:n, 0:2 * N]
    padbc[pl.ds(0, 8), :] = product[n + 8:n + 16, 0:2 * N] * inside
    z_pair.second(0)
    z_pair.second(1)
    big.last()
    big.finish()
    at_home[1].wait()
    for part in range(4):
        lanes = slice(part * 256, (part + 1) * 256)
        product = jnp.dot(normed[...], wxa[:, lanes], preferred_element_type=f32)
        padx[pl.ds(8, n), lanes] = product[0:n]
        padx[pl.ds(0, 8), lanes] = product[n + 8:n + 16] * inside
    z_ring.forward(0)
    z_ring.forward(1)

    state[...] = jnp.zeros_like(state)
    row = lax.broadcasted_iota(jnp.int32, (QB, QB), 0)
    col = lax.broadcasted_iota(jnp.int32, (QB, QB), 1)
    causal = row >= col
    tri = jnp.where(causal, 1.0, 0.0).astype(f32)
    low = col < P_SIZE

    def conv(pad, taps, start, lanes):
        whole_rows = pad[pl.ds(start, QB + 8), lanes]
        total = taps[0:1, lanes] * whole_rows[5:5 + QB]
        for j in range(1, 4):
            total = total + taps[j:j + 1, lanes] * whole_rows[5 + j:5 + j + QB]
        return total / (1.0 + jnp.exp(-total))

    def one(c, before):
        start = pl.multiple_of(c * QB, QB)
        here = pl.ds(start, QB)
        bv = conv(padbc, cbc_ref, start, slice(0, N))
        cv = conv(padbc, cbc_ref, start, slice(N, 2 * N)).astype(bf)
        cc[here, :] = cv
        raw = bcd[here, :] + bias_ref[...]
        step = jnp.maximum(raw, 0.0) + jnp.log1p(jnp.exp(-jnp.abs(raw)))
        decay = -rate_ref[...] * step
        cum = jnp.dot(tri, decay, precision=lax.Precision.HIGHEST, preferred_element_type=f32)
        cumul[here, :] = cum + before
        cum_t, step_t = cum.T, step.T
        last = cum[QB - 1:QB, :]
        bt = bv.T.astype(bf)
        affinity = jnp.dot(cv, bt, preferred_element_type=f32)
        for p in range(width // 128):
            lanes = slice(p * 128, (p + 1) * 128)
            xv = conv(padx, cx_ref, start, lanes)
            mixes, grown, tails, ends = [], [], [], []
            for h in (2 * p, 2 * p + 1):
                ct = jnp.broadcast_to(cum[:, h:h + 1], (QB, QB))
                st = jnp.broadcast_to(step[:, h:h + 1], (QB, QB))
                end = jnp.broadcast_to(last[:, h:h + 1], (1, QB))
                spread = jnp.where(causal, ct - cum_t[h:h + 1, :], -jnp.inf)
                mixes.append((affinity * jnp.exp(spread) * step_t[h:h + 1, :]).astype(bf))
                grown.append(ct)
                tails.append(jnp.exp(end - ct) * st)
                ends.append(end)
            mixed = jnp.concatenate(mixes, axis=1)
            xs2 = jnp.concatenate([jnp.where(low, xv, 0.0).astype(bf), jnp.where(low, 0.0, xv).astype(bf)], axis=0)
            out = jnp.dot(mixed, xs2, preferred_element_type=f32)
            old = state[:, lanes]
            carried = jnp.dot(cv, old.astype(bf), preferred_element_type=f32)
            out = out + jnp.exp(jnp.where(low, grown[0], grown[1])) * carried
            y[here, lanes] = out + skip_ref[0:1, lanes] * xv
            weighted = (xv * jnp.where(low, tails[0], tails[1])).astype(bf)
            fresh = jnp.dot(bt, weighted, preferred_element_type=f32)
            state[:, lanes] = jnp.exp(jnp.where(low[0:1], ends[0], ends[1])) * old + fresh
        return before + last

    total = lax.fori_loop(0, count, one, jnp.zeros((1, 128), f32))
    mine[0:N, :] = state[...].astype(bf)
    for p in range(width // 128):
        lanes = slice(p * 128, (p + 1) * 128)
        ends = [jnp.broadcast_to(total[:, h:h + 1], (16, 128)) for h in (2 * p, 2 * p + 1)]
        mine[N:N + 16, lanes] = three_terms(jnp.exp(jnp.where(low[0:16], ends[0], ends[1])))
    swapped = to_device(mine, theirs, 1, {"seq": place + 1 - 2 * core})
    for which in range(2):
        for k in range(2):
            z_pair.forward(which, k)
    swapped.wait_recv()
    half = width // 2
    ours = pl.ds(pl.multiple_of(core * half, half), half)
    rest = pl.ds(pl.multiple_of((1 - core) * half, half), half)
    a, b = mine[:, ours].astype(f32), theirs[:, ours].astype(f32)
    head = core == 0
    early, late = jnp.where(head, a, b), jnp.where(head, b, a)
    early_decay, late_decay = decay_of(early[N:N + 16]), decay_of(late[N:N + 16])
    agg[0:N, :] = (late_decay * early[0:N] + late[0:N]).astype(bf)
    agg[N:N + 16, :] = three_terms(jnp.broadcast_to(early_decay * late_decay, (16, half)))
    chip = pair * 4 + ring
    chips = Gather(lambda pair, ring, core, piece: aggs.at[pair * 4 + ring, piece], lambda piece: agg.at[piece], seq_names,
                   pair, ring, core, gs, gr, 0, [pl.ds(0, 80), pl.ds(80, N + 16 - 80)], False)
    chips.begin()
    o_ring.begin()
    o_pair.begin()
    z_ring.last()
    chips.second(0)
    chips.second(1)
    z_pair.last()
    o_pair.second(0)
    o_pair.second(1)
    for which in range(2):
        for k in range(2):
            chips.forward(which, k)
    z_ring.pairs()
    o_ring.forward(0)
    o_ring.forward(1)
    z_pair.finish()
    z_ring.finish()
    at_home[3].wait()

    def open_gate(part):
        lanes = slice(part * 256, (part + 1) * 256)
        gate[:, lanes] = jnp.dot(normed[0:n, :], wza[:, lanes], preferred_element_type=f32)

    open_gate(0)
    o_pair.forward(0, 0)
    o_pair.forward(0, 1)
    open_gate(1)
    chips.last()
    half_out[...] = jnp.zeros_like(half_out)

    def add(k, _):
        half_out[...] = decay_of(aggs[k, N:N + 16, :]) * half_out[...] + aggs[k, 0:N, :].astype(f32)
        return 0

    lax.fori_loop(0, chip, add, 0)
    turn[...] = half_out[...].astype(bf)
    given = to_device(turn, half_in, 2, {"seq": place + 1 - 2 * core})
    o_pair.forward(1, 0)
    o_pair.forward(1, 1)
    open_gate(2)
    o_ring.last()
    open_gate(3)
    given.wait_recv()
    incoming[:, ours] = half_out[...]
    incoming[:, rest] = half_in[...].astype(f32)
    keep = jnp.where(head, 0.0, 1.0)
    before = theirs[N:N + 16, :].astype(f32)
    before_decay = jnp.where(head, 1.0, before[0:1] + (before[1:2] + before[2:3]))
    incoming[...] = before_decay * incoming[...] + keep * theirs[0:N, :].astype(f32)
    low_rows = low

    def close(c, _):
        here = pl.ds(pl.multiple_of(c * QB, QB), QB)
        cv = cc[here, :]
        cum = cumul[here, :]
        square = jnp.zeros((QB, 128), f32)
        for p in range(width // 128):
            lanes = slice(p * 128, (p + 1) * 128)
            ct = jnp.where(low_rows, jnp.broadcast_to(cum[:, 2 * p:2 * p + 1], (QB, 128)),
                           jnp.broadcast_to(cum[:, 2 * p + 1:2 * p + 2], (QB, 128)))
            carried = jnp.dot(cv, incoming[:, lanes].astype(bf), preferred_element_type=f32)
            g = gate[here, lanes]
            value = (y[here, lanes] + jnp.exp(ct) * carried) * (g / (1.0 + jnp.exp(-g)))
            gate[here, lanes] = value
            square = square + value * value
        scale = lax.rsqrt(jnp.sum(square, axis=1, keepdims=True) / width + 1e-05)
        out_ref[here, :] = (gate[here, :] * scale * gain_ref[...]).astype(bf)
        return 0

    lax.fori_loop(0, count, close, 0)
    o_pair.last()
    o_ring.pairs()
    for g in (o_pair, o_ring, hidden, edge, chips):
        g.finish()
    at_home[4].wait()
    for copy in (shifted, swapped, given):
        copy.wait_send()


def run_mixer(x, wx, wb, wz, wo, norm_gain, conv_x, conv_bc, bias, rate, skip, gain, cid):
    n, w = x.shape
    depth, width = wx.shape
    tall, cols = wo.shape
    D, V = pltpu.SemaphoreType.DMA, pltpu.VMEM
    bf, f32 = jnp.bfloat16, jnp.float32
    fan2, plain2 = copies_of(2, True), copies_of(2, False)
    pairs = []
    for size in (3, plain2, copies_of(1, False), fan2, fan2, 2 * fan2, 2 * fan2, plain2):
        pairs += [D((size,)), D((size,))]
    return pl.pallas_call(
        mixer_kernel,
        out_shape=(jax.ShapeDtypeStruct((n, width), bf), jax.ShapeDtypeStruct((16, tall, cols), bf)),
        in_specs=[VM] * 12, out_specs=(VM, VM),
        scratch_shapes=[V((8, n + 16, w), bf), V((n + 16, 8 * w), bf), V((16 * depth, width), bf), V((16 * depth, wb.shape[1]), bf),
                        V((16 * depth, width), bf), V((n + 8, width), f32), V((n + 8, 2 * N), f32), V((n, N), f32),
                        V((n, width), f32), V((n, width), f32), V((N, width), f32), V((n, N), bf), V((n, 128), f32),
                        V((16, w), bf), V((N + 16, width), bf), V((N + 16, width), bf), V((N + 16, width // 2), bf),
                        V((8, N + 16, width // 2), bf), V((N, width // 2), bf), V((N, width // 2), bf), V((N, width // 2), f32), V((N, width), f32),
                        D((6,))] + pairs,
        compiler_params=pltpu.CompilerParams(collective_id=cid, has_side_effects=True, vmem_limit_bytes=63 << 20),
    )(x, wx, wb, wz, wo, norm_gain, conv_x, conv_bc, bias, rate, skip, gain)


def mix_kernel(y_ref, w_hbm, hidden_ref, gain_ref, mixed_ref, normed_ref, w, p, tmp, d1, d2, ysrc, ydst, whole, wsem,
               s1, r1, s2, r2, sraw, rraw, sy, ry, gs, gr):
    high, low = mp_place()
    right, left, far = (low + 1) % 4, (low + 3) % 4, (low + 2) % 4
    me = high * 4 + low
    order = (1 - high, high)
    sides = ((right, left), (left, right))
    n = y_ref.shape[0]
    half, quarter = n // 2, n // 4
    f32 = jnp.float32
    blocks = [pair * 4 + ring for ring in (far, right, left, low) for pair in order]
    loads = [pltpu.make_async_copy(w_hbm.at[pl.ds(2 * b, 2)], w.at[pl.ds(2 * b, 2)], wsem.at[i]) for i, b in enumerate(blocks)]
    for load in loads:
        load.start()
    greet(neighbours(mp_names, high, low, 0, False))

    def send(src, dst, pair, ring, ssem, rsem):
        copy = pltpu.make_async_remote_copy(src_ref=src, dst_ref=dst, send_sem=ssem, recv_sem=rsem,
                                            device_id=mp_names(pair, ring, 0), device_id_type=MESH)
        copy.start()
        sent.append(copy)
        return copy

    def product(h, b):
        here = slice(h * half, (h + 1) * half)
        cols = w.shape[2]
        for c in range(2):
            p[b, here, c * cols:(c + 1) * cols] = jnp.dot(
                y_ref[here, :], w[2 * b + c], preferred_element_type=f32).astype(p.dtype)

    def start_first(h, k):
        return [send(p.at[order[k] * 4 + far, rows(h * half + d * quarter, quarter)], d1.at[h, k, d], high, sides[d][0],
                     s1.at[h, k, d], r1.at[h, k, d]) for d in range(2)]

    def start_raw(h, k, d):
        return send(p.at[order[k] * 4 + sides[d][0], rows(h * half + (1 - d) * quarter, quarter)],
                    d2.at[h, k, d, rows((1 - d) * quarter, quarter)], high, sides[d][0], sraw.at[h, k, d], rraw.at[h, k, d])

    def pass_on(h, k):
        result = []
        for d in range(2):
            first[h][k][d].wait_recv()
            here = slice(h * half + d * quarter, h * half + (d + 1) * quarter)
            tmp[h, k, d] = (d1[h, k, d].astype(f32) + p[order[k] * 4 + sides[d][0], here, :].astype(f32)).astype(tmp.dtype)
            result.append(send(tmp.at[h, k, d], d2.at[h, k, d, rows(d * quarter, quarter)], high, sides[d][0],
                               s2.at[h, k, d], r2.at[h, k, d]))
        second[h][k] = result

    def total(h, k):
        for d in range(2):
            raw[h][k][d].wait_recv()
            second[h][k][d].wait_recv()
        here = slice(h * half, (h + 1) * half)
        return p[order[k] * 4 + low, here, :].astype(f32) + d2[h, k, 0].astype(f32) + d2[h, k, 1].astype(f32)

    def give(h):
        ysrc[h] = total(h, 0).astype(ysrc.dtype)
        across[h] = send(ysrc.at[h], ydst.at[h], 1 - high, low, sy.at[h], ry.at[h])

    def close(h):
        here = slice(h * half, (h + 1) * half)
        own = total(h, 1)
        across[h].wait_recv()
        result = hidden_ref[here, :].astype(f32) + (own + ydst[h].astype(f32))
        mixed_ref[here, :] = result
        whole[me, here, :] = result.astype(whole.dtype)
        gathers[h].begin()

    sent = []
    first, raw, second = [[None, None] for _ in range(2)], [[None, None] for _ in range(2)], [[None, None] for _ in range(2)]
    across = [None, None]

    def view(pair, ring, core, piece):
        return whole.at[pair * 4 + ring, piece]

    gathers = [Gather(view, lambda piece: whole.at[me, piece], mp_names, high, low, 0, gs, gr, h * copies_of(2, False),
                      [pl.ds(h * half, quarter), pl.ds(h * half + quarter, quarter)], False) for h in range(2)]
    for h in range(2):
        raw[h] = [[None, None], [None, None]]
        for i, b in enumerate(blocks):
            if h == 0:
                loads[i].wait()
            product(h, b)
            if h == 0 and i < 2:
                first[0][i] = start_first(0, i)
            if h == 0 and 2 <= i < 6:
                raw[0][i % 2][i // 2 - 1] = start_raw(0, i % 2, i // 2 - 1)
    pass_on(0, 0)
    pass_on(0, 1)
    for k in range(2):
        first[1][k] = start_first(1, k)
    for k in range(2):
        for d in range(2):
            raw[1][k][d] = start_raw(1, k, d)
    give(0)
    pass_on(1, 0)
    pass_on(1, 1)
    close(0)
    give(1)
    early, late = gathers
    early.second(0)
    early.second(1)
    early.forward(0, 0)
    early.forward(0, 1)
    close(1)
    early.forward(1, 0)
    early.forward(1, 1)
    late.second(0)
    late.second(1)
    late.forward(0, 0)
    late.forward(0, 1)
    early.last()
    late.forward(1, 0)
    late.forward(1, 1)
    write_normed(whole, gain_ref, normed_ref, 0, half, 32)
    late.last()
    write_normed(whole, gain_ref, normed_ref, half, half, 32)
    early.finish()
    late.finish()
    for copy in sent:
        copy.wait_send()


def run_mix(y, w, hidden, gain, cid):
    n, width = hidden.shape
    D = pltpu.SemaphoreType.DMA
    bf = jnp.bfloat16
    V = pltpu.VMEM
    few = 2 * copies_of(2, False)
    return pl.pallas_call(
        mix_kernel,
        out_shape=(jax.ShapeDtypeStruct((n, width), jnp.float32), jax.ShapeDtypeStruct((n, 8 * width), bf)),
        in_specs=[VM, pl.BlockSpec(memory_space=pl.ANY), VM, VM], out_specs=(VM, VM),
        scratch_shapes=[V(w.shape, bf), V((8, n, width), bf), V((2, 2, 2, n // 4, width), bf), V((2, 2, 2, n // 4, width), bf),
                        V((2, 2, 2, n // 2, width), bf), V((2, n // 2, width), bf), V((2, n // 2, width), bf), V((8, n, width), bf),
                        D((8,))] + [D((2, 2, 2))] * 6 + [D((2,))] * 2 + [D((few,))] * 2,
        compiler_params=pltpu.CompilerParams(collective_id=cid, has_side_effects=True, vmem_limit_bytes=48 << 20),
    )(y, w, hidden, gain)


def attention_kernel(x_ref, wq_ref, wk_ref, wv_ref, out_ref, own, kv, q, peak, total, local, ss, sr):
    place = lax.axis_index("seq")
    pair, ring, core = seq_place()
    greet(neighbours(seq_names, pair, ring, core, True))
    n = x_ref.shape[0]
    heads = q.shape[0]
    bf, f32 = jnp.bfloat16, jnp.float32
    scale = HD ** -0.5 * 1.4426950408889634
    own[:, 0:HD] = jnp.dot(x_ref[...], wk_ref[...], preferred_element_type=f32).astype(bf)
    own[:, HD:2 * HD] = jnp.dot(x_ref[...], wv_ref[...], preferred_element_type=f32).astype(bf)
    every = Gather(lambda pair, ring, core, piece: kv.at[(pair * 4 + ring) * 2 + core, piece], lambda piece: own.at[piece],
                   seq_names, pair, ring, core, ss, sr, 0, cut(n, 2), True)
    every.begin()
    for h in range(heads):
        q[h] = jnp.dot(x_ref[...], wq_ref[:, h * HD:(h + 1) * HD], preferred_element_type=f32).astype(bf)
    peak[...] = jnp.full_like(peak, -1e30)
    total[...] = jnp.zeros_like(total)

    def work(block, edge):
        def head(h, _):
            keys = block[:, 0:HD]
            both = jnp.concatenate([block[:, HD:2 * HD], jnp.ones((n, HD), bf)], axis=1)
            if edge is not None:
                t = lax.broadcasted_iota(jnp.int32, (n, n), 0)
                s = lax.broadcasted_iota(jnp.int32, (n, n), 1)
                allowed = s > t if edge == 0 else s <= t
            scores = lax.dot_general(q[h], keys, (((1,), (1,)), ((), ())), preferred_element_type=f32) * scale
            if edge is not None:
                scores = jnp.where(allowed, scores, -1e30)
            old = peak[h]
            new = jnp.maximum(old, jnp.max(scores, axis=1, keepdims=True))
            weights = jnp.exp2(scores - new[:, 0:1])
            if edge == 0:
                weights = jnp.where(allowed, weights, 0.0)
            shrink = jnp.exp2(old - new)
            peak[h] = new
            total[h] = jnp.concatenate([shrink, shrink], axis=1) * total[h] + jnp.dot(
                weights.astype(bf), both, preferred_element_type=f32)
            return 0

        lax.fori_loop(0, heads, head, 0)

    def visit(first, count, chip):
        def one(j, _):
            other_pair, other_ring = chip(j // 2)
            which = (other_pair * 4 + other_ring) * 2 + j % 2
            away = place - which

            @pl.when((away >= 1) & (away < WINDOW // n))
            def _():
                work(kv.at[which], None)
            return 0

        lax.fori_loop(first, count, one, 0)

    work(own, 1)
    every.second(0)
    every.second(1)

    @pl.when(pair == 1)
    def _():
        work(kv.at[ring * 2 + core], 0)

    every.forward(0, 0)
    every.forward(0, 1)
    for copy in every.across[0:4]:
        copy.wait_recv()
    mine = pltpu.make_async_copy(own, kv.at[place], local)
    mine.start()
    mine.wait()
    visit(0, 4, lambda g: (jnp.where(g == 0, pair, 1 - pair), ring))
    every.forward(1, 0)
    every.forward(1, 1)
    for copy in every.across[4:12]:
        copy.wait_recv()
    visit(0, 8, lambda g: (jnp.where(g < 2, pair, 1 - pair), (ring + 1 + 2 * (g % 2)) % 4))
    every.last()
    for copy in every.across[12:]:
        copy.wait_recv()
    visit(0, 4, lambda g: (jnp.where(g == 0, pair, 1 - pair), (ring + 2) % 4))
    for copy in every.started:
        copy.wait_send()
    for h in range(heads):
        out_ref[:, h * HD:(h + 1) * HD] = total[h, :, 0:HD] / total[h, :, HD:2 * HD]


def run_attention(x, wq, wk, wv, cid):
    n = x.shape[0]
    width = wq.shape[1]
    heads = width // HD
    D = pltpu.SemaphoreType.DMA
    many = copies_of(2, True)
    bf, f32 = jnp.bfloat16, jnp.float32
    return pl.pallas_call(
        attention_kernel,
        out_shape=jax.ShapeDtypeStruct((n, width), f32),
        in_specs=[VM] * 4, out_specs=VM,
        scratch_shapes=[pltpu.VMEM((n, 2 * HD), bf), pltpu.VMEM((16, n, 2 * HD), bf), pltpu.VMEM((heads, n, HD), bf),
                        pltpu.VMEM((heads, n, HD), f32), pltpu.VMEM((heads, n, 2 * HD), f32), D, D((many,)), D((many,))],
        compiler_params=pltpu.CompilerParams(collective_id=cid, has_side_effects=True, vmem_limit_bytes=40 << 20),
    )(x, wq, wk, wv)


def padded(vector):
    return jnp.pad(vector, (0, 128 - vector.shape[0]))[None, :]


def on_device(hidden_in, norm_gain, w_z, w_x, w_b, w_c, w_dt, conv_x, conv_b, conv_c, dt_bias, a_rate,
              skip_gain, group_gain, w_out, attn_gain, w_q, w_k, w_v):
    w_bcd = jnp.concatenate([w_b, w_c, jnp.pad(w_dt, ((0, 0), (0, 128 - w_dt.shape[1])))], axis=1)
    y_normed, w_out_all = run_mixer(
        hidden_in, w_x, w_bcd, w_z, w_out, norm_gain[None, :], conv_x, jnp.concatenate([conv_b, conv_c], axis=1),
        padded(dt_bias), padded(a_rate), jnp.repeat(skip_gain, P_SIZE)[None, :], group_gain[None, :], 0)
    mixed, normed_two = run_mix(y_normed, w_out_all, hidden_in, attn_gain[None, :], 1)
    return (mixed, run_attention(normed_two, w_q, w_k, w_v, 2))


def solution(mesh):
    tile, cols = P("seq", "mp"), P(None, "mp")
    placed = (tile, P(), tile, tile, tile, tile, tile, cols, cols, cols, P("mp"), P("mp"), P("mp"), P("mp"),
              P("mp", "seq"), P(), cols, cols, cols)
    return jax.shard_map(on_device, mesh=mesh, in_specs=placed, out_specs=(tile, tile), check_vma=False)
```

```python
import jax
import jax.numpy as jnp
from jax import lax
from jax.experimental import pallas as pl
from jax.experimental.pallas import tpu as pltpu
from jax.sharding import PartitionSpec as P

MESH = pl.DeviceIdType.MESH
VM = pl.BlockSpec(memory_space=pltpu.VMEM)
P_SIZE = 64
N = 128
HD = 128
WINDOW = 4096
QB = 128


def rows(start, size):
    return pl.ds(start, size)


class Gather:
    def __init__(self, view, own, names, pair, ring, core, sends, recvs, base, pieces, fan):
        self.view, self.own, self.names = view, own, names
        self.pair, self.ring, self.core = pair, ring, core
        self.sends, self.recvs, self.next, self.pieces, self.fan = sends, recvs, base, pieces, fan
        self.right, self.left, self.far = (ring + 1) % 4, (ring + 3) % 4, (ring + 2) % 4
        self.started, self.across = [], []
        self.y, self.a, self.b, self.f = {}, {}, {}, []

    def send(self, src, block, piece, pair, ring, core):
        copy = pltpu.make_async_remote_copy(
            src_ref=src, dst_ref=self.view(*block, piece), send_sem=self.sends.at[self.next], recv_sem=self.recvs.at[self.next],
            device_id=self.names(pair, ring, core), device_id_type=MESH)
        self.next += 1
        copy.start()
        self.started.append(copy)
        return copy

    def over(self, src, block, piece):
        if self.fan:
            self.across.append(self.send(src, block, piece, self.pair, self.ring, 1 - self.core))

    def begin(self):
        me = (self.pair, self.ring, self.core)
        for k, piece in enumerate(self.pieces):
            src = self.own(piece)
            self.y[k] = self.send(src, me, piece, 1 - self.pair, self.ring, self.core)
            self.a[k] = [self.send(src, me, piece, self.pair, to, self.core) for to in (self.right, self.left)]
            self.over(src, me, piece)

    def second(self, k):
        piece, block = self.pieces[k], (1 - self.pair, self.ring, self.core)
        self.y[k].wait_recv()
        src = self.view(*block, piece)
        self.b[k] = [self.send(src, block, piece, self.pair, to, self.core) for to in (self.right, self.left)]
        self.over(src, block, piece)

    def forward(self, which, k):
        pair = self.pair if which == 0 else 1 - self.pair
        piece, first = self.pieces[k], k < len(self.pieces) // 2
        for d, (to, origin) in enumerate(((self.right, self.left), (self.left, self.right))):
            (self.a, self.b)[which][k][d].wait_recv()
            block = (pair, origin, self.core)
            src = self.view(*block, piece)
            if first == (d == 0):
                self.f.append((self.send(src, block, piece, self.pair, to, self.core), (pair, self.far, self.core), piece))
            self.over(src, block, piece)

    def last(self):
        for copy, block, piece in self.f:
            copy.wait_recv()
            self.over(self.view(*block, piece), block, piece)

    def finish(self):
        for copy in self.across:
            copy.wait_recv()
        for copy in self.started:
            copy.wait_send()


def copies_of(pieces, fan):
    return pieces * (7 + (8 if fan else 0))


def seq_names(pair, ring, core):
    return {"seq": (pair * 4 + ring) * 2 + core}


def mp_names(pair, ring, core):
    return {"mp": pair * 4 + ring}


def greet(ids):
    barrier = pltpu.get_barrier_semaphore()
    for other in ids:
        pl.semaphore_signal(barrier, inc=1, device_id=other, device_id_type=MESH)
    pl.semaphore_wait(barrier, len(ids))


def seq_place():
    me = lax.axis_index("seq")
    return me // 8, (me // 2) % 4, me % 2


def mp_place():
    me = lax.axis_index("mp")
    return me // 4, me % 4


def neighbours(names, pair, ring, core, fan):
    ids = [names(1 - pair, ring, core), names(pair, (ring + 1) % 4, core), names(pair, (ring + 3) % 4, core)]
    return ids + ([names(pair, ring, 1 - core)] if fan else [])


def cut(total, count):
    return [pl.ds(k * (total // count), total // count) for k in range(count)]


def write_normed(whole, gain_ref, normed_ref, start, count, size):
    blocks, _, wide = whole.shape

    def norm(c, _):
        piece = rows(pl.multiple_of(start + c * size, 16), size)
        square = jnp.zeros((size, wide), jnp.float32)
        for b in range(blocks):
            value = whole[b, piece, :].astype(jnp.float32)
            square = square + value * value
        scale = lax.rsqrt(jnp.sum(square, axis=1, keepdims=True) / (blocks * wide) + 1e-05)
        for b in range(blocks):
            lanes = slice(b * wide, (b + 1) * wide)
            normed_ref[piece, lanes] = (whole[b, piece, :].astype(jnp.float32) * scale * gain_ref[:, lanes]).astype(normed_ref.dtype)
        return 0

    lax.fori_loop(0, count // size, norm, 0)


class RingFirst(Gather):
    def begin(self):
        me = (self.pair, self.ring, self.core)
        self.pairs_open = []
        for k, piece in enumerate(self.pieces):
            src = self.own(piece)
            self.a[k] = [self.send(src, me, piece, self.pair, to, self.core) for to in (self.right, self.left)]
            self.pairs_open.append((self.send(src, me, piece, 1 - self.pair, self.ring, self.core), self.ring, piece))
            self.over(src, me, piece)

    def beside(self, src, block, piece):
        self.pairs_open.append((self.send(src, block, piece, 1 - self.pair, self.ring, self.core), block[1], piece))
        self.over(src, block, piece)

    def forward(self, k):
        piece, first = self.pieces[k], k < len(self.pieces) // 2
        for d, (to, origin) in enumerate(((self.right, self.left), (self.left, self.right))):
            self.a[k][d].wait_recv()
            block = (self.pair, origin, self.core)
            src = self.view(*block, piece)
            if first == (d == 0):
                self.f.append((self.send(src, block, piece, self.pair, to, self.core), (self.pair, self.far, self.core), piece))
            self.beside(src, block, piece)

    def last(self):
        for copy, block, piece in self.f:
            copy.wait_recv()
            self.beside(self.view(*block, piece), block, piece)

    def pairs(self):
        for copy, ring, piece in self.pairs_open:
            copy.wait_recv()
            block = (1 - self.pair, ring, self.core)
            self.over(self.view(*block, piece), block, piece)


def three_terms(decay):
    bf, f32 = jnp.bfloat16, jnp.float32
    big = decay.astype(bf).astype(f32)
    middle = (decay - big).astype(bf).astype(f32)
    small = (decay - big - middle).astype(bf).astype(f32)
    which = lax.broadcasted_iota(jnp.int32, decay.shape, 0)
    return jnp.where(which == 0, big, jnp.where(which == 1, middle, small)).astype(bf)


def decay_of(block):
    tail = block.astype(jnp.float32)
    return tail[0:1] + (tail[1:2] + tail[2:3])


def mixer_kernel(x_ref, wx_ref, wb_ref, wc_ref, wdt_ref, wz_ref, wo_ref, norm_ref, cx_ref, cb_ref, cc_ref, bias_ref, rate_ref,
                 skip_ref, gain_ref,
                 out_ref, woa, wbc, vectors, wda, whole, normed, wxa, wba, wza, padx, padbc, bcd, y, gate, state, cc, cumul, tail, mine, theirs,
                 agg, aggs, turn, half_in, half_out, incoming, local, ts, tr, hs, hr, es, er, ds, dr, bs, br, xs, xr, zs, zr, os, orr, gs, gr):
    bf, f32 = jnp.bfloat16, jnp.float32
    mpair, mring = mp_place()
    pair, ring, core = seq_place()
    place = lax.axis_index("seq")
    following, previous = (place + 1) % 16, (place + 15) % 16
    joined = [pltpu.make_async_copy(wb_ref, wbc.at[:, pl.ds(0, N)], local.at[6]),
              pltpu.make_async_copy(wc_ref, wbc.at[:, pl.ds(N, N)], local.at[7])]
    for copy in joined:
        copy.start()
    greet(neighbours(mp_names, mpair, mring, 0, False) + neighbours(seq_names, pair, ring, core, True)
          + [{"seq": following}, {"seq": previous}])
    n = x_ref.shape[0]
    depth, tall = wx_ref.shape[0], wo_ref.shape[0]
    count = n // QB
    width = wx_ref.shape[1]

    def wide_view(ref):
        return lambda pair, ring, core, piece: ref.at[pl.ds(((pair * 4 + ring) * 2 + core) * depth + piece.start, piece.size), :]

    def seq_gather(kind, view, own, sends, recvs, base, pieces, fan=True):
        return kind(view, lambda piece: own.at[piece], seq_names, pair, ring, core, sends, recvs, base, pieces, fan)

    def mp_view(pair, ring, core, piece):
        return whole.at[pair * 4 + ring, piece]

    hidden = Gather(mp_view, lambda piece: x_ref.at[piece], mp_names, mpair, mring, 0, hs, hr, 0, cut(n, 2), False)
    edge = Gather(mp_view, lambda piece: tail, mp_names, mpair, mring, 0, es, er, 0, [pl.ds(n, 16)], False)
    small = seq_gather(Gather, wide_view(wba), wbc, bs, br, 0, cut(depth, 2))

    def step_view(pair, ring, core, piece):
        return wda.at[:, pl.ds(((pair * 4 + ring) * 2 + core) * depth, depth)]

    steps = Gather(step_view, lambda piece: wdt_ref, seq_names, pair, ring, core, ds, dr, 0, [None], True)
    big = seq_gather(Gather, wide_view(wxa), wx_ref, xs, xr, 0, cut(depth, 2))
    fan2 = copies_of(2, True)
    quarters, parts = cut(depth, 4), cut(tall, 4)
    z_pair = seq_gather(Gather, wide_view(wza), wz_ref, zs, zr, 0, quarters[0:2])
    z_ring = seq_gather(RingFirst, wide_view(wza), wz_ref, zs, zr, fan2, quarters[2:4])

    def out_view(pair, ring, core, piece):
        return woa.at[(pair * 4 + ring) * 2 + core, piece]

    o_pair = seq_gather(Gather, out_view, wo_ref, os, orr, 0, parts[0:2])
    o_ring = seq_gather(RingFirst, out_view, wo_ref, os, orr, fan2, parts[2:4])
    own_rows = pl.ds(place * depth, depth)
    at_home = [pltpu.make_async_copy(x_ref, whole.at[mpair * 4 + mring, pl.ds(0, n)], local.at[0]),
               pltpu.make_async_copy(wx_ref, wxa.at[own_rows, :], local.at[1]),
               pltpu.make_async_copy(wbc, wba.at[own_rows, :], local.at[2]),
               pltpu.make_async_copy(wdt_ref, wda.at[:, own_rows], local.at[8]),
               pltpu.make_async_copy(wz_ref, wza.at[own_rows, :], local.at[3]),
               pltpu.make_async_copy(wo_ref, woa.at[place], local.at[4])]

    def to_device(src, dst, index, device):
        copy = pltpu.make_async_remote_copy(src_ref=src, dst_ref=dst, send_sem=ts.at[index], recv_sem=tr.at[index],
                                            device_id=device, device_id_type=MESH)
        copy.start()
        return copy

    shifted = to_device(x_ref.at[pl.ds(n - 16, 16)], tail, 0, {"seq": following})
    hidden.begin()
    for copy in joined:
        copy.wait()
    small.begin()
    steps.begin()
    big.begin()
    for copy in at_home:
        copy.start()
    shifted.wait_recv()
    edge.begin()
    home_tail = pltpu.make_async_copy(tail, whole.at[mpair * 4 + mring, pl.ds(n, 16)], local.at[5])
    home_tail.start()
    for k in range(2):
        small.second(k)
        hidden.second(k)
        big.second(k)
    steps.second(0)
    edge.second(0)
    for which in range(2):
        for k in range(2):
            for g in (small, hidden, big):
                g.forward(which, k)
        steps.forward(which, 0)
        edge.forward(which, 0)
    z_ring.begin()
    z_pair.begin()
    hidden.last()
    edge.last()
    at_home[0].wait()
    home_tail.wait()
    write_normed(whole, norm_ref, normed, 0, n, 32)
    write_normed(whole, norm_ref, normed, n, 16, 16)
    vectors[...] = jnp.zeros_like(vectors)
    vectors[0:1, 0:bias_ref.shape[1]] = bias_ref[...]
    vectors[1:2, 0:rate_ref.shape[1]] = rate_ref[...]
    bcd[...] = jnp.zeros_like(bcd)
    small.last()
    steps.last()
    small.finish()
    steps.finish()
    at_home[2].wait()
    at_home[3].wait()
    inside = jnp.where(place > 0, 1.0, 0.0)
    product = jnp.dot(normed[...], wba[...], preferred_element_type=f32)
    bcd[:, 0:bias_ref.shape[1]] = lax.dot_general(
        normed[0:n, :], wda[...], (((1,), (1,)), ((), ())), preferred_element_type=f32)
    padbc[pl.ds(8, n), :] = product[0:n]
    padbc[pl.ds(0, 8), :] = product[n + 8:n + 16] * inside
    z_pair.second(0)
    z_pair.second(1)
    big.last()
    big.finish()
    at_home[1].wait()
    for part in range(4):
        lanes = slice(part * 256, (part + 1) * 256)
        product = jnp.dot(normed[...], wxa[:, lanes], preferred_element_type=f32)
        padx[pl.ds(8, n), lanes] = product[0:n]
        padx[pl.ds(0, 8), lanes] = product[n + 8:n + 16] * inside
    z_ring.forward(0)
    z_ring.forward(1)

    state[...] = jnp.zeros_like(state)
    row = lax.broadcasted_iota(jnp.int32, (QB, QB), 0)
    col = lax.broadcasted_iota(jnp.int32, (QB, QB), 1)
    causal = row >= col
    tri = jnp.where(causal, 1.0, 0.0).astype(f32)
    low = col < P_SIZE

    def conv(pad, taps, start, lanes, tap_lanes):
        whole_rows = pad[pl.ds(start, QB + 8), lanes]
        total = taps[0:1, tap_lanes] * whole_rows[5:5 + QB]
        for j in range(1, 4):
            total = total + taps[j:j + 1, tap_lanes] * whole_rows[5 + j:5 + j + QB]
        return total / (1.0 + jnp.exp(-total))

    def one(c, before):
        start = pl.multiple_of(c * QB, QB)
        here = pl.ds(start, QB)
        bv = conv(padbc, cb_ref, start, slice(0, N), slice(0, N))
        cv = conv(padbc, cc_ref, start, slice(N, 2 * N), slice(0, N)).astype(bf)
        cc[here, :] = cv
        raw = bcd[here, :] + vectors[0:1, :]
        step = jnp.maximum(raw, 0.0) + jnp.log1p(jnp.exp(-jnp.abs(raw)))
        decay = -vectors[1:2, :] * step
        cum = jnp.dot(tri, decay, precision=lax.Precision.HIGHEST, preferred_element_type=f32)
        cumul[here, :] = cum + before
        cum_t, step_t = cum.T, step.T
        last = cum[QB - 1:QB, :]
        bt = bv.T.astype(bf)
        affinity = jnp.dot(cv, bt, preferred_element_type=f32)
        for p in range(width // 128):
            lanes = slice(p * 128, (p + 1) * 128)
            xv = conv(padx, cx_ref, start, lanes, lanes)
            mixes, grown, tails, ends = [], [], [], []
            for h in (2 * p, 2 * p + 1):
                ct = jnp.broadcast_to(cum[:, h:h + 1], (QB, QB))
                st = jnp.broadcast_to(step[:, h:h + 1], (QB, QB))
                end = jnp.broadcast_to(last[:, h:h + 1], (1, QB))
                spread = jnp.where(causal, ct - cum_t[h:h + 1, :], -jnp.inf)
                mixes.append((affinity * jnp.exp(spread) * step_t[h:h + 1, :]).astype(bf))
                grown.append(ct)
                tails.append(jnp.exp(end - ct) * st)
                ends.append(end)
            mixed = jnp.concatenate(mixes, axis=1)
            xs2 = jnp.concatenate([jnp.where(low, xv, 0.0).astype(bf), jnp.where(low, 0.0, xv).astype(bf)], axis=0)
            out = jnp.dot(mixed, xs2, preferred_element_type=f32)
            old = state[:, lanes]
            carried = jnp.dot(cv, old.astype(bf), preferred_element_type=f32)
            out = out + jnp.exp(jnp.where(low, grown[0], grown[1])) * carried
            skips = [jnp.broadcast_to(skip_ref[:, h:h + 1], (1, QB)) for h in (2 * p, 2 * p + 1)]
            y[here, lanes] = out + jnp.where(low[0:1], skips[0], skips[1]) * xv
            weighted = (xv * jnp.where(low, tails[0], tails[1])).astype(bf)
            fresh = jnp.dot(bt, weighted, preferred_element_type=f32)
            state[:, lanes] = jnp.exp(jnp.where(low[0:1], ends[0], ends[1])) * old + fresh
        return before + last

    total = lax.fori_loop(0, count, one, jnp.zeros((1, 128), f32))
    mine[0:N, :] = state[...].astype(bf)
    for p in range(width // 128):
        lanes = slice(p * 128, (p + 1) * 128)
        ends = [jnp.broadcast_to(total[:, h:h + 1], (16, 128)) for h in (2 * p, 2 * p + 1)]
        mine[N:N + 16, lanes] = three_terms(jnp.exp(jnp.where(low[0:16], ends[0], ends[1])))
    swapped = to_device(mine, theirs, 1, {"seq": place + 1 - 2 * core})
    for which in range(2):
        for k in range(2):
            z_pair.forward(which, k)
    swapped.wait_recv()
    half = width // 2
    ours = pl.ds(pl.multiple_of(core * half, half), half)
    rest = pl.ds(pl.multiple_of((1 - core) * half, half), half)
    a, b = mine[:, ours].astype(f32), theirs[:, ours].astype(f32)
    head = core == 0
    early, late = jnp.where(head, a, b), jnp.where(head, b, a)
    early_decay, late_decay = decay_of(early[N:N + 16]), decay_of(late[N:N + 16])
    agg[0:N, :] = (late_decay * early[0:N] + late[0:N]).astype(bf)
    agg[N:N + 16, :] = three_terms(jnp.broadcast_to(early_decay * late_decay, (16, half)))
    chip = pair * 4 + ring
    chips = Gather(lambda pair, ring, core, piece: aggs.at[pair * 4 + ring, piece], lambda piece: agg.at[piece], seq_names,
                   pair, ring, core, gs, gr, 0, [pl.ds(0, 80), pl.ds(80, N + 16 - 80)], False)
    chips.begin()
    o_ring.begin()
    o_pair.begin()
    z_ring.last()
    chips.second(0)
    chips.second(1)
    z_pair.last()
    o_pair.second(0)
    o_pair.second(1)
    for which in range(2):
        for k in range(2):
            chips.forward(which, k)
    z_ring.pairs()
    o_ring.forward(0)
    o_ring.forward(1)
    z_pair.finish()
    z_ring.finish()
    at_home[4].wait()

    def open_gate(part):
        lanes = slice(part * 256, (part + 1) * 256)
        gate[:, lanes] = jnp.dot(normed[0:n, :], wza[:, lanes], preferred_element_type=f32)

    open_gate(0)
    o_pair.forward(0, 0)
    o_pair.forward(0, 1)
    open_gate(1)
    chips.last()
    half_out[...] = jnp.zeros_like(half_out)

    def add(k, _):
        half_out[...] = decay_of(aggs[k, N:N + 16, :]) * half_out[...] + aggs[k, 0:N, :].astype(f32)
        return 0

    lax.fori_loop(0, chip, add, 0)
    turn[...] = half_out[...].astype(bf)
    given = to_device(turn, half_in, 2, {"seq": place + 1 - 2 * core})
    o_pair.forward(1, 0)
    o_pair.forward(1, 1)
    open_gate(2)
    o_ring.last()
    open_gate(3)
    given.wait_recv()
    incoming[:, ours] = half_out[...]
    incoming[:, rest] = half_in[...].astype(f32)
    keep = jnp.where(head, 0.0, 1.0)
    before = theirs[N:N + 16, :].astype(f32)
    before_decay = jnp.where(head, 1.0, before[0:1] + (before[1:2] + before[2:3]))
    incoming[...] = before_decay * incoming[...] + keep * theirs[0:N, :].astype(f32)
    low_rows = low

    def close(c, _):
        here = pl.ds(pl.multiple_of(c * QB, QB), QB)
        cv = cc[here, :]
        cum = cumul[here, :]
        square = jnp.zeros((QB, 128), f32)
        for p in range(width // 128):
            lanes = slice(p * 128, (p + 1) * 128)
            ct = jnp.where(low_rows, jnp.broadcast_to(cum[:, 2 * p:2 * p + 1], (QB, 128)),
                           jnp.broadcast_to(cum[:, 2 * p + 1:2 * p + 2], (QB, 128)))
            carried = jnp.dot(cv, incoming[:, lanes].astype(bf), preferred_element_type=f32)
            g = gate[here, lanes]
            value = (y[here, lanes] + jnp.exp(ct) * carried) * (g / (1.0 + jnp.exp(-g)))
            gate[here, lanes] = value
            square = square + value * value
        scale = lax.rsqrt(jnp.sum(square, axis=1, keepdims=True) / width + 1e-05)
        out_ref[here, :] = (gate[here, :] * scale * gain_ref[...]).astype(bf)
        return 0

    lax.fori_loop(0, count, close, 0)
    o_pair.last()
    o_ring.pairs()
    for g in (o_pair, o_ring, hidden, edge, chips):
        g.finish()
    at_home[5].wait()
    for copy in (shifted, swapped, given):
        copy.wait_send()


def run_mixer(x, wx, wb, wc, wdt, wz, wo, norm_gain, conv_x, conv_b, conv_c, bias, rate, skip, gain, cid):
    n, w = x.shape
    depth, width = wx.shape
    tall, cols = wo.shape
    D, V = pltpu.SemaphoreType.DMA, pltpu.VMEM
    bf, f32 = jnp.bfloat16, jnp.float32
    fan2, plain2 = copies_of(2, True), copies_of(2, False)
    pairs = []
    for size in (3, plain2, copies_of(1, False), copies_of(1, True), fan2, fan2, 2 * fan2, 2 * fan2, plain2):
        pairs += [D((size,)), D((size,))]
    return pl.pallas_call(
        mixer_kernel,
        out_shape=(jax.ShapeDtypeStruct((n, width), bf), jax.ShapeDtypeStruct((16, tall, cols), bf)),
        in_specs=[VM] * 15, out_specs=(VM, VM),
        scratch_shapes=[V((depth, 2 * N), bf), V((8, 128), f32), V((16, 16 * depth), bf),
                        V((8, n + 16, w), bf), V((n + 16, 8 * w), bf), V((16 * depth, width), bf), V((16 * depth, 2 * N), bf),
                        V((16 * depth, width), bf), V((n + 8, width), f32), V((n + 8, 2 * N), f32), V((n, N), f32),
                        V((n, width), f32), V((n, width), f32), V((N, width), f32), V((n, N), bf), V((n, 128), f32),
                        V((16, w), bf), V((N + 16, width), bf), V((N + 16, width), bf), V((N + 16, width // 2), bf),
                        V((8, N + 16, width // 2), bf), V((N, width // 2), bf), V((N, width // 2), bf), V((N, width // 2), f32), V((N, width), f32),
                        D((9,))] + pairs,
        compiler_params=pltpu.CompilerParams(collective_id=cid, has_side_effects=True, vmem_limit_bytes=63 << 20),
    )(x, wx, wb, wc, wdt, wz, wo, norm_gain, conv_x, conv_b, conv_c, bias, rate, skip, gain)


def mix_kernel(y_ref, w_hbm, hidden_ref, gain_ref, mixed_ref, normed_ref, w, p, tmp, d1, d2, ysrc, ydst, whole, wsem,
               s1, r1, s2, r2, sraw, rraw, sy, ry, gs, gr):
    high, low = mp_place()
    right, left, far = (low + 1) % 4, (low + 3) % 4, (low + 2) % 4
    me = high * 4 + low
    order = (1 - high, high)
    sides = ((right, left), (left, right))
    n = y_ref.shape[0]
    half, quarter = n // 2, n // 4
    f32 = jnp.float32
    blocks = [pair * 4 + ring for ring in (far, right, left, low) for pair in order]
    loads = [pltpu.make_async_copy(w_hbm.at[pl.ds(2 * b, 2)], w.at[pl.ds(2 * b, 2)], wsem.at[i]) for i, b in enumerate(blocks)]
    for load in loads:
        load.start()
    greet(neighbours(mp_names, high, low, 0, False))

    def send(src, dst, pair, ring, ssem, rsem):
        copy = pltpu.make_async_remote_copy(src_ref=src, dst_ref=dst, send_sem=ssem, recv_sem=rsem,
                                            device_id=mp_names(pair, ring, 0), device_id_type=MESH)
        copy.start()
        sent.append(copy)
        return copy

    def product(h, b):
        here = slice(h * half, (h + 1) * half)
        cols = w.shape[2]
        for c in range(2):
            p[b, here, c * cols:(c + 1) * cols] = jnp.dot(
                y_ref[here, :], w[2 * b + c], preferred_element_type=f32).astype(p.dtype)

    def start_first(h, k):
        return [send(p.at[order[k] * 4 + far, rows(h * half + d * quarter, quarter)], d1.at[h, k, d], high, sides[d][0],
                     s1.at[h, k, d], r1.at[h, k, d]) for d in range(2)]

    def start_raw(h, k, d):
        return send(p.at[order[k] * 4 + sides[d][0], rows(h * half + (1 - d) * quarter, quarter)],
                    d2.at[h, k, d, rows((1 - d) * quarter, quarter)], high, sides[d][0], sraw.at[h, k, d], rraw.at[h, k, d])

    def pass_on(h, k):
        result = []
        for d in range(2):
            first[h][k][d].wait_recv()
            here = slice(h * half + d * quarter, h * half + (d + 1) * quarter)
            tmp[h, k, d] = (d1[h, k, d].astype(f32) + p[order[k] * 4 + sides[d][0], here, :].astype(f32)).astype(tmp.dtype)
            result.append(send(tmp.at[h, k, d], d2.at[h, k, d, rows(d * quarter, quarter)], high, sides[d][0],
                               s2.at[h, k, d], r2.at[h, k, d]))
        second[h][k] = result

    def total(h, k):
        for d in range(2):
            raw[h][k][d].wait_recv()
            second[h][k][d].wait_recv()
        here = slice(h * half, (h + 1) * half)
        return p[order[k] * 4 + low, here, :].astype(f32) + d2[h, k, 0].astype(f32) + d2[h, k, 1].astype(f32)

    def give(h):
        ysrc[h] = total(h, 0).astype(ysrc.dtype)
        across[h] = send(ysrc.at[h], ydst.at[h], 1 - high, low, sy.at[h], ry.at[h])

    def close(h):
        here = slice(h * half, (h + 1) * half)
        own = total(h, 1)
        across[h].wait_recv()
        result = hidden_ref[here, :].astype(f32) + (own + ydst[h].astype(f32))
        mixed_ref[here, :] = result
        whole[me, here, :] = result.astype(whole.dtype)
        gathers[h].begin()

    sent = []
    first, raw, second = [[None, None] for _ in range(2)], [[None, None] for _ in range(2)], [[None, None] for _ in range(2)]
    across = [None, None]

    def view(pair, ring, core, piece):
        return whole.at[pair * 4 + ring, piece]

    gathers = [Gather(view, lambda piece: whole.at[me, piece], mp_names, high, low, 0, gs, gr, h * copies_of(2, False),
                      [pl.ds(h * half, quarter), pl.ds(h * half + quarter, quarter)], False) for h in range(2)]
    for h in range(2):
        raw[h] = [[None, None], [None, None]]
        for i, b in enumerate(blocks):
            if h == 0:
                loads[i].wait()
            product(h, b)
            if h == 0 and i < 2:
                first[0][i] = start_first(0, i)
            if h == 0 and 2 <= i < 6:
                raw[0][i % 2][i // 2 - 1] = start_raw(0, i % 2, i // 2 - 1)
    pass_on(0, 0)
    pass_on(0, 1)
    for k in range(2):
        first[1][k] = start_first(1, k)
    for k in range(2):
        for d in range(2):
            raw[1][k][d] = start_raw(1, k, d)
    give(0)
    pass_on(1, 0)
    pass_on(1, 1)
    close(0)
    give(1)
    early, late = gathers
    early.second(0)
    early.second(1)
    early.forward(0, 0)
    early.forward(0, 1)
    close(1)
    early.forward(1, 0)
    early.forward(1, 1)
    late.second(0)
    late.second(1)
    late.forward(0, 0)
    late.forward(0, 1)
    early.last()
    late.forward(1, 0)
    late.forward(1, 1)
    write_normed(whole, gain_ref, normed_ref, 0, half, 32)
    late.last()
    write_normed(whole, gain_ref, normed_ref, half, half, 32)
    early.finish()
    late.finish()
    for copy in sent:
        copy.wait_send()


def run_mix(y, w, hidden, gain, cid):
    n, width = hidden.shape
    D = pltpu.SemaphoreType.DMA
    bf = jnp.bfloat16
    V = pltpu.VMEM
    few = 2 * copies_of(2, False)
    return pl.pallas_call(
        mix_kernel,
        out_shape=(jax.ShapeDtypeStruct((n, width), jnp.float32), jax.ShapeDtypeStruct((n, 8 * width), bf)),
        in_specs=[VM, pl.BlockSpec(memory_space=pl.ANY), VM, VM], out_specs=(VM, VM),
        scratch_shapes=[V(w.shape, bf), V((8, n, width), bf), V((2, 2, 2, n // 4, width), bf), V((2, 2, 2, n // 4, width), bf),
                        V((2, 2, 2, n // 2, width), bf), V((2, n // 2, width), bf), V((2, n // 2, width), bf), V((8, n, width), bf),
                        D((8,))] + [D((2, 2, 2))] * 6 + [D((2,))] * 2 + [D((few,))] * 2,
        compiler_params=pltpu.CompilerParams(collective_id=cid, has_side_effects=True, vmem_limit_bytes=48 << 20),
    )(y, w, hidden, gain)


def attention_kernel(x_ref, wq_ref, wk_ref, wv_ref, out_ref, own, kv, q, peak, total, local, ss, sr):
    place = lax.axis_index("seq")
    pair, ring, core = seq_place()
    greet(neighbours(seq_names, pair, ring, core, True))
    n = x_ref.shape[0]
    heads = q.shape[0]
    bf, f32 = jnp.bfloat16, jnp.float32
    scale = HD ** -0.5 * 1.4426950408889634
    own[:, 0:HD] = jnp.dot(x_ref[...], wk_ref[...], preferred_element_type=f32).astype(bf)
    own[:, HD:2 * HD] = jnp.dot(x_ref[...], wv_ref[...], preferred_element_type=f32).astype(bf)
    every = Gather(lambda pair, ring, core, piece: kv.at[(pair * 4 + ring) * 2 + core, piece], lambda piece: own.at[piece],
                   seq_names, pair, ring, core, ss, sr, 0, cut(n, 2), True)
    every.begin()
    mine = pltpu.make_async_copy(own, kv.at[place], local)
    mine.start()
    for h in range(0, heads, 2):
        both = jnp.dot(x_ref[...], wq_ref[:, h * HD:(h + 2) * HD], preferred_element_type=f32) * scale
        q[h] = both[:, 0:HD].astype(bf)
        q[h + 1] = both[:, HD:2 * HD].astype(bf)
    peak[...] = jnp.full_like(peak, -1e30)
    total[...] = jnp.zeros_like(total)

    def work(block, bounds):
        keys = block[:, 0:HD]
        both = jnp.concatenate([block[:, HD:2 * HD], jnp.ones((n, HD), bf)], axis=1)
        if bounds is not None:
            away = lax.broadcasted_iota(jnp.int32, (n, n), 1) - lax.broadcasted_iota(jnp.int32, (n, n), 0)
            allowed = (away > bounds[0]) & (away <= bounds[1])
        for h in range(heads):
            scores = lax.dot_general(q[h], keys, (((1,), (1,)), ((), ())), preferred_element_type=f32)
            if bounds is not None:
                scores = jnp.where(allowed, scores, -1e30)
            old = peak[h]
            new = jnp.maximum(old, jnp.max(scores, axis=1, keepdims=True))
            weights = jnp.exp2(scores - new[:, 0:1])
            if bounds is not None:
                weights = jnp.where(allowed, weights, 0.0)
            shrink = jnp.exp2(old - new)
            peak[h] = new
            total[h] = jnp.concatenate([shrink, shrink], axis=1) * total[h] + jnp.dot(
                weights.astype(bf), both, preferred_element_type=f32)

    def visit(count, chip):
        def one(j, _):
            other_pair, other_ring = chip(j // 2)
            which = (other_pair * 4 + other_ring) * 2 + j % 2
            away = place - which

            @pl.when((away >= 1) & (away < WINDOW // n))
            def _():
                work(kv.at[which], None)
            return 0

        lax.fori_loop(0, count, one, 0)

    every.second(0)
    every.second(1)
    every.forward(0, 0)
    every.forward(0, 1)
    mine.wait()

    def rim(j, _):
        @pl.when((j == 0) | (pair == 1))
        def _():
            work(kv.at[jnp.where(j == 0, place, ring * 2 + core)], (jnp.where(j == 0, -n, 0), jnp.where(j == 0, 0, n)))
        return 0

    lax.fori_loop(0, 2, rim, 0)
    every.forward(1, 0)
    every.forward(1, 1)
    for copy in every.across[0:12]:
        copy.wait_recv()
    visit(12, lambda g: (jnp.where(g % 2 == 0, pair, 1 - pair), (ring + jnp.where(g < 2, 0, jnp.where(g < 4, 1, 3))) % 4))
    every.last()
    for copy in every.across[12:]:
        copy.wait_recv()
    visit(4, lambda g: (jnp.where(g == 0, pair, 1 - pair), (ring + 2) % 4))
    for copy in every.started:
        copy.wait_send()
    for h in range(heads):
        out_ref[:, h * HD:(h + 1) * HD] = total[h, :, 0:HD] / total[h, :, HD:2 * HD]


def run_attention(x, wq, wk, wv, cid):
    n = x.shape[0]
    width = wq.shape[1]
    heads = width // HD
    D = pltpu.SemaphoreType.DMA
    many = copies_of(2, True)
    bf, f32 = jnp.bfloat16, jnp.float32
    return pl.pallas_call(
        attention_kernel,
        out_shape=jax.ShapeDtypeStruct((n, width), f32),
        in_specs=[VM] * 4, out_specs=VM,
        scratch_shapes=[pltpu.VMEM((n, 2 * HD), bf), pltpu.VMEM((16, n, 2 * HD), bf), pltpu.VMEM((heads, n, HD), bf),
                        pltpu.VMEM((heads, n, HD), f32), pltpu.VMEM((heads, n, 2 * HD), f32), D, D((many,)), D((many,))],
        compiler_params=pltpu.CompilerParams(collective_id=cid, has_side_effects=True, vmem_limit_bytes=40 << 20),
    )(x, wq, wk, wv)


def on_device(hidden_in, norm_gain, w_z, w_x, w_b, w_c, w_dt, conv_x, conv_b, conv_c, dt_bias, a_rate,
              skip_gain, group_gain, w_out, attn_gain, w_q, w_k, w_v):
    y_normed, w_out_all = run_mixer(
        hidden_in, w_x, w_b, w_c, w_dt.T, w_z, w_out, norm_gain[None, :], conv_x, conv_b, conv_c,
        dt_bias[None, :], a_rate[None, :], skip_gain[None, :], group_gain[None, :], 0)
    mixed, normed_two = run_mix(y_normed, w_out_all, hidden_in, attn_gain[None, :], 1)
    return (mixed, run_attention(normed_two, w_q, w_k, w_v, 2))


def solution(mesh):
    tile, cols = P("seq", "mp"), P(None, "mp")
    placed = (tile, P(), tile, tile, tile, tile, tile, cols, cols, cols, P("mp"), P("mp"), P("mp"), P("mp"),
              P("mp", "seq"), P(), cols, cols, cols)
    return jax.shard_map(on_device, mesh=mesh, in_specs=placed, out_specs=(tile, tile), check_vma=False)
```

```python
import jax
import jax.numpy as jnp
from jax import lax
from jax.experimental import pallas as pl
from jax.experimental.pallas import tpu as pltpu
from jax.sharding import PartitionSpec as P

MESH = pl.DeviceIdType.MESH
VM = pl.BlockSpec(memory_space=pltpu.VMEM)
P_SIZE = 64
N = 128
HD = 128
WINDOW = 4096
QB = 128


def rows(start, size):
    return pl.ds(start, size)


class Gather:
    def __init__(self, view, own, names, pair, ring, core, sends, recvs, base, pieces, fan):
        self.view, self.own, self.names = view, own, names
        self.pair, self.ring, self.core = pair, ring, core
        self.sends, self.recvs, self.next, self.pieces, self.fan = sends, recvs, base, pieces, fan
        self.right, self.left, self.far = (ring + 1) % 4, (ring + 3) % 4, (ring + 2) % 4
        self.started, self.across = [], []
        self.y, self.a, self.b, self.f = {}, {}, {}, []

    def send(self, src, block, piece, pair, ring, core):
        copy = pltpu.make_async_remote_copy(
            src_ref=src, dst_ref=self.view(*block, piece), send_sem=self.sends.at[self.next], recv_sem=self.recvs.at[self.next],
            device_id=self.names(pair, ring, core), device_id_type=MESH)
        self.next += 1
        copy.start()
        self.started.append(copy)
        return copy

    def over(self, src, block, piece):
        if self.fan:
            self.across.append(self.send(src, block, piece, self.pair, self.ring, 1 - self.core))

    def begin(self):
        me = (self.pair, self.ring, self.core)
        for k, piece in enumerate(self.pieces):
            src = self.own(piece)
            self.y[k] = self.send(src, me, piece, 1 - self.pair, self.ring, self.core)
            self.a[k] = [self.send(src, me, piece, self.pair, to, self.core) for to in (self.right, self.left)]
            self.over(src, me, piece)

    def second(self, k):
        piece, block = self.pieces[k], (1 - self.pair, self.ring, self.core)
        self.y[k].wait_recv()
        src = self.view(*block, piece)
        self.b[k] = [self.send(src, block, piece, self.pair, to, self.core) for to in (self.right, self.left)]
        self.over(src, block, piece)

    def forward(self, which, k):
        pair = self.pair if which == 0 else 1 - self.pair
        piece, first = self.pieces[k], k < len(self.pieces) // 2
        for d, (to, origin) in enumerate(((self.right, self.left), (self.left, self.right))):
            (self.a, self.b)[which][k][d].wait_recv()
            block = (pair, origin, self.core)
            src = self.view(*block, piece)
            if first == (d == 0):
                self.f.append((self.send(src, block, piece, self.pair, to, self.core), (pair, self.far, self.core), piece))
            self.over(src, block, piece)

    def last(self):
        for copy, block, piece in self.f:
            copy.wait_recv()
            self.over(self.view(*block, piece), block, piece)

    def finish(self):
        for copy in self.across:
            copy.wait_recv()
        for copy in self.started:
            copy.wait_send()


def copies_of(pieces, fan):
    return pieces * (7 + (8 if fan else 0))


def seq_names(pair, ring, core):
    return {"seq": (pair * 4 + ring) * 2 + core}


def mp_names(pair, ring, core):
    return {"mp": pair * 4 + ring}


def greet(ids):
    barrier = pltpu.get_barrier_semaphore()
    for other in ids:
        pl.semaphore_signal(barrier, inc=1, device_id=other, device_id_type=MESH)
    pl.semaphore_wait(barrier, len(ids))


def seq_place():
    me = lax.axis_index("seq")
    return me // 8, (me // 2) % 4, me % 2


def mp_place():
    me = lax.axis_index("mp")
    return me // 4, me % 4


def neighbours(names, pair, ring, core, fan):
    ids = [names(1 - pair, ring, core), names(pair, (ring + 1) % 4, core), names(pair, (ring + 3) % 4, core)]
    return ids + ([names(pair, ring, 1 - core)] if fan else [])


def cut(total, count):
    return [pl.ds(k * (total // count), total // count) for k in range(count)]


def write_normed(whole, gain_ref, normed_ref, start, count, size):
    blocks, _, wide = whole.shape

    def norm(c, _):
        piece = rows(pl.multiple_of(start + c * size, 16), size)
        square = jnp.zeros((size, wide), jnp.float32)
        for b in range(blocks):
            value = whole[b, piece, :].astype(jnp.float32)
            square = square + value * value
        scale = lax.rsqrt(jnp.sum(square, axis=1, keepdims=True) / (blocks * wide) + 1e-05)
        for b in range(blocks):
            lanes = slice(b * wide, (b + 1) * wide)
            normed_ref[piece, lanes] = (whole[b, piece, :].astype(jnp.float32) * scale * gain_ref[:, lanes]).astype(normed_ref.dtype)
        return 0

    lax.fori_loop(0, count // size, norm, 0)


class RingFirst(Gather):
    def begin(self):
        me = (self.pair, self.ring, self.core)
        self.pairs_open = []
        for k, piece in enumerate(self.pieces):
            src = self.own(piece)
            self.a[k] = [self.send(src, me, piece, self.pair, to, self.core) for to in (self.right, self.left)]
            self.pairs_open.append((self.send(src, me, piece, 1 - self.pair, self.ring, self.core), self.ring, piece))
            self.over(src, me, piece)

    def beside(self, src, block, piece):
        self.pairs_open.append((self.send(src, block, piece, 1 - self.pair, self.ring, self.core), block[1], piece))
        self.over(src, block, piece)

    def forward(self, k):
        piece, first = self.pieces[k], k < len(self.pieces) // 2
        for d, (to, origin) in enumerate(((self.right, self.left), (self.left, self.right))):
            self.a[k][d].wait_recv()
            block = (self.pair, origin, self.core)
            src = self.view(*block, piece)
            if first == (d == 0):
                self.f.append((self.send(src, block, piece, self.pair, to, self.core), (self.pair, self.far, self.core), piece))
            self.beside(src, block, piece)

    def last(self):
        for copy, block, piece in self.f:
            copy.wait_recv()
            self.beside(self.view(*block, piece), block, piece)

    def pairs(self):
        for copy, ring, piece in self.pairs_open:
            copy.wait_recv()
            block = (1 - self.pair, ring, self.core)
            self.over(self.view(*block, piece), block, piece)


def three_terms(decay):
    bf, f32 = jnp.bfloat16, jnp.float32
    big = decay.astype(bf).astype(f32)
    middle = (decay - big).astype(bf).astype(f32)
    small = (decay - big - middle).astype(bf).astype(f32)
    which = lax.broadcasted_iota(jnp.int32, decay.shape, 0)
    return jnp.where(which == 0, big, jnp.where(which == 1, middle, small)).astype(bf)


def decay_of(block):
    tail = block.astype(jnp.float32)
    return tail[0:1] + (tail[1:2] + tail[2:3])


def mixer_kernel(x_ref, wx_ref, wb_ref, wc_ref, wdt_ref, wz_ref, wo_ref, norm_ref, cx_ref, cb_ref, cc_ref, bias_ref, rate_ref,
                 skip_ref, gain_ref,
                 out_ref, woa, wbc, vectors, wda, whole, normed, wxa, wba, wza, padx, padbc, bcd, y, gate, state, cc, cumul, tail, mine, theirs,
                 agg, aggs, turn, half_in, half_out, incoming, local, ts, tr, hs, hr, es, er, ds, dr, bs, br, xs, xr, zs, zr, os, orr, gs, gr):
    bf, f32 = jnp.bfloat16, jnp.float32
    mpair, mring = mp_place()
    pair, ring, core = seq_place()
    place = lax.axis_index("seq")
    following, previous = (place + 1) % 16, (place + 15) % 16
    joined = [pltpu.make_async_copy(wb_ref, wbc.at[:, pl.ds(0, N)], local.at[6]),
              pltpu.make_async_copy(wc_ref, wbc.at[:, pl.ds(N, N)], local.at[7])]
    for copy in joined:
        copy.start()
    greet(neighbours(mp_names, mpair, mring, 0, False) + neighbours(seq_names, pair, ring, core, True)
          + [{"seq": following}, {"seq": previous}])
    n = x_ref.shape[0]
    depth, tall = wx_ref.shape[0], wo_ref.shape[0]
    count = n // QB
    width = wx_ref.shape[1]

    def wide_view(ref):
        return lambda pair, ring, core, piece: ref.at[pl.ds(((pair * 4 + ring) * 2 + core) * depth + piece.start, piece.size), :]

    def seq_gather(kind, view, own, sends, recvs, base, pieces, fan=True):
        return kind(view, lambda piece: own.at[piece], seq_names, pair, ring, core, sends, recvs, base, pieces, fan)

    def mp_view(pair, ring, core, piece):
        return whole.at[pair * 4 + ring, piece]

    hidden = Gather(mp_view, lambda piece: x_ref.at[piece], mp_names, mpair, mring, 0, hs, hr, 0, cut(n, 2), False)
    edge = Gather(mp_view, lambda piece: tail, mp_names, mpair, mring, 0, es, er, 0, [pl.ds(n, 16)], False)
    small = seq_gather(Gather, wide_view(wba), wbc, bs, br, 0, cut(depth, 2))

    def step_view(pair, ring, core, piece):
        return wda.at[:, pl.ds(((pair * 4 + ring) * 2 + core) * depth, depth)]

    steps = Gather(step_view, lambda piece: wdt_ref, seq_names, pair, ring, core, ds, dr, 0, [None], True)
    big = seq_gather(Gather, wide_view(wxa), wx_ref, xs, xr, 0, cut(depth, 2))
    fan2 = copies_of(2, True)
    quarters, parts = cut(depth, 4), cut(tall, 4)
    z_pair = seq_gather(Gather, wide_view(wza), wz_ref, zs, zr, 0, quarters[0:2])
    z_ring = seq_gather(RingFirst, wide_view(wza), wz_ref, zs, zr, fan2, quarters[2:4])

    def out_view(pair, ring, core, piece):
        return woa.at[(pair * 4 + ring) * 2 + core, piece]

    o_pair = seq_gather(Gather, out_view, wo_ref, os, orr, 0, parts[0:2])
    o_ring = seq_gather(RingFirst, out_view, wo_ref, os, orr, fan2, parts[2:4])
    own_rows = pl.ds(place * depth, depth)
    at_home = [pltpu.make_async_copy(x_ref, whole.at[mpair * 4 + mring, pl.ds(0, n)], local.at[0]),
               pltpu.make_async_copy(wx_ref, wxa.at[own_rows, :], local.at[1]),
               pltpu.make_async_copy(wbc, wba.at[own_rows, :], local.at[2]),
               pltpu.make_async_copy(wdt_ref, wda.at[:, own_rows], local.at[8]),
               pltpu.make_async_copy(wz_ref, wza.at[own_rows, :], local.at[3]),
               pltpu.make_async_copy(wo_ref, woa.at[place], local.at[4])]

    def to_device(src, dst, index, device):
        copy = pltpu.make_async_remote_copy(src_ref=src, dst_ref=dst, send_sem=ts.at[index], recv_sem=tr.at[index],
                                            device_id=device, device_id_type=MESH)
        copy.start()
        return copy

    shifted = to_device(x_ref.at[pl.ds(n - 16, 16)], tail, 0, {"seq": following})
    hidden.begin()
    for copy in joined:
        copy.wait()
    small.begin()
    steps.begin()
    big.begin()
    for copy in at_home:
        copy.start()
    shifted.wait_recv()
    edge.begin()
    home_tail = pltpu.make_async_copy(tail, whole.at[mpair * 4 + mring, pl.ds(n, 16)], local.at[5])
    home_tail.start()
    for k in range(2):
        small.second(k)
        hidden.second(k)
        big.second(k)
    steps.second(0)
    edge.second(0)
    for which in range(2):
        for k in range(2):
            for g in (small, hidden, big):
                g.forward(which, k)
        steps.forward(which, 0)
        edge.forward(which, 0)
    z_ring.begin()
    z_pair.begin()
    hidden.last()
    edge.last()
    at_home[0].wait()
    home_tail.wait()
    write_normed(whole, norm_ref, normed, 0, n, 32)
    write_normed(whole, norm_ref, normed, n, 16, 16)
    vectors[...] = jnp.zeros_like(vectors)
    vectors[0:1, 0:bias_ref.shape[1]] = bias_ref[...]
    vectors[1:2, 0:rate_ref.shape[1]] = rate_ref[...]
    bcd[...] = jnp.zeros_like(bcd)
    small.last()
    steps.last()
    small.finish()
    steps.finish()
    at_home[2].wait()
    at_home[3].wait()
    inside = jnp.where(place > 0, 1.0, 0.0)
    product = jnp.dot(normed[...], wba[...], preferred_element_type=f32)
    bcd[:, 0:bias_ref.shape[1]] = lax.dot_general(
        normed[0:n, :], wda[...], (((1,), (1,)), ((), ())), preferred_element_type=f32)
    padbc[pl.ds(8, n), :] = product[0:n]
    padbc[pl.ds(0, 8), :] = product[n + 8:n + 16] * inside
    z_pair.second(0)
    z_pair.second(1)
    big.last()
    big.finish()
    at_home[1].wait()
    for part in range(4):
        lanes = slice(part * 256, (part + 1) * 256)
        product = jnp.dot(normed[...], wxa[:, lanes], preferred_element_type=f32)
        padx[pl.ds(8, n), lanes] = product[0:n]
        padx[pl.ds(0, 8), lanes] = product[n + 8:n + 16] * inside
    z_ring.forward(0)
    z_ring.forward(1)

    state[...] = jnp.zeros_like(state)
    row = lax.broadcasted_iota(jnp.int32, (QB, QB), 0)
    col = lax.broadcasted_iota(jnp.int32, (QB, QB), 1)
    causal = row >= col
    tri = jnp.where(causal, 1.0, 0.0).astype(f32)
    low = col < P_SIZE

    def conv(pad, taps, start, lanes, tap_lanes):
        whole_rows = pad[pl.ds(start, QB + 8), lanes]
        total = taps[0:1, tap_lanes] * whole_rows[5:5 + QB]
        for j in range(1, 4):
            total = total + taps[j:j + 1, tap_lanes] * whole_rows[5 + j:5 + j + QB]
        return total / (1.0 + jnp.exp(-total))

    def one(c, before):
        start = pl.multiple_of(c * QB, QB)
        here = pl.ds(start, QB)
        bv = conv(padbc, cb_ref, start, slice(0, N), slice(0, N))
        cv = conv(padbc, cc_ref, start, slice(N, 2 * N), slice(0, N)).astype(bf)
        cc[here, :] = cv
        raw = bcd[here, :] + vectors[0:1, :]
        step = jnp.maximum(raw, 0.0) + jnp.log1p(jnp.exp(-jnp.abs(raw)))
        decay = -vectors[1:2, :] * step
        cum = jnp.dot(tri, decay, precision=lax.Precision.HIGHEST, preferred_element_type=f32)
        cumul[here, :] = cum + before
        cum_t, step_t = cum.T, step.T
        last = cum[QB - 1:QB, :]
        bt = bv.T.astype(bf)
        affinity = jnp.dot(cv, bt, preferred_element_type=f32)
        for p in range(width // 128):
            lanes = slice(p * 128, (p + 1) * 128)
            xv = conv(padx, cx_ref, start, lanes, lanes)
            mixes, grown, tails, ends = [], [], [], []
            for h in (2 * p, 2 * p + 1):
                ct = jnp.broadcast_to(cum[:, h:h + 1], (QB, QB))
                st = jnp.broadcast_to(step[:, h:h + 1], (QB, QB))
                end = jnp.broadcast_to(last[:, h:h + 1], (1, QB))
                spread = jnp.where(causal, ct - cum_t[h:h + 1, :], -jnp.inf)
                mixes.append((affinity * jnp.exp(spread) * step_t[h:h + 1, :]).astype(bf))
                grown.append(ct)
                tails.append(jnp.exp(end - ct) * st)
                ends.append(end)
            mixed = jnp.concatenate(mixes, axis=1)
            xs2 = jnp.concatenate([jnp.where(low, xv, 0.0).astype(bf), jnp.where(low, 0.0, xv).astype(bf)], axis=0)
            out = jnp.dot(mixed, xs2, preferred_element_type=f32)
            old = state[:, lanes]
            carried = jnp.dot(cv, old.astype(bf), preferred_element_type=f32)
            out = out + jnp.exp(jnp.where(low, grown[0], grown[1])) * carried
            skips = [jnp.broadcast_to(skip_ref[:, h:h + 1], (1, QB)) for h in (2 * p, 2 * p + 1)]
            y[here, lanes] = out + jnp.where(low[0:1], skips[0], skips[1]) * xv
            weighted = (xv * jnp.where(low, tails[0], tails[1])).astype(bf)
            fresh = jnp.dot(bt, weighted, preferred_element_type=f32)
            state[:, lanes] = jnp.exp(jnp.where(low[0:1], ends[0], ends[1])) * old + fresh
        return before + last

    total = lax.fori_loop(0, count, one, jnp.zeros((1, 128), f32))
    mine[0:N, :] = state[...].astype(bf)
    for p in range(width // 128):
        lanes = slice(p * 128, (p + 1) * 128)
        ends = [jnp.broadcast_to(total[:, h:h + 1], (16, 128)) for h in (2 * p, 2 * p + 1)]
        mine[N:N + 16, lanes] = three_terms(jnp.exp(jnp.where(low[0:16], ends[0], ends[1])))
    swapped = to_device(mine, theirs, 1, {"seq": place + 1 - 2 * core})
    for which in range(2):
        for k in range(2):
            z_pair.forward(which, k)
    swapped.wait_recv()
    half = width // 2
    ours = pl.ds(pl.multiple_of(core * half, half), half)
    rest = pl.ds(pl.multiple_of((1 - core) * half, half), half)
    a, b = mine[:, ours].astype(f32), theirs[:, ours].astype(f32)
    head = core == 0
    early, late = jnp.where(head, a, b), jnp.where(head, b, a)
    early_decay, late_decay = decay_of(early[N:N + 16]), decay_of(late[N:N + 16])
    agg[0:N, :] = (late_decay * early[0:N] + late[0:N]).astype(bf)
    agg[N:N + 16, :] = three_terms(jnp.broadcast_to(early_decay * late_decay, (16, half)))
    chip = pair * 4 + ring
    chips = Gather(lambda pair, ring, core, piece: aggs.at[pair * 4 + ring, piece], lambda piece: agg.at[piece], seq_names,
                   pair, ring, core, gs, gr, 0, [pl.ds(0, 80), pl.ds(80, N + 16 - 80)], False)
    chips.begin()
    o_ring.begin()
    o_pair.begin()
    z_ring.last()
    chips.second(0)
    chips.second(1)
    z_pair.last()
    o_pair.second(0)
    o_pair.second(1)
    for which in range(2):
        for k in range(2):
            chips.forward(which, k)
    z_ring.pairs()
    o_ring.forward(0)
    o_ring.forward(1)
    z_pair.finish()
    z_ring.finish()
    at_home[4].wait()

    def open_gate(part):
        lanes = slice(part * 256, (part + 1) * 256)
        gate[:, lanes] = jnp.dot(normed[0:n, :], wza[:, lanes], preferred_element_type=f32)

    open_gate(0)
    o_pair.forward(0, 0)
    o_pair.forward(0, 1)
    open_gate(1)
    chips.last()
    half_out[...] = jnp.zeros_like(half_out)

    def add(k, _):
        half_out[...] = decay_of(aggs[k, N:N + 16, :]) * half_out[...] + aggs[k, 0:N, :].astype(f32)
        return 0

    lax.fori_loop(0, chip, add, 0)
    turn[...] = half_out[...].astype(bf)
    given = to_device(turn, half_in, 2, {"seq": place + 1 - 2 * core})
    o_pair.forward(1, 0)
    o_pair.forward(1, 1)
    open_gate(2)
    o_ring.last()
    open_gate(3)
    given.wait_recv()
    incoming[:, ours] = half_out[...]
    incoming[:, rest] = half_in[...].astype(f32)
    keep = jnp.where(head, 0.0, 1.0)
    before = theirs[N:N + 16, :].astype(f32)
    before_decay = jnp.where(head, 1.0, before[0:1] + (before[1:2] + before[2:3]))
    incoming[...] = before_decay * incoming[...] + keep * theirs[0:N, :].astype(f32)
    low_rows = low

    def close(c, _):
        here = pl.ds(pl.multiple_of(c * QB, QB), QB)
        cv = cc[here, :]
        cum = cumul[here, :]
        square = jnp.zeros((QB, 128), f32)
        for p in range(width // 128):
            lanes = slice(p * 128, (p + 1) * 128)
            ct = jnp.where(low_rows, jnp.broadcast_to(cum[:, 2 * p:2 * p + 1], (QB, 128)),
                           jnp.broadcast_to(cum[:, 2 * p + 1:2 * p + 2], (QB, 128)))
            carried = jnp.dot(cv, incoming[:, lanes].astype(bf), preferred_element_type=f32)
            g = gate[here, lanes]
            value = (y[here, lanes] + jnp.exp(ct) * carried) * (g / (1.0 + jnp.exp(-g)))
            gate[here, lanes] = value
            square = square + value * value
        scale = lax.rsqrt(jnp.sum(square, axis=1, keepdims=True) / width + 1e-05)
        out_ref[here, :] = (gate[here, :] * scale * gain_ref[...]).astype(bf)
        return 0

    lax.fori_loop(0, count, close, 0)
    o_pair.last()
    o_ring.pairs()
    for g in (o_pair, o_ring, hidden, edge, chips):
        g.finish()
    at_home[5].wait()
    for copy in (shifted, swapped, given):
        copy.wait_send()


def run_mixer(x, wx, wb, wc, wdt, wz, wo, norm_gain, conv_x, conv_b, conv_c, bias, rate, skip, gain, cid):
    n, w = x.shape
    depth, width = wx.shape
    tall, cols = wo.shape
    D, V = pltpu.SemaphoreType.DMA, pltpu.VMEM
    bf, f32 = jnp.bfloat16, jnp.float32
    fan2, plain2 = copies_of(2, True), copies_of(2, False)
    pairs = []
    for size in (3, plain2, copies_of(1, False), copies_of(1, True), fan2, fan2, 2 * fan2, 2 * fan2, plain2):
        pairs += [D((size,)), D((size,))]
    return pl.pallas_call(
        mixer_kernel,
        out_shape=(jax.ShapeDtypeStruct((n, width), bf), jax.ShapeDtypeStruct((16, tall, cols), bf)),
        in_specs=[VM] * 15, out_specs=(VM, VM),
        scratch_shapes=[V((depth, 2 * N), bf), V((8, 128), f32), V((16, 16 * depth), bf),
                        V((8, n + 16, w), bf), V((n + 16, 8 * w), bf), V((16 * depth, width), bf), V((16 * depth, 2 * N), bf),
                        V((16 * depth, width), bf), V((n + 8, width), f32), V((n + 8, 2 * N), f32), V((n, N), f32),
                        V((n, width), f32), V((n, width), f32), V((N, width), f32), V((n, N), bf), V((n, 128), f32),
                        V((16, w), bf), V((N + 16, width), bf), V((N + 16, width), bf), V((N + 16, width // 2), bf),
                        V((8, N + 16, width // 2), bf), V((N, width // 2), bf), V((N, width // 2), bf), V((N, width // 2), f32), V((N, width), f32),
                        D((9,))] + pairs,
        compiler_params=pltpu.CompilerParams(collective_id=cid, has_side_effects=True, vmem_limit_bytes=63 << 20),
    )(x, wx, wb, wc, wdt, wz, wo, norm_gain, conv_x, conv_b, conv_c, bias, rate, skip, gain)


def mix_kernel(y_ref, w_hbm, hidden_ref, gain_ref, mixed_ref, normed_ref, w, p, tmp, d1, d2, ysrc, ydst, yb, joint, tmpb, d1b, d2b, whole,
               wsem, s1, r1, s2, r2, sraw, rraw, sy, ry, syb, ryb, s1b, r1b, s2b, r2b, srb, rrb, gs, gr):
    high, low = mp_place()
    right, left, far = (low + 1) % 4, (low + 3) % 4, (low + 2) % 4
    me = high * 4 + low
    order = (1 - high, high)
    sides = ((right, left), (left, right))
    n = y_ref.shape[0]
    half = n // 2
    na, nb = ydst.shape[1], yb.shape[2]
    ha, hb = na // 2, nb // 2
    f32 = jnp.float32
    rings = (far, right, left, low)
    blocks = [pair * 4 + ring for ring in rings for pair in order]
    loads = [pltpu.make_async_copy(w_hbm.at[pl.ds(2 * b, 2)], w.at[pl.ds(2 * b, 2)], wsem.at[i]) for i, b in enumerate(blocks)]
    for load in loads:
        load.start()
    greet(neighbours(mp_names, high, low, 0, False))

    def send(src, dst, pair, ring, ssem, rsem):
        copy = pltpu.make_async_remote_copy(src_ref=src, dst_ref=dst, send_sem=ssem, recv_sem=rsem,
                                            device_id=mp_names(pair, ring, 0), device_id_type=MESH)
        copy.start()
        sent.append(copy)
        return copy

    def product(h, b):
        here = slice(h * half, (h + 1) * half)
        cols = w.shape[2]
        for c in range(2):
            p[b, here, c * cols:(c + 1) * cols] = jnp.dot(
                y_ref[here, :], w[2 * b + c], preferred_element_type=f32).astype(p.dtype)

    def start_first(h, k):
        first[h][k] = [send(p.at[order[k] * 4 + far, rows(h * half + d * ha, ha)], d1.at[h, k, d], high, sides[d][0],
                            s1.at[h, k, d], r1.at[h, k, d]) for d in range(2)]

    def start_raw(h, k, d):
        raw[h][k][d] = send(p.at[order[k] * 4 + sides[d][0], rows(h * half + (1 - d) * ha, ha)],
                            d2.at[h, k, d, rows((1 - d) * ha, ha)], high, sides[d][0], sraw.at[h, k, d], rraw.at[h, k, d])

    def pass_on(h, k):
        result = []
        for d in range(2):
            first[h][k][d].wait_recv()
            here = slice(h * half + d * ha, h * half + (d + 1) * ha)
            tmp[h, k, d] = (d1[h, k, d].astype(f32) + p[order[k] * 4 + sides[d][0], here, :].astype(f32)).astype(tmp.dtype)
            result.append(send(tmp.at[h, k, d], d2.at[h, k, d, rows(d * ha, ha)], high, sides[d][0],
                               s2.at[h, k, d], r2.at[h, k, d]))
        second[h][k] = result

    def total(h, k):
        for d in range(2):
            raw[h][k][d].wait_recv()
            second[h][k][d].wait_recv()
        here = slice(h * half, h * half + na)
        return p[order[k] * 4 + low, here, :].astype(f32) + d2[h, k, 0].astype(f32) + d2[h, k, 1].astype(f32)

    def give(h):
        ysrc[h] = total(h, 0).astype(ysrc.dtype)
        across[h] = send(ysrc.at[h], ydst.at[h], 1 - high, low, sy.at[h], ry.at[h])

    def start_pair(h, i):
        open_pair[h][i] = send(p.at[(1 - high) * 4 + rings[i], rows(h * half + na, nb)], yb.at[h, i], 1 - high, low,
                               syb.at[h, i], ryb.at[h, i])

    def join(h, i):
        open_pair[h][i].wait_recv()
        here = slice(h * half + na, (h + 1) * half)
        value = p[high * 4 + rings[i], here, :].astype(f32) + yb[h, i].astype(f32)
        if i < 3:
            joint[h, i] = value.astype(joint.dtype)
        return value

    def start_ring(h):
        join(h, 0)
        first_b[h] = [send(joint.at[h, 0, rows(d * hb, hb)], d1b.at[h, d], high, sides[d][0], s1b.at[h, d], r1b.at[h, d])
                      for d in range(2)]
        for d in range(2):
            join(h, 1 + d)
            raw_b[h][d] = send(joint.at[h, 1 + d, rows((1 - d) * hb, hb)], d2b.at[h, d, rows((1 - d) * hb, hb)], high, sides[d][0],
                               srb.at[h, d], rrb.at[h, d])

    def pass_ring(h):
        for d in range(2):
            first_b[h][d].wait_recv()
            tmpb[h, d] = (d1b[h, d].astype(f32) + joint[h, 1 + d, d * hb:(d + 1) * hb, :].astype(f32)).astype(tmpb.dtype)
            second_b[h][d] = send(tmpb.at[h, d], d2b.at[h, d, rows(d * hb, hb)], high, sides[d][0], s2b.at[h, d], r2b.at[h, d])

    def keep(start, result):
        here = slice(start, start + result.shape[0])
        value = hidden_ref[here, :].astype(f32) + result
        mixed_ref[here, :] = value
        whole[me, here, :] = value.astype(whole.dtype)

    def close(h):
        own = total(h, 1)
        across[h].wait_recv()
        keep(h * half, own + ydst[h].astype(f32))
        pair_first[h].begin()

    def close_ring(h):
        own = join(h, 3)
        for d in range(2):
            raw_b[h][d].wait_recv()
            second_b[h][d].wait_recv()
            own = own + d2b[h, d].astype(f32)
        keep(h * half + na, own)
        ring_first[h].begin()

    sent = []
    first, second = [[None, None] for _ in range(2)], [[None, None] for _ in range(2)]
    raw = [[[None, None], [None, None]] for _ in range(2)]
    across = [None, None]
    open_pair = [[None] * 4 for _ in range(2)]
    first_b, raw_b, second_b = [None, None], [[None, None] for _ in range(2)], [[None, None] for _ in range(2)]

    def view(pair, ring, core, piece):
        return whole.at[pair * 4 + ring, piece]

    def gather(kind, index, start, size):
        return kind(view, lambda piece: whole.at[me, piece], mp_names, high, low, 0, gs, gr, index * copies_of(2, False),
                    [pl.ds(start, size), pl.ds(start + size, size)], False)

    pair_first = [gather(Gather, h, h * half, ha) for h in range(2)]
    ring_first = [gather(RingFirst, 2 + h, h * half + na, hb) for h in range(2)]
    for h in range(2):
        for i, b in enumerate(blocks):
            if h == 0:
                loads[i].wait()
            product(h, b)
            if h == 0:
                if i % 2 == 0:
                    start_pair(0, i // 2)
                if i < 2:
                    start_first(0, i)
                elif i < 6:
                    start_raw(0, i % 2, i // 2 - 1)
    for i in range(4):
        start_pair(1, i)
    pass_on(0, 0)
    start_ring(0)
    pass_on(0, 1)
    for k in range(2):
        start_first(1, k)
    pass_ring(0)
    for k in range(2):
        for d in range(2):
            start_raw(1, k, d)
    give(0)
    pass_on(1, 0)
    start_ring(1)
    close_ring(0)
    pass_on(1, 1)
    pass_ring(1)
    close(0)
    ring_first[0].forward(0)
    ring_first[0].forward(1)
    give(1)
    for k in range(2):
        pair_first[0].second(k)
    for k in range(2):
        pair_first[0].forward(0, k)
    close_ring(1)
    ring_first[0].last()
    close(1)
    for k in range(2):
        pair_first[0].forward(1, k)
    ring_first[1].forward(0)
    ring_first[1].forward(1)
    for k in range(2):
        pair_first[1].second(k)
    for k in range(2):
        pair_first[1].forward(0, k)
    ring_first[1].last()
    pair_first[0].last()
    ring_first[0].pairs()
    for k in range(2):
        pair_first[1].forward(1, k)
    write_normed(whole, gain_ref, normed_ref, 0, half, 32)
    pair_first[1].last()
    ring_first[1].pairs()
    write_normed(whole, gain_ref, normed_ref, half, half, 32)
    for g in pair_first + ring_first:
        g.finish()
    for copy in sent:
        copy.wait_send()


def run_mix(y, w, hidden, gain, cid):
    n, width = hidden.shape
    D = pltpu.SemaphoreType.DMA
    bf = jnp.bfloat16
    V = pltpu.VMEM
    half = n // 2
    na = half // 8 * 5
    nb = half - na
    few = 4 * copies_of(2, False)
    return pl.pallas_call(
        mix_kernel,
        out_shape=(jax.ShapeDtypeStruct((n, width), jnp.float32), jax.ShapeDtypeStruct((n, 8 * width), bf)),
        in_specs=[VM, pl.BlockSpec(memory_space=pl.ANY), VM, VM], out_specs=(VM, VM),
        scratch_shapes=[V(w.shape, bf), V((8, n, width), bf), V((2, 2, 2, na // 2, width), bf), V((2, 2, 2, na // 2, width), bf),
                        V((2, 2, 2, na, width), bf), V((2, na, width), bf), V((2, na, width), bf), V((2, 4, nb, width), bf),
                        V((2, 3, nb, width), bf), V((2, 2, nb // 2, width), bf), V((2, 2, nb // 2, width), bf),
                        V((2, 2, nb, width), bf), V((8, n, width), bf), D((8,))]
        + [D((2, 2, 2))] * 6 + [D((2,))] * 2 + [D((2, 4))] * 2 + [D((2, 2))] * 6 + [D((few,))] * 2,
        compiler_params=pltpu.CompilerParams(collective_id=cid, has_side_effects=True, vmem_limit_bytes=48 << 20),
    )(y, w, hidden, gain)


def attention_kernel(x_ref, wq_ref, wk_ref, wv_ref, out_ref, own, kv, q, peak, total, local, ss, sr):
    place = lax.axis_index("seq")
    pair, ring, core = seq_place()
    greet(neighbours(seq_names, pair, ring, core, True))
    n = x_ref.shape[0]
    heads = q.shape[0]
    bf, f32 = jnp.bfloat16, jnp.float32
    scale = HD ** -0.5 * 1.4426950408889634
    own[:, 0:HD] = jnp.dot(x_ref[...], wk_ref[...], preferred_element_type=f32).astype(bf)
    own[:, HD:2 * HD] = jnp.dot(x_ref[...], wv_ref[...], preferred_element_type=f32).astype(bf)
    every = Gather(lambda pair, ring, core, piece: kv.at[(pair * 4 + ring) * 2 + core, piece], lambda piece: own.at[piece],
                   seq_names, pair, ring, core, ss, sr, 0, cut(n, 2), True)
    every.begin()
    mine = pltpu.make_async_copy(own, kv.at[place], local)
    mine.start()
    for h in range(0, heads, 2):
        both = jnp.dot(x_ref[...], wq_ref[:, h * HD:(h + 2) * HD], preferred_element_type=f32) * scale
        q[h] = both[:, 0:HD].astype(bf)
        q[h + 1] = both[:, HD:2 * HD].astype(bf)
    peak[...] = jnp.full_like(peak, -1e30)
    total[...] = jnp.zeros_like(total)

    def work(block, bounds):
        keys = block[:, 0:HD]
        both = jnp.concatenate([block[:, HD:2 * HD], jnp.ones((n, HD), bf)], axis=1)
        if bounds is not None:
            away = lax.broadcasted_iota(jnp.int32, (n, n), 1) - lax.broadcasted_iota(jnp.int32, (n, n), 0)
            allowed = (away > bounds[0]) & (away <= bounds[1])
        for h in range(heads):
            scores = lax.dot_general(q[h], keys, (((1,), (1,)), ((), ())), preferred_element_type=f32)
            if bounds is not None:
                scores = jnp.where(allowed, scores, -1e30)
            old = peak[h]
            new = jnp.maximum(old, jnp.max(scores, axis=1, keepdims=True))
            weights = jnp.exp2(scores - new[:, 0:1])
            if bounds is not None:
                weights = jnp.where(allowed, weights, 0.0)
            shrink = jnp.exp2(old - new)
            peak[h] = new
            total[h] = jnp.concatenate([shrink, shrink], axis=1) * total[h] + jnp.dot(
                weights.astype(bf), both, preferred_element_type=f32)

    def visit(count, chip):
        def one(j, _):
            other_pair, other_ring = chip(j // 2)
            which = (other_pair * 4 + other_ring) * 2 + j % 2
            away = place - which

            @pl.when((away >= 1) & (away < WINDOW // n))
            def _():
                work(kv.at[which], None)
            return 0

        lax.fori_loop(0, count, one, 0)

    every.second(0)
    every.second(1)
    every.forward(0, 0)
    every.forward(0, 1)
    mine.wait()

    for copy in every.across[0:4]:
        copy.wait_recv()

    def rim(j, _):
        other_core = jnp.where(j % 2 == 0, core, 1 - core)
        which = (jnp.where(j < 2, pair, 1 - pair) * 4 + ring) * 2 + other_core
        away = place - which

        @pl.when((away >= 0) & (away <= WINDOW // n))
        def _():
            work(kv.at[which], (jnp.where(away == WINDOW // n, 0, -n), jnp.where(away == 0, 0, n)))
        return 0

    lax.fori_loop(0, 4, rim, 0)
    every.forward(1, 0)
    every.forward(1, 1)
    for copy in every.across[4:12]:
        copy.wait_recv()
    visit(8, lambda g: (jnp.where(g % 2 == 0, pair, 1 - pair), (ring + jnp.where(g < 2, 1, 3)) % 4))
    every.last()
    for copy in every.across[12:]:
        copy.wait_recv()
    visit(4, lambda g: (jnp.where(g == 0, pair, 1 - pair), (ring + 2) % 4))
    for copy in every.started:
        copy.wait_send()
    for h in range(heads):
        out_ref[:, h * HD:(h + 1) * HD] = total[h, :, 0:HD] / total[h, :, HD:2 * HD]


def run_attention(x, wq, wk, wv, cid):
    n = x.shape[0]
    width = wq.shape[1]
    heads = width // HD
    D = pltpu.SemaphoreType.DMA
    many = copies_of(2, True)
    bf, f32 = jnp.bfloat16, jnp.float32
    return pl.pallas_call(
        attention_kernel,
        out_shape=jax.ShapeDtypeStruct((n, width), f32),
        in_specs=[VM] * 4, out_specs=VM,
        scratch_shapes=[pltpu.VMEM((n, 2 * HD), bf), pltpu.VMEM((16, n, 2 * HD), bf), pltpu.VMEM((heads, n, HD), bf),
                        pltpu.VMEM((heads, n, HD), f32), pltpu.VMEM((heads, n, 2 * HD), f32), D, D((many,)), D((many,))],
        compiler_params=pltpu.CompilerParams(collective_id=cid, has_side_effects=True, vmem_limit_bytes=40 << 20),
    )(x, wq, wk, wv)


def on_device(hidden_in, norm_gain, w_z, w_x, w_b, w_c, w_dt, conv_x, conv_b, conv_c, dt_bias, a_rate,
              skip_gain, group_gain, w_out, attn_gain, w_q, w_k, w_v):
    y_normed, w_out_all = run_mixer(
        hidden_in, w_x, w_b, w_c, w_dt.T, w_z, w_out, norm_gain[None, :], conv_x, conv_b, conv_c,
        dt_bias[None, :], a_rate[None, :], skip_gain[None, :], group_gain[None, :], 0)
    mixed, normed_two = run_mix(y_normed, w_out_all, hidden_in, attn_gain[None, :], 1)
    return (mixed, run_attention(normed_two, w_q, w_k, w_v, 2))


def solution(mesh):
    tile, cols = P("seq", "mp"), P(None, "mp")
    placed = (tile, P(), tile, tile, tile, tile, tile, cols, cols, cols, P("mp"), P("mp"), P("mp"), P("mp"),
              P("mp", "seq"), P(), cols, cols, cols)
    return jax.shard_map(on_device, mesh=mesh, in_specs=placed, out_specs=(tile, tile), check_vma=False)
```

```python
import jax
import jax.numpy as jnp
from jax import lax
from jax.experimental import pallas as pl
from jax.experimental.pallas import tpu as pltpu
from jax.sharding import PartitionSpec as P

MESH = pl.DeviceIdType.MESH
VM = pl.BlockSpec(memory_space=pltpu.VMEM)
P_SIZE = 64
N = 128
HD = 128
WINDOW = 4096
QB = 128


def rows(start, size):
    return pl.ds(start, size)


class Gather:
    def __init__(self, view, own, names, pair, ring, core, sends, recvs, base, pieces, fan):
        self.view, self.own, self.names = view, own, names
        self.pair, self.ring, self.core = pair, ring, core
        self.sends, self.recvs, self.next, self.pieces, self.fan = sends, recvs, base, pieces, fan
        self.right, self.left, self.far = (ring + 1) % 4, (ring + 3) % 4, (ring + 2) % 4
        self.started, self.across = [], []
        self.y, self.a, self.b, self.f = {}, {}, {}, []

    def send(self, src, block, piece, pair, ring, core):
        copy = pltpu.make_async_remote_copy(
            src_ref=src, dst_ref=self.view(*block, piece), send_sem=self.sends.at[self.next], recv_sem=self.recvs.at[self.next],
            device_id=self.names(pair, ring, core), device_id_type=MESH)
        self.next += 1
        copy.start()
        self.started.append(copy)
        return copy

    def over(self, src, block, piece):
        if self.fan:
            self.across.append(self.send(src, block, piece, self.pair, self.ring, 1 - self.core))

    def begin_piece(self, k):
        me, piece = (self.pair, self.ring, self.core), self.pieces[k]
        src = self.own(piece)
        self.y[k] = self.send(src, me, piece, 1 - self.pair, self.ring, self.core)
        self.a[k] = [self.send(src, me, piece, self.pair, to, self.core) for to in (self.right, self.left)]
        self.over(src, me, piece)

    def begin(self):
        for k in range(len(self.pieces)):
            self.begin_piece(k)

    def second(self, k):
        piece, block = self.pieces[k], (1 - self.pair, self.ring, self.core)
        self.y[k].wait_recv()
        src = self.view(*block, piece)
        self.b[k] = [self.send(src, block, piece, self.pair, to, self.core) for to in (self.right, self.left)]
        self.over(src, block, piece)

    def forward(self, which, k):
        pair = self.pair if which == 0 else 1 - self.pair
        piece, first = self.pieces[k], k < len(self.pieces) // 2
        for d, (to, origin) in enumerate(((self.right, self.left), (self.left, self.right))):
            (self.a, self.b)[which][k][d].wait_recv()
            block = (pair, origin, self.core)
            src = self.view(*block, piece)
            if first == (d == 0):
                self.f.append((self.send(src, block, piece, self.pair, to, self.core), (pair, self.far, self.core), piece))
            self.over(src, block, piece)

    def last(self):
        for copy, block, piece in self.f:
            copy.wait_recv()
            self.over(self.view(*block, piece), block, piece)

    def finish(self):
        for copy in self.across:
            copy.wait_recv()
        for copy in self.started:
            copy.wait_send()


def copies_of(pieces, fan):
    return pieces * (7 + (8 if fan else 0))


def seq_names(pair, ring, core):
    return {"seq": (pair * 4 + ring) * 2 + core}


def mp_names(pair, ring, core):
    return {"mp": pair * 4 + ring}


def greet(ids):
    barrier = pltpu.get_barrier_semaphore()
    for other in ids:
        pl.semaphore_signal(barrier, inc=1, device_id=other, device_id_type=MESH)
    pl.semaphore_wait(barrier, len(ids))


def seq_place():
    me = lax.axis_index("seq")
    return me // 8, (me // 2) % 4, me % 2


def mp_place():
    me = lax.axis_index("mp")
    return me // 4, me % 4


def neighbours(names, pair, ring, core, fan):
    ids = [names(1 - pair, ring, core), names(pair, (ring + 1) % 4, core), names(pair, (ring + 3) % 4, core)]
    return ids + ([names(pair, ring, 1 - core)] if fan else [])


def cut(total, count):
    return [pl.ds(k * (total // count), total // count) for k in range(count)]


def write_normed(whole, gain_ref, normed_ref, start, count, size):
    blocks, _, wide = whole.shape

    def norm(c, _):
        piece = rows(pl.multiple_of(start + c * size, 16), size)
        square = jnp.zeros((size, wide), jnp.float32)
        for b in range(blocks):
            value = whole[b, piece, :].astype(jnp.float32)
            square = square + value * value
        scale = lax.rsqrt(jnp.sum(square, axis=1, keepdims=True) / (blocks * wide) + 1e-05)
        for b in range(blocks):
            lanes = slice(b * wide, (b + 1) * wide)
            normed_ref[piece, lanes] = (whole[b, piece, :].astype(jnp.float32) * scale * gain_ref[:, lanes]).astype(normed_ref.dtype)
        return 0

    lax.fori_loop(0, count // size, norm, 0)


class RingFirst(Gather):
    def begin(self):
        me = (self.pair, self.ring, self.core)
        self.pairs_open = []
        for k, piece in enumerate(self.pieces):
            src = self.own(piece)
            self.a[k] = [self.send(src, me, piece, self.pair, to, self.core) for to in (self.right, self.left)]
            self.pairs_open.append((self.send(src, me, piece, 1 - self.pair, self.ring, self.core), self.ring, piece))
            self.over(src, me, piece)

    def beside(self, src, block, piece):
        self.pairs_open.append((self.send(src, block, piece, 1 - self.pair, self.ring, self.core), block[1], piece))
        self.over(src, block, piece)

    def forward(self, k):
        piece, first = self.pieces[k], k < len(self.pieces) // 2
        for d, (to, origin) in enumerate(((self.right, self.left), (self.left, self.right))):
            self.a[k][d].wait_recv()
            block = (self.pair, origin, self.core)
            src = self.view(*block, piece)
            if first == (d == 0):
                self.f.append((self.send(src, block, piece, self.pair, to, self.core), (self.pair, self.far, self.core), piece))
            self.beside(src, block, piece)

    def last(self):
        for copy, block, piece in self.f:
            copy.wait_recv()
            self.beside(self.view(*block, piece), block, piece)

    def pairs(self):
        for copy, ring, piece in self.pairs_open:
            copy.wait_recv()
            block = (1 - self.pair, ring, self.core)
            self.over(self.view(*block, piece), block, piece)


def three_terms(decay):
    bf, f32 = jnp.bfloat16, jnp.float32
    big = decay.astype(bf).astype(f32)
    middle = (decay - big).astype(bf).astype(f32)
    small = (decay - big - middle).astype(bf).astype(f32)
    which = lax.broadcasted_iota(jnp.int32, decay.shape, 0)
    return jnp.where(which == 0, big, jnp.where(which == 1, middle, small)).astype(bf)


def decay_of(block):
    tail = block.astype(jnp.float32)
    return tail[0:1] + (tail[1:2] + tail[2:3])


def mixer_kernel(x_ref, wx_ref, wb_ref, wc_ref, wdt_ref, wz_ref, wo_ref, norm_ref, cx_ref, cb_ref, cc_ref, bias_ref, rate_ref,
                 skip_ref, gain_ref,
                 out_ref, woa, wbc, vectors, wda, whole, normed, wxa, wba, wza, padx, padbc, bcd, y, gate, state, cc, cumul, tail, mine, theirs,
                 agg, aggs, turn, half_in, half_out, incoming, local, ts, tr, hs, hr, es, er, ds, dr, bs, br, xs, xr, zs, zr, os, orr, gs, gr):
    bf, f32 = jnp.bfloat16, jnp.float32
    mpair, mring = mp_place()
    pair, ring, core = seq_place()
    place = lax.axis_index("seq")
    following, previous = (place + 1) % 16, (place + 15) % 16
    joined = [pltpu.make_async_copy(wb_ref, wbc.at[:, pl.ds(0, N)], local.at[6]),
              pltpu.make_async_copy(wc_ref, wbc.at[:, pl.ds(N, N)], local.at[7])]
    for copy in joined:
        copy.start()
    greet(neighbours(mp_names, mpair, mring, 0, False) + neighbours(seq_names, pair, ring, core, True)
          + [{"seq": following}, {"seq": previous}])
    n = x_ref.shape[0]
    depth, tall = wx_ref.shape[0], wo_ref.shape[0]
    count = n // QB
    width = wx_ref.shape[1]

    def wide_view(ref):
        return lambda pair, ring, core, piece: ref.at[pl.ds(((pair * 4 + ring) * 2 + core) * depth + piece.start, piece.size), :]

    def seq_gather(kind, view, own, sends, recvs, base, pieces, fan=True):
        return kind(view, lambda piece: own.at[piece], seq_names, pair, ring, core, sends, recvs, base, pieces, fan)

    def mp_view(pair, ring, core, piece):
        return whole.at[pair * 4 + ring, piece]

    hidden = Gather(mp_view, lambda piece: x_ref.at[piece], mp_names, mpair, mring, 0, hs, hr, 0, cut(n, 2), False)
    edge = Gather(mp_view, lambda piece: tail, mp_names, mpair, mring, 0, es, er, 0, [pl.ds(n, 16)], False)
    small = seq_gather(Gather, wide_view(wba), wbc, bs, br, 0, cut(depth, 2))

    def step_view(pair, ring, core, piece):
        return wda.at[:, pl.ds(((pair * 4 + ring) * 2 + core) * depth, depth)]

    steps = Gather(step_view, lambda piece: wdt_ref, seq_names, pair, ring, core, ds, dr, 0, [None], True)
    big = seq_gather(Gather, wide_view(wxa), wx_ref, xs, xr, 0, cut(depth, 2))
    fan2 = copies_of(2, True)
    quarters, parts = cut(depth, 4), cut(tall, 4)
    z_pair = seq_gather(Gather, wide_view(wza), wz_ref, zs, zr, 0, quarters[0:2])
    z_ring = seq_gather(RingFirst, wide_view(wza), wz_ref, zs, zr, fan2, quarters[2:4])

    def out_view(pair, ring, core, piece):
        return woa.at[(pair * 4 + ring) * 2 + core, piece]

    lead = wo_ref.at[:, pl.ds(0, wo_ref.shape[1] // 2)]
    o_pair = seq_gather(Gather, out_view, lead, os, orr, 0, parts[0:2])
    o_ring = seq_gather(RingFirst, out_view, lead, os, orr, fan2, parts[2:4])
    own_rows = pl.ds(place * depth, depth)
    at_home = [pltpu.make_async_copy(x_ref, whole.at[mpair * 4 + mring, pl.ds(0, n)], local.at[0]),
               pltpu.make_async_copy(wx_ref, wxa.at[own_rows, :], local.at[1]),
               pltpu.make_async_copy(wbc, wba.at[own_rows, :], local.at[2]),
               pltpu.make_async_copy(wdt_ref, wda.at[:, own_rows], local.at[8]),
               pltpu.make_async_copy(wz_ref, wza.at[own_rows, :], local.at[3]),
               pltpu.make_async_copy(lead, woa.at[place], local.at[4])]

    def to_device(src, dst, index, device):
        copy = pltpu.make_async_remote_copy(src_ref=src, dst_ref=dst, send_sem=ts.at[index], recv_sem=tr.at[index],
                                            device_id=device, device_id_type=MESH)
        copy.start()
        return copy

    shifted = to_device(x_ref.at[pl.ds(n - 16, 16)], tail, 0, {"seq": following})
    for copy in joined:
        copy.wait()
    steps.begin()
    small.begin()
    for k in range(2):
        big.begin_piece(k)
        hidden.begin_piece(k)
    for copy in at_home:
        copy.start()
    shifted.wait_recv()
    edge.begin()
    home_tail = pltpu.make_async_copy(tail, whole.at[mpair * 4 + mring, pl.ds(n, 16)], local.at[5])
    home_tail.start()
    steps.second(0)
    small.second(0)
    small.second(1)
    for k in range(2):
        big.second(k)
        small.forward(0, k)
        hidden.forward(0, k)
        big.forward(0, k)
        hidden.second(k)
    steps.forward(0, 0)
    steps.forward(1, 0)
    edge.second(0)
    edge.forward(0, 0)
    small.forward(1, 0)
    small.forward(1, 1)
    for k in range(2):
        hidden.forward(1, k)
        big.forward(1, k)
    edge.forward(1, 0)
    z_ring.begin()
    z_pair.begin()
    hidden.last()
    edge.last()
    at_home[0].wait()
    home_tail.wait()
    write_normed(whole, norm_ref, normed, 0, n, 32)
    write_normed(whole, norm_ref, normed, n, 16, 16)
    vectors[...] = jnp.zeros_like(vectors)
    vectors[0:1, 0:bias_ref.shape[1]] = bias_ref[...]
    vectors[1:2, 0:rate_ref.shape[1]] = rate_ref[...]
    bcd[...] = jnp.zeros_like(bcd)
    small.last()
    steps.last()
    small.finish()
    steps.finish()
    at_home[2].wait()
    at_home[3].wait()
    inside = jnp.where(place > 0, 1.0, 0.0)
    product = jnp.dot(normed[...], wba[...], preferred_element_type=f32)
    bcd[:, 0:bias_ref.shape[1]] = lax.dot_general(
        normed[0:n, :], wda[...], (((1,), (1,)), ((), ())), preferred_element_type=f32)
    padbc[pl.ds(8, n), :] = product[0:n]
    padbc[pl.ds(0, 8), :] = product[n + 8:n + 16] * inside
    z_pair.second(0)
    z_pair.second(1)
    big.last()
    big.finish()
    at_home[1].wait()
    for part in range(4):
        lanes = slice(part * 256, (part + 1) * 256)
        product = jnp.dot(normed[...], wxa[:, lanes], preferred_element_type=f32)
        padx[pl.ds(8, n), lanes] = product[0:n]
        padx[pl.ds(0, 8), lanes] = product[n + 8:n + 16] * inside
    z_ring.forward(0)
    z_ring.forward(1)

    state[...] = jnp.zeros_like(state)
    row = lax.broadcasted_iota(jnp.int32, (QB, QB), 0)
    col = lax.broadcasted_iota(jnp.int32, (QB, QB), 1)
    causal = row >= col
    tri = jnp.where(causal, 1.0, 0.0).astype(f32)
    low = col < P_SIZE

    def conv(pad, taps, start, lanes, tap_lanes):
        whole_rows = pad[pl.ds(start, QB + 8), lanes]
        total = taps[0:1, tap_lanes] * whole_rows[5:5 + QB]
        for j in range(1, 4):
            total = total + taps[j:j + 1, tap_lanes] * whole_rows[5 + j:5 + j + QB]
        return total / (1.0 + jnp.exp(-total))

    def one(c, before):
        start = pl.multiple_of(c * QB, QB)
        here = pl.ds(start, QB)
        bv = conv(padbc, cb_ref, start, slice(0, N), slice(0, N))
        cv = conv(padbc, cc_ref, start, slice(N, 2 * N), slice(0, N)).astype(bf)
        cc[here, :] = cv
        raw = bcd[here, :] + vectors[0:1, :]
        step = jnp.maximum(raw, 0.0) + jnp.log1p(jnp.exp(-jnp.abs(raw)))
        decay = -vectors[1:2, :] * step
        cum = jnp.dot(tri, decay, precision=lax.Precision.HIGHEST, preferred_element_type=f32)
        cumul[here, :] = cum + before
        cum_t, step_t = cum.T, step.T
        last = cum[QB - 1:QB, :]
        bt = bv.T.astype(bf)
        affinity = jnp.dot(cv, bt, preferred_element_type=f32)
        for p in range(width // 128):
            lanes = slice(p * 128, (p + 1) * 128)
            xv = conv(padx, cx_ref, start, lanes, lanes)
            mixes, grown, tails, ends = [], [], [], []
            for h in (2 * p, 2 * p + 1):
                ct = jnp.broadcast_to(cum[:, h:h + 1], (QB, QB))
                st = jnp.broadcast_to(step[:, h:h + 1], (QB, QB))
                end = jnp.broadcast_to(last[:, h:h + 1], (1, QB))
                spread = jnp.where(causal, ct - cum_t[h:h + 1, :], -jnp.inf)
                mixes.append((affinity * jnp.exp(spread) * step_t[h:h + 1, :]).astype(bf))
                grown.append(ct)
                tails.append(jnp.exp(end - ct) * st)
                ends.append(end)
            mixed = jnp.concatenate(mixes, axis=1)
            xs2 = jnp.concatenate([jnp.where(low, xv, 0.0).astype(bf), jnp.where(low, 0.0, xv).astype(bf)], axis=0)
            out = jnp.dot(mixed, xs2, preferred_element_type=f32)
            old = state[:, lanes]
            carried = jnp.dot(cv, old.astype(bf), preferred_element_type=f32)
            out = out + jnp.exp(jnp.where(low, grown[0], grown[1])) * carried
            skips = [jnp.broadcast_to(skip_ref[:, h:h + 1], (1, QB)) for h in (2 * p, 2 * p + 1)]
            y[here, lanes] = out + jnp.where(low[0:1], skips[0], skips[1]) * xv
            weighted = (xv * jnp.where(low, tails[0], tails[1])).astype(bf)
            fresh = jnp.dot(bt, weighted, preferred_element_type=f32)
            state[:, lanes] = jnp.exp(jnp.where(low[0:1], ends[0], ends[1])) * old + fresh
        return before + last

    total = lax.fori_loop(0, count, one, jnp.zeros((1, 128), f32))
    mine[0:N, :] = state[...].astype(bf)
    for p in range(width // 128):
        lanes = slice(p * 128, (p + 1) * 128)
        ends = [jnp.broadcast_to(total[:, h:h + 1], (16, 128)) for h in (2 * p, 2 * p + 1)]
        mine[N:N + 16, lanes] = three_terms(jnp.exp(jnp.where(low[0:16], ends[0], ends[1])))
    swapped = to_device(mine, theirs, 1, {"seq": place + 1 - 2 * core})
    for which in range(2):
        for k in range(2):
            z_pair.forward(which, k)
    swapped.wait_recv()
    half = width // 2
    ours = pl.ds(pl.multiple_of(core * half, half), half)
    rest = pl.ds(pl.multiple_of((1 - core) * half, half), half)
    a, b = mine[:, ours].astype(f32), theirs[:, ours].astype(f32)
    head = core == 0
    early, late = jnp.where(head, a, b), jnp.where(head, b, a)
    early_decay, late_decay = decay_of(early[N:N + 16]), decay_of(late[N:N + 16])
    agg[0:N, :] = (late_decay * early[0:N] + late[0:N]).astype(bf)
    agg[N:N + 16, :] = three_terms(jnp.broadcast_to(early_decay * late_decay, (16, half)))
    chip = pair * 4 + ring
    chips = Gather(lambda pair, ring, core, piece: aggs.at[pair * 4 + ring, piece], lambda piece: agg.at[piece], seq_names,
                   pair, ring, core, gs, gr, 0, [pl.ds(0, 80), pl.ds(80, N + 16 - 80)], False)
    chips.begin()
    o_ring.begin()
    o_pair.begin()
    z_ring.last()
    chips.second(0)
    chips.second(1)
    z_pair.last()
    o_pair.second(0)
    o_pair.second(1)
    for which in range(2):
        for k in range(2):
            chips.forward(which, k)
    z_ring.pairs()
    o_ring.forward(0)
    o_ring.forward(1)
    z_pair.finish()
    z_ring.finish()
    at_home[4].wait()

    def open_gate(part):
        lanes = slice(part * 256, (part + 1) * 256)
        gate[:, lanes] = jnp.dot(normed[0:n, :], wza[:, lanes], preferred_element_type=f32)

    open_gate(0)
    o_pair.forward(0, 0)
    o_pair.forward(0, 1)
    open_gate(1)
    chips.last()
    half_out[...] = jnp.zeros_like(half_out)

    def add(k, _):
        half_out[...] = decay_of(aggs[k, N:N + 16, :]) * half_out[...] + aggs[k, 0:N, :].astype(f32)
        return 0

    lax.fori_loop(0, chip, add, 0)
    turn[...] = half_out[...].astype(bf)
    given = to_device(turn, half_in, 2, {"seq": place + 1 - 2 * core})
    o_pair.forward(1, 0)
    o_pair.forward(1, 1)
    open_gate(2)
    o_ring.last()
    open_gate(3)
    given.wait_recv()
    incoming[:, ours] = half_out[...]
    incoming[:, rest] = half_in[...].astype(f32)
    keep = jnp.where(head, 0.0, 1.0)
    before = theirs[N:N + 16, :].astype(f32)
    before_decay = jnp.where(head, 1.0, before[0:1] + (before[1:2] + before[2:3]))
    incoming[...] = before_decay * incoming[...] + keep * theirs[0:N, :].astype(f32)
    low_rows = low

    def close(c, _):
        here = pl.ds(pl.multiple_of(c * QB, QB), QB)
        cv = cc[here, :]
        cum = cumul[here, :]
        square = jnp.zeros((QB, 128), f32)
        for p in range(width // 128):
            lanes = slice(p * 128, (p + 1) * 128)
            ct = jnp.where(low_rows, jnp.broadcast_to(cum[:, 2 * p:2 * p + 1], (QB, 128)),
                           jnp.broadcast_to(cum[:, 2 * p + 1:2 * p + 2], (QB, 128)))
            carried = jnp.dot(cv, incoming[:, lanes].astype(bf), preferred_element_type=f32)
            g = gate[here, lanes]
            value = (y[here, lanes] + jnp.exp(ct) * carried) * (g / (1.0 + jnp.exp(-g)))
            gate[here, lanes] = value
            square = square + value * value
        scale = lax.rsqrt(jnp.sum(square, axis=1, keepdims=True) / width + 1e-05)
        out_ref[here, :] = (gate[here, :] * scale * gain_ref[...]).astype(bf)
        return 0

    lax.fori_loop(0, count, close, 0)
    o_pair.last()
    o_ring.pairs()
    for g in (o_pair, o_ring, hidden, edge, chips):
        g.finish()
    at_home[5].wait()
    for copy in (shifted, swapped, given):
        copy.wait_send()


def run_mixer(x, wx, wb, wc, wdt, wz, wo, norm_gain, conv_x, conv_b, conv_c, bias, rate, skip, gain, cid):
    n, w = x.shape
    depth, width = wx.shape
    tall, cols = wo.shape
    D, V = pltpu.SemaphoreType.DMA, pltpu.VMEM
    bf, f32 = jnp.bfloat16, jnp.float32
    fan2, plain2 = copies_of(2, True), copies_of(2, False)
    pairs = []
    for size in (3, plain2, copies_of(1, False), copies_of(1, True), fan2, fan2, 2 * fan2, 2 * fan2, plain2):
        pairs += [D((size,)), D((size,))]
    return pl.pallas_call(
        mixer_kernel,
        out_shape=(jax.ShapeDtypeStruct((n, width), bf), jax.ShapeDtypeStruct((16, tall, cols // 2), bf)),
        in_specs=[VM] * 15, out_specs=(VM, VM),
        scratch_shapes=[V((depth, 2 * N), bf), V((8, 128), f32), V((16, 16 * depth), bf),
                        V((8, n + 16, w), bf), V((n + 16, 8 * w), bf), V((16 * depth, width), bf), V((16 * depth, 2 * N), bf),
                        V((16 * depth, width), bf), V((n + 8, width), f32), V((n + 8, 2 * N), f32), V((n, N), f32),
                        V((n, width), f32), V((n, width), f32), V((N, width), f32), V((n, N), bf), V((n, 128), f32),
                        V((16, w), bf), V((N + 16, width), bf), V((N + 16, width), bf), V((N + 16, width // 2), bf),
                        V((8, N + 16, width // 2), bf), V((N, width // 2), bf), V((N, width // 2), bf), V((N, width // 2), f32), V((N, width), f32),
                        D((9,))] + pairs,
        compiler_params=pltpu.CompilerParams(collective_id=cid, has_side_effects=True, vmem_limit_bytes=63 << 20),
    )(x, wx, wb, wc, wdt, wz, wo, norm_gain, conv_x, conv_b, conv_c, bias, rate, skip, gain)


def mix_kernel(y_ref, w_hbm, wo_ref, hidden_ref, gain_ref, mixed_ref, normed_ref, w, p, tmp, d1, d2, ysrc, ydst, yb, joint, tmpb, d1b, d2b, whole,
               wsem, s1, r1, s2, r2, sraw, rraw, sy, ry, syb, ryb, s1b, r1b, s2b, r2b, srb, rrb, gs, gr, ls, lr, local):
    high, low = mp_place()
    right, left, far = (low + 1) % 4, (low + 3) % 4, (low + 2) % 4
    me = high * 4 + low
    order = (1 - high, high)
    sides = ((right, left), (left, right))
    n = y_ref.shape[0]
    cols = w_hbm.shape[2]
    place = lax.axis_index("seq")
    spair, sring, score = seq_place()
    na, nb = ydst.shape[1], yb.shape[2]
    ha, hb = na // 2, nb // 2
    f32 = jnp.float32
    rings = (far, right, left, low)
    blocks = [pair * 4 + ring for ring in rings for pair in order]
    loads = [pltpu.make_async_copy(w_hbm.at[pl.ds(2 * b, 2)], w.at[0, pl.ds(2 * b, 2)], wsem.at[i]) for i, b in enumerate(blocks)]
    for load in loads:
        load.start()
    greet(neighbours(mp_names, high, low, 0, False) + neighbours(seq_names, spair, sring, score, True))
    trail = wo_ref.at[:, pl.ds(cols, cols)]
    later = Gather(lambda pair, ring, core, piece: w.at[1, (pair * 4 + ring) * 2 + core, piece], lambda piece: trail.at[piece],
                   seq_names, spair, sring, score, ls, lr, 0, cut(wo_ref.shape[0], 2), True)
    later.begin()
    home = pltpu.make_async_copy(trail, w.at[1, place], local)
    home.start()

    def send(src, dst, pair, ring, ssem, rsem):
        copy = pltpu.make_async_remote_copy(src_ref=src, dst_ref=dst, send_sem=ssem, recv_sem=rsem,
                                            device_id=mp_names(pair, ring, 0), device_id_type=MESH)
        copy.start()
        sent.append(copy)
        return copy

    def product(h, b):
        both = jnp.concatenate([w[h, 2 * b], w[h, 2 * b + 1]], axis=1)
        p[h, b] = jnp.dot(y_ref[...], both, preferred_element_type=f32).astype(p.dtype)

    def start_first(h, k):
        first[h][k] = [send(p.at[h, order[k] * 4 + far, rows(d * ha, ha)], d1.at[h, k, d], high, sides[d][0],
                            s1.at[h, k, d], r1.at[h, k, d]) for d in range(2)]

    def start_raw(h, k, d):
        raw[h][k][d] = send(p.at[h, order[k] * 4 + sides[d][0], rows((1 - d) * ha, ha)],
                            d2.at[h, k, d, rows((1 - d) * ha, ha)], high, sides[d][0], sraw.at[h, k, d], rraw.at[h, k, d])

    def pass_on(h, k):
        result = []
        for d in range(2):
            first[h][k][d].wait_recv()
            here = slice(d * ha, (d + 1) * ha)
            tmp[h, k, d] = (d1[h, k, d].astype(f32) + p[h, order[k] * 4 + sides[d][0], here, :].astype(f32)).astype(tmp.dtype)
            result.append(send(tmp.at[h, k, d], d2.at[h, k, d, rows(d * ha, ha)], high, sides[d][0],
                               s2.at[h, k, d], r2.at[h, k, d]))
        second[h][k] = result

    def total(h, k):
        for d in range(2):
            raw[h][k][d].wait_recv()
            second[h][k][d].wait_recv()
        return p[h, order[k] * 4 + low, 0:na, :].astype(f32) + d2[h, k, 0].astype(f32) + d2[h, k, 1].astype(f32)

    def give(h):
        ysrc[h] = total(h, 0).astype(ysrc.dtype)
        across[h] = send(ysrc.at[h], ydst.at[h], 1 - high, low, sy.at[h], ry.at[h])

    def start_pair(h, i):
        open_pair[h][i] = send(p.at[h, (1 - high) * 4 + rings[i], rows(na, nb)], yb.at[h, i], 1 - high, low,
                               syb.at[h, i], ryb.at[h, i])

    def join(h, i):
        open_pair[h][i].wait_recv()
        value = p[h, high * 4 + rings[i], na:n, :].astype(f32) + yb[h, i].astype(f32)
        if i < 3:
            joint[h, i] = value.astype(joint.dtype)
        return value

    def start_ring(h):
        join(h, 0)
        first_b[h] = [send(joint.at[h, 0, rows(d * hb, hb)], d1b.at[h, d], high, sides[d][0], s1b.at[h, d], r1b.at[h, d])
                      for d in range(2)]
        for d in range(2):
            join(h, 1 + d)
            raw_b[h][d] = send(joint.at[h, 1 + d, rows((1 - d) * hb, hb)], d2b.at[h, d, rows((1 - d) * hb, hb)], high, sides[d][0],
                               srb.at[h, d], rrb.at[h, d])

    def pass_ring(h):
        for d in range(2):
            first_b[h][d].wait_recv()
            tmpb[h, d] = (d1b[h, d].astype(f32) + joint[h, 1 + d, d * hb:(d + 1) * hb, :].astype(f32)).astype(tmpb.dtype)
            second_b[h][d] = send(tmpb.at[h, d], d2b.at[h, d, rows(d * hb, hb)], high, sides[d][0], s2b.at[h, d], r2b.at[h, d])

    def keep(h, start, result):
        here = slice(start, start + result.shape[0])
        for c in range(2):
            lanes = slice((2 * c + h) * cols, (2 * c + h + 1) * cols)
            value = hidden_ref[here, lanes].astype(f32) + result[:, c * cols:(c + 1) * cols]
            mixed_ref[here, lanes] = value
            whole[h, me, here, c * cols:(c + 1) * cols] = value.astype(whole.dtype)

    def close(h):
        own = total(h, 1)
        across[h].wait_recv()
        keep(h, 0, own + ydst[h].astype(f32))
        pair_first[h].begin()

    def close_ring(h):
        own = join(h, 3)
        for d in range(2):
            raw_b[h][d].wait_recv()
            second_b[h][d].wait_recv()
            own = own + d2b[h, d].astype(f32)
        keep(h, na, own)
        ring_first[h].begin()

    sent = []
    first, second = [[None, None] for _ in range(2)], [[None, None] for _ in range(2)]
    raw = [[[None, None], [None, None]] for _ in range(2)]
    across = [None, None]
    open_pair = [[None] * 4 for _ in range(2)]
    first_b, raw_b, second_b = [None, None], [[None, None] for _ in range(2)], [[None, None] for _ in range(2)]

    def gather(kind, index, h, start, size):
        return kind(lambda pair, ring, core, piece: whole.at[h, pair * 4 + ring, piece], lambda piece: whole.at[h, me, piece],
                    mp_names, high, low, 0, gs, gr, index * copies_of(2, False),
                    [pl.ds(start, size), pl.ds(start + size, size)], False)

    pair_first = [gather(Gather, h, h, 0, ha) for h in range(2)]
    ring_first = [gather(RingFirst, 2 + h, h, na, hb) for h in range(2)]
    def issue(h):
        for i, b in enumerate(blocks):
            if h == 0:
                loads[i].wait()
            product(h, b)
            if i % 2 == 0:
                start_pair(h, i // 2)
            if i < 2:
                start_first(h, i)
            elif i < 6:
                start_raw(h, i % 2, i // 2 - 1)

    issue(0)
    pass_on(0, 0)
    later.second(0)
    later.second(1)
    later.forward(0, 0)
    later.forward(0, 1)
    start_ring(0)
    pass_on(0, 1)
    pass_ring(0)
    later.forward(1, 0)
    later.forward(1, 1)
    later.last()
    later.finish()
    home.wait()
    issue(1)
    give(0)
    pass_on(1, 0)
    start_ring(1)
    close_ring(0)
    pass_on(1, 1)
    pass_ring(1)
    close(0)
    ring_first[0].forward(0)
    ring_first[0].forward(1)
    give(1)
    for k in range(2):
        pair_first[0].second(k)
    for k in range(2):
        pair_first[0].forward(0, k)
    close_ring(1)
    ring_first[0].last()
    close(1)
    for k in range(2):
        pair_first[0].forward(1, k)
    ring_first[1].forward(0)
    ring_first[1].forward(1)
    for k in range(2):
        pair_first[1].second(k)
    for k in range(2):
        pair_first[1].forward(0, k)
    ring_first[1].last()
    pair_first[0].last()
    ring_first[0].pairs()
    for k in range(2):
        pair_first[1].forward(1, k)
    pair_first[1].last()
    ring_first[1].pairs()
    wide = whole.shape[3]

    def norm(c, _):
        piece = rows(pl.multiple_of(c * 32, 32), 32)
        square = jnp.zeros((32, wide), f32)
        for b in range(8):
            for h in range(2):
                value = whole[h, b, piece, :].astype(f32)
                square = square + value * value
        scale = lax.rsqrt(jnp.sum(square, axis=1, keepdims=True) / (16 * wide) + 1e-05)
        for b in range(8):
            for h in range(2):
                for q in range(2):
                    start = b * 2 * wide + (2 * q + h) * cols
                    normed_ref[piece, start:start + cols] = (
                        whole[h, b, piece, q * cols:(q + 1) * cols].astype(f32) * scale
                        * gain_ref[:, start:start + cols]).astype(normed_ref.dtype)
        return 0

    lax.fori_loop(0, n // 32, norm, 0)
    for g in pair_first + ring_first:
        g.finish()
    for copy in sent:
        copy.wait_send()


def run_mix(y, w, wo, hidden, gain, cid):
    n, width = hidden.shape
    D = pltpu.SemaphoreType.DMA
    bf = jnp.bfloat16
    V = pltpu.VMEM
    na = n // 8 * 5
    nb = n - na
    lanes = width // 2
    few = 4 * copies_of(2, False)
    fan2 = copies_of(2, True)
    return pl.pallas_call(
        mix_kernel,
        out_shape=(jax.ShapeDtypeStruct((n, width), jnp.float32), jax.ShapeDtypeStruct((n, 8 * width), bf)),
        in_specs=[VM, pl.BlockSpec(memory_space=pl.ANY), VM, VM, VM], out_specs=(VM, VM),
        scratch_shapes=[V((2,) + w.shape, bf), V((2, 8, n, lanes), bf), V((2, 2, 2, na // 2, lanes), bf),
                        V((2, 2, 2, na // 2, lanes), bf), V((2, 2, 2, na, lanes), bf), V((2, na, lanes), bf), V((2, na, lanes), bf),
                        V((2, 4, nb, lanes), bf), V((2, 3, nb, lanes), bf), V((2, 2, nb // 2, lanes), bf),
                        V((2, 2, nb // 2, lanes), bf), V((2, 2, nb, lanes), bf), V((2, 8, n, lanes), bf), D((8,))]
        + [D((2, 2, 2))] * 6 + [D((2,))] * 2 + [D((2, 4))] * 2 + [D((2, 2))] * 6 + [D((few,))] * 2 + [D((fan2,))] * 2 + [D],
        compiler_params=pltpu.CompilerParams(collective_id=cid, has_side_effects=True, vmem_limit_bytes=48 << 20),
    )(y, w, wo, hidden, gain)


def attention_kernel(x_ref, wq_ref, wk_ref, wv_ref, out_ref, own, kv, q, peak, total, local, ss, sr):
    place = lax.axis_index("seq")
    pair, ring, core = seq_place()
    greet(neighbours(seq_names, pair, ring, core, True))
    n = x_ref.shape[0]
    heads = q.shape[0]
    bf, f32 = jnp.bfloat16, jnp.float32
    scale = HD ** -0.5 * 1.4426950408889634
    own[:, 0:HD] = jnp.dot(x_ref[...], wk_ref[...], preferred_element_type=f32).astype(bf)
    own[:, HD:2 * HD] = jnp.dot(x_ref[...], wv_ref[...], preferred_element_type=f32).astype(bf)
    every = Gather(lambda pair, ring, core, piece: kv.at[(pair * 4 + ring) * 2 + core, piece], lambda piece: own.at[piece],
                   seq_names, pair, ring, core, ss, sr, 0, cut(n, 2), True)
    every.begin()
    mine = pltpu.make_async_copy(own, kv.at[place], local)
    mine.start()
    for h in range(0, heads, 2):
        both = jnp.dot(x_ref[...], wq_ref[:, h * HD:(h + 2) * HD], preferred_element_type=f32) * scale
        q[h] = both[:, 0:HD].astype(bf)
        q[h + 1] = both[:, HD:2 * HD].astype(bf)
    peak[...] = jnp.full_like(peak, -1e30)
    total[...] = jnp.zeros_like(total)

    def work(block, bounds):
        keys = block[:, 0:HD]
        both = jnp.concatenate([block[:, HD:2 * HD], jnp.ones((n, HD), bf)], axis=1)
        if bounds is not None:
            away = lax.broadcasted_iota(jnp.int32, (n, n), 1) - lax.broadcasted_iota(jnp.int32, (n, n), 0)
            allowed = (away > bounds[0]) & (away <= bounds[1])
        for h in range(heads):
            scores = lax.dot_general(q[h], keys, (((1,), (1,)), ((), ())), preferred_element_type=f32)
            if bounds is not None:
                scores = jnp.where(allowed, scores, -1e30)
            old = peak[h]
            new = jnp.maximum(old, jnp.max(scores, axis=1, keepdims=True))
            weights = jnp.exp2(scores - new[:, 0:1])
            if bounds is not None:
                weights = jnp.where(allowed, weights, 0.0)
            shrink = jnp.exp2(old - new)
            peak[h] = new
            total[h] = jnp.concatenate([shrink, shrink], axis=1) * total[h] + jnp.dot(
                weights.astype(bf), both, preferred_element_type=f32)

    def visit(count, chip):
        def one(j, _):
            other_pair, other_ring = chip(j // 2)
            which = (other_pair * 4 + other_ring) * 2 + j % 2
            away = place - which

            @pl.when((away >= 1) & (away < WINDOW // n))
            def _():
                work(kv.at[which], None)
            return 0

        lax.fori_loop(0, count, one, 0)

    every.second(0)
    every.second(1)
    every.forward(0, 0)
    every.forward(0, 1)
    mine.wait()

    for copy in every.across[0:4]:
        copy.wait_recv()

    def rim(j, _):
        other_core = jnp.where(j % 2 == 0, core, 1 - core)
        which = (jnp.where(j < 2, pair, 1 - pair) * 4 + ring) * 2 + other_core
        away = place - which

        @pl.when((away >= 0) & (away <= WINDOW // n))
        def _():
            work(kv.at[which], (jnp.where(away == WINDOW // n, 0, -n), jnp.where(away == 0, 0, n)))
        return 0

    lax.fori_loop(0, 4, rim, 0)
    every.forward(1, 0)
    every.forward(1, 1)
    for copy in every.across[4:12]:
        copy.wait_recv()
    visit(8, lambda g: (jnp.where(g % 2 == 0, pair, 1 - pair), (ring + jnp.where(g < 2, 1, 3)) % 4))
    every.last()
    for copy in every.across[12:]:
        copy.wait_recv()
    visit(4, lambda g: (jnp.where(g == 0, pair, 1 - pair), (ring + 2) % 4))
    for copy in every.started:
        copy.wait_send()
    for h in range(heads):
        out_ref[:, h * HD:(h + 1) * HD] = total[h, :, 0:HD] / total[h, :, HD:2 * HD]


def run_attention(x, wq, wk, wv, cid):
    n = x.shape[0]
    width = wq.shape[1]
    heads = width // HD
    D = pltpu.SemaphoreType.DMA
    many = copies_of(2, True)
    bf, f32 = jnp.bfloat16, jnp.float32
    return pl.pallas_call(
        attention_kernel,
        out_shape=jax.ShapeDtypeStruct((n, width), f32),
        in_specs=[VM] * 4, out_specs=VM,
        scratch_shapes=[pltpu.VMEM((n, 2 * HD), bf), pltpu.VMEM((16, n, 2 * HD), bf), pltpu.VMEM((heads, n, HD), bf),
                        pltpu.VMEM((heads, n, HD), f32), pltpu.VMEM((heads, n, 2 * HD), f32), D, D((many,)), D((many,))],
        compiler_params=pltpu.CompilerParams(collective_id=cid, has_side_effects=True, vmem_limit_bytes=40 << 20),
    )(x, wq, wk, wv)


def on_device(hidden_in, norm_gain, w_z, w_x, w_b, w_c, w_dt, conv_x, conv_b, conv_c, dt_bias, a_rate,
              skip_gain, group_gain, w_out, attn_gain, w_q, w_k, w_v):
    y_normed, w_out_half = run_mixer(
        hidden_in, w_x, w_b, w_c, w_dt.T, w_z, w_out, norm_gain[None, :], conv_x, conv_b, conv_c,
        dt_bias[None, :], a_rate[None, :], skip_gain[None, :], group_gain[None, :], 0)
    mixed, normed_two = run_mix(y_normed, w_out_half, w_out, hidden_in, attn_gain[None, :], 1)
    return (mixed, run_attention(normed_two, w_q, w_k, w_v, 2))


def solution(mesh):
    tile, cols = P("seq", "mp"), P(None, "mp")
    placed = (tile, P(), tile, tile, tile, tile, tile, cols, cols, cols, P("mp"), P("mp"), P("mp"), P("mp"),
              P("mp", "seq"), P(), cols, cols, cols)
    return jax.shard_map(on_device, mesh=mesh, in_specs=placed, out_specs=(tile, tile), check_vma=False)
```

```python
import jax
import jax.numpy as jnp
from jax import lax
from jax.experimental import pallas as pl
from jax.experimental.pallas import tpu as pltpu
from jax.sharding import PartitionSpec as P

MESH = pl.DeviceIdType.MESH
VM = pl.BlockSpec(memory_space=pltpu.VMEM)
ANY = pl.BlockSpec(memory_space=pl.ANY)
P_SIZE = 64
N = 128
HD = 128
WINDOW = 4096
QB = 128


def rows(start, size):
    return pl.ds(start, size)


class Gather:
    def __init__(self, view, own, names, pair, ring, core, sends, recvs, base, pieces, fan):
        self.view, self.own, self.names = view, own, names
        self.pair, self.ring, self.core = pair, ring, core
        self.sends, self.recvs, self.next, self.pieces, self.fan = sends, recvs, base, pieces, fan
        self.right, self.left, self.far = (ring + 1) % 4, (ring + 3) % 4, (ring + 2) % 4
        self.started, self.across = [], []
        self.y, self.a, self.b, self.f = {}, {}, {}, []

    def send(self, src, block, piece, pair, ring, core):
        copy = pltpu.make_async_remote_copy(
            src_ref=src, dst_ref=self.view(*block, piece), send_sem=self.sends.at[self.next], recv_sem=self.recvs.at[self.next],
            device_id=self.names(pair, ring, core), device_id_type=MESH)
        self.next += 1
        copy.start()
        self.started.append(copy)
        return copy

    def over(self, src, block, piece):
        if self.fan:
            self.across.append(self.send(src, block, piece, self.pair, self.ring, 1 - self.core))

    def begin_piece(self, k):
        me, piece = (self.pair, self.ring, self.core), self.pieces[k]
        src = self.own(piece)
        self.y[k] = self.send(src, me, piece, 1 - self.pair, self.ring, self.core)
        self.a[k] = [self.send(src, me, piece, self.pair, to, self.core) for to in (self.right, self.left)]
        self.over(src, me, piece)

    def begin(self):
        for k in range(len(self.pieces)):
            self.begin_piece(k)

    def second(self, k):
        piece, block = self.pieces[k], (1 - self.pair, self.ring, self.core)
        self.y[k].wait_recv()
        src = self.view(*block, piece)
        self.b[k] = [self.send(src, block, piece, self.pair, to, self.core) for to in (self.right, self.left)]
        self.over(src, block, piece)

    def forward(self, which, k):
        pair = self.pair if which == 0 else 1 - self.pair
        piece, first = self.pieces[k], k < len(self.pieces) // 2
        for d, (to, origin) in enumerate(((self.right, self.left), (self.left, self.right))):
            (self.a, self.b)[which][k][d].wait_recv()
            block = (pair, origin, self.core)
            src = self.view(*block, piece)
            if first == (d == 0):
                self.f.append((self.send(src, block, piece, self.pair, to, self.core), (pair, self.far, self.core), piece))
            self.over(src, block, piece)

    def last(self):
        for copy, block, piece in self.f:
            copy.wait_recv()
            self.over(self.view(*block, piece), block, piece)

    def finish(self):
        for copy in self.across:
            copy.wait_recv()
        for copy in self.started:
            copy.wait_send()


def copies_of(pieces, fan):
    return pieces * (7 + (8 if fan else 0))


def seq_names(pair, ring, core):
    return {"seq": (pair * 4 + ring) * 2 + core}


def mp_names(pair, ring, core):
    return {"mp": pair * 4 + ring}


def greet(ids):
    barrier = pltpu.get_barrier_semaphore()
    for other in ids:
        pl.semaphore_signal(barrier, inc=1, device_id=other, device_id_type=MESH)
    pl.semaphore_wait(barrier, len(ids))


def seq_place():
    me = lax.axis_index("seq")
    return me // 8, (me // 2) % 4, me % 2


def mp_place():
    me = lax.axis_index("mp")
    return me // 4, me % 4


def neighbours(names, pair, ring, core, fan):
    ids = [names(1 - pair, ring, core), names(pair, (ring + 1) % 4, core), names(pair, (ring + 3) % 4, core)]
    return ids + ([names(pair, ring, 1 - core)] if fan else [])


def cut(total, count):
    return [pl.ds(k * (total // count), total // count) for k in range(count)]


def write_normed(whole, gain_ref, normed_ref, start, count, size):
    blocks, _, wide = whole.shape

    def norm(c, _):
        piece = rows(pl.multiple_of(start + c * size, 16), size)
        square = jnp.zeros((size, wide), jnp.float32)
        for b in range(blocks):
            value = whole[b, piece, :].astype(jnp.float32)
            square = square + value * value
        scale = lax.rsqrt(jnp.sum(square, axis=1, keepdims=True) / (blocks * wide) + 1e-05)
        for b in range(blocks):
            lanes = slice(b * wide, (b + 1) * wide)
            normed_ref[piece, lanes] = (whole[b, piece, :].astype(jnp.float32) * scale * gain_ref[:, lanes]).astype(normed_ref.dtype)
        return 0

    lax.fori_loop(0, count // size, norm, 0)


class RingFirst(Gather):
    def begin(self):
        me = (self.pair, self.ring, self.core)
        self.pairs_open = []
        for k, piece in enumerate(self.pieces):
            src = self.own(piece)
            self.a[k] = [self.send(src, me, piece, self.pair, to, self.core) for to in (self.right, self.left)]
            self.pairs_open.append((self.send(src, me, piece, 1 - self.pair, self.ring, self.core), self.ring, piece))
            self.over(src, me, piece)

    def beside(self, src, block, piece):
        self.pairs_open.append((self.send(src, block, piece, 1 - self.pair, self.ring, self.core), block[1], piece))
        self.over(src, block, piece)

    def forward(self, k):
        piece, first = self.pieces[k], k < len(self.pieces) // 2
        for d, (to, origin) in enumerate(((self.right, self.left), (self.left, self.right))):
            self.a[k][d].wait_recv()
            block = (self.pair, origin, self.core)
            src = self.view(*block, piece)
            if first == (d == 0):
                self.f.append((self.send(src, block, piece, self.pair, to, self.core), (self.pair, self.far, self.core), piece))
            self.beside(src, block, piece)

    def last(self):
        for copy, block, piece in self.f:
            copy.wait_recv()
            self.beside(self.view(*block, piece), block, piece)

    def pairs(self):
        for copy, ring, piece in self.pairs_open:
            copy.wait_recv()
            block = (1 - self.pair, ring, self.core)
            self.over(self.view(*block, piece), block, piece)


def three_terms(decay):
    bf, f32 = jnp.bfloat16, jnp.float32
    big = decay.astype(bf).astype(f32)
    middle = (decay - big).astype(bf).astype(f32)
    small = (decay - big - middle).astype(bf).astype(f32)
    which = lax.broadcasted_iota(jnp.int32, decay.shape, 0)
    return jnp.where(which == 0, big, jnp.where(which == 1, middle, small)).astype(bf)


def decay_of(block):
    tail = block.astype(jnp.float32)
    return tail[0:1] + (tail[1:2] + tail[2:3])


def mixer_kernel(x_ref, wx_ref, wb_ref, wc_ref, wdt_ref, wz_ref, wo_ref, norm_ref, cx_ref, cb_ref, cc_ref, bias_ref, rate_ref,
                 skip_ref, gain_ref,
                 out_ref, woa, wbc, vectors, wda, whole, normed, wxa, wba, wza, padx, padbc, bcd, y, gate, state, cc, cumul, tail, mine, theirs,
                 agg, aggs, turn, half_in, half_out, incoming, local, ts, tr, hs, hr, es, er, ds, dr, bs, br, xs, xr, zs, zr, os, orr, gs, gr):
    bf, f32 = jnp.bfloat16, jnp.float32
    mpair, mring = mp_place()
    pair, ring, core = seq_place()
    place = lax.axis_index("seq")
    following, previous = (place + 1) % 16, (place + 15) % 16
    joined = [pltpu.make_async_copy(wb_ref, wbc.at[:, pl.ds(0, N)], local.at[6]),
              pltpu.make_async_copy(wc_ref, wbc.at[:, pl.ds(N, N)], local.at[7])]
    for copy in joined:
        copy.start()
    greet(neighbours(mp_names, mpair, mring, 0, False) + neighbours(seq_names, pair, ring, core, True)
          + [{"seq": following}, {"seq": previous}])
    n = x_ref.shape[0]
    depth, tall = wx_ref.shape[0], wo_ref.shape[0]
    count = n // QB
    width = wx_ref.shape[1]

    def wide_view(ref):
        return lambda pair, ring, core, piece: ref.at[pl.ds(((pair * 4 + ring) * 2 + core) * depth + piece.start, piece.size), :]

    def seq_gather(kind, view, own, sends, recvs, base, pieces, fan=True):
        return kind(view, lambda piece: own.at[piece], seq_names, pair, ring, core, sends, recvs, base, pieces, fan)

    def mp_view(pair, ring, core, piece):
        return whole.at[pair * 4 + ring, piece]

    hidden = Gather(mp_view, lambda piece: x_ref.at[piece], mp_names, mpair, mring, 0, hs, hr, 0, cut(n, 2), False)
    edge = Gather(mp_view, lambda piece: tail, mp_names, mpair, mring, 0, es, er, 0, [pl.ds(n, 16)], False)
    small = seq_gather(Gather, wide_view(wba), wbc, bs, br, 0, cut(depth, 2))

    def step_view(pair, ring, core, piece):
        return wda.at[:, pl.ds(((pair * 4 + ring) * 2 + core) * depth, depth)]

    steps = Gather(step_view, lambda piece: wdt_ref, seq_names, pair, ring, core, ds, dr, 0, [None], True)
    big = seq_gather(Gather, wide_view(wxa), wx_ref, xs, xr, 0, cut(depth, 2))
    fan2 = copies_of(2, True)
    quarters, parts = cut(depth, 4), cut(tall, 4)
    z_pair = seq_gather(Gather, wide_view(wza), wz_ref, zs, zr, 0, quarters[0:2])
    z_ring = seq_gather(RingFirst, wide_view(wza), wz_ref, zs, zr, fan2, quarters[2:4])

    def out_view(pair, ring, core, piece):
        return woa.at[(pair * 4 + ring) * 2 + core, piece]

    lead = wo_ref.at[:, pl.ds(0, wo_ref.shape[1] // 2)]
    o_pair = seq_gather(Gather, out_view, lead, os, orr, 0, parts[0:2])
    o_ring = seq_gather(RingFirst, out_view, lead, os, orr, fan2, parts[2:4])
    own_rows = pl.ds(place * depth, depth)
    at_home = [pltpu.make_async_copy(x_ref, whole.at[mpair * 4 + mring, pl.ds(0, n)], local.at[0]),
               pltpu.make_async_copy(wx_ref, wxa.at[own_rows, :], local.at[1]),
               pltpu.make_async_copy(wbc, wba.at[own_rows, :], local.at[2]),
               pltpu.make_async_copy(wdt_ref, wda.at[:, own_rows], local.at[8]),
               pltpu.make_async_copy(wz_ref, wza.at[own_rows, :], local.at[3]),
               pltpu.make_async_copy(lead, woa.at[place], local.at[4])]

    def to_device(src, dst, index, device):
        copy = pltpu.make_async_remote_copy(src_ref=src, dst_ref=dst, send_sem=ts.at[index], recv_sem=tr.at[index],
                                            device_id=device, device_id_type=MESH)
        copy.start()
        return copy

    shifted = to_device(x_ref.at[pl.ds(n - 16, 16)], tail, 0, {"seq": following})
    for copy in joined:
        copy.wait()
    steps.begin()
    small.begin()
    for k in range(2):
        big.begin_piece(k)
        hidden.begin_piece(k)
    for copy in at_home:
        copy.start()
    shifted.wait_recv()
    edge.begin()
    home_tail = pltpu.make_async_copy(tail, whole.at[mpair * 4 + mring, pl.ds(n, 16)], local.at[5])
    home_tail.start()
    steps.second(0)
    small.second(0)
    small.second(1)
    for k in range(2):
        big.second(k)
        small.forward(0, k)
        hidden.forward(0, k)
        big.forward(0, k)
        hidden.second(k)
    steps.forward(0, 0)
    steps.forward(1, 0)
    edge.second(0)
    edge.forward(0, 0)
    small.forward(1, 0)
    small.forward(1, 1)
    for k in range(2):
        hidden.forward(1, k)
        big.forward(1, k)
    edge.forward(1, 0)
    z_ring.begin()
    z_pair.begin()
    hidden.last()
    edge.last()
    at_home[0].wait()
    home_tail.wait()
    write_normed(whole, norm_ref, normed, 0, n, 32)
    write_normed(whole, norm_ref, normed, n, 16, 16)
    vectors[...] = jnp.zeros_like(vectors)
    vectors[0:1, 0:bias_ref.shape[1]] = bias_ref[...]
    vectors[1:2, 0:rate_ref.shape[1]] = rate_ref[...]
    bcd[...] = jnp.zeros_like(bcd)
    small.last()
    steps.last()
    small.finish()
    steps.finish()
    at_home[2].wait()
    at_home[3].wait()
    inside = jnp.where(place > 0, 1.0, 0.0)
    product = jnp.dot(normed[...], wba[...], preferred_element_type=f32)
    bcd[:, 0:bias_ref.shape[1]] = lax.dot_general(
        normed[0:n, :], wda[...], (((1,), (1,)), ((), ())), preferred_element_type=f32)
    padbc[pl.ds(8, n), :] = product[0:n]
    padbc[pl.ds(0, 8), :] = product[n + 8:n + 16] * inside
    z_pair.second(0)
    z_pair.second(1)
    big.last()
    big.finish()
    at_home[1].wait()
    for part in range(4):
        lanes = slice(part * 256, (part + 1) * 256)
        product = jnp.dot(normed[...], wxa[:, lanes], preferred_element_type=f32)
        padx[pl.ds(8, n), lanes] = product[0:n]
        padx[pl.ds(0, 8), lanes] = product[n + 8:n + 16] * inside
    z_ring.forward(0)
    z_ring.forward(1)

    state[...] = jnp.zeros_like(state)
    row = lax.broadcasted_iota(jnp.int32, (QB, QB), 0)
    col = lax.broadcasted_iota(jnp.int32, (QB, QB), 1)
    causal = row >= col
    tri = jnp.where(causal, 1.0, 0.0).astype(f32)
    low = col < P_SIZE

    def conv(pad, taps, start, lanes, tap_lanes):
        whole_rows = pad[pl.ds(start, QB + 8), lanes]
        total = taps[0:1, tap_lanes] * whole_rows[5:5 + QB]
        for j in range(1, 4):
            total = total + taps[j:j + 1, tap_lanes] * whole_rows[5 + j:5 + j + QB]
        return total / (1.0 + jnp.exp(-total))

    def one(c, before):
        start = pl.multiple_of(c * QB, QB)
        here = pl.ds(start, QB)
        bv = conv(padbc, cb_ref, start, slice(0, N), slice(0, N))
        cv = conv(padbc, cc_ref, start, slice(N, 2 * N), slice(0, N)).astype(bf)
        cc[here, :] = cv
        raw = bcd[here, :] + vectors[0:1, :]
        step = jnp.maximum(raw, 0.0) + jnp.log1p(jnp.exp(-jnp.abs(raw)))
        decay = -vectors[1:2, :] * step
        cum = jnp.dot(tri, decay, precision=lax.Precision.HIGHEST, preferred_element_type=f32)
        cumul[here, :] = cum + before
        cum_t, step_t = cum.T, step.T
        last = cum[QB - 1:QB, :]
        bt = bv.T.astype(bf)
        affinity = jnp.dot(cv, bt, preferred_element_type=f32)
        for p in range(width // 128):
            lanes = slice(p * 128, (p + 1) * 128)
            xv = conv(padx, cx_ref, start, lanes, lanes)
            mixes, grown, tails, ends = [], [], [], []
            for h in (2 * p, 2 * p + 1):
                ct = jnp.broadcast_to(cum[:, h:h + 1], (QB, QB))
                st = jnp.broadcast_to(step[:, h:h + 1], (QB, QB))
                end = jnp.broadcast_to(last[:, h:h + 1], (1, QB))
                spread = jnp.where(causal, ct - cum_t[h:h + 1, :], -jnp.inf)
                mixes.append((affinity * jnp.exp(spread) * step_t[h:h + 1, :]).astype(bf))
                grown.append(ct)
                tails.append(jnp.exp(end - ct) * st)
                ends.append(end)
            mixed = jnp.concatenate(mixes, axis=1)
            xs2 = jnp.concatenate([jnp.where(low, xv, 0.0).astype(bf), jnp.where(low, 0.0, xv).astype(bf)], axis=0)
            out = jnp.dot(mixed, xs2, preferred_element_type=f32)
            old = state[:, lanes]
            carried = jnp.dot(cv, old.astype(bf), preferred_element_type=f32)
            out = out + jnp.exp(jnp.where(low, grown[0], grown[1])) * carried
            skips = [jnp.broadcast_to(skip_ref[:, h:h + 1], (1, QB)) for h in (2 * p, 2 * p + 1)]
            y[here, lanes] = out + jnp.where(low[0:1], skips[0], skips[1]) * xv
            weighted = (xv * jnp.where(low, tails[0], tails[1])).astype(bf)
            fresh = jnp.dot(bt, weighted, preferred_element_type=f32)
            state[:, lanes] = jnp.exp(jnp.where(low[0:1], ends[0], ends[1])) * old + fresh
        return before + last

    total = lax.fori_loop(0, count, one, jnp.zeros((1, 128), f32))
    mine[0:N, :] = state[...].astype(bf)
    for p in range(width // 128):
        lanes = slice(p * 128, (p + 1) * 128)
        ends = [jnp.broadcast_to(total[:, h:h + 1], (16, 128)) for h in (2 * p, 2 * p + 1)]
        mine[N:N + 16, lanes] = three_terms(jnp.exp(jnp.where(low[0:16], ends[0], ends[1])))
    swapped = to_device(mine, theirs, 1, {"seq": place + 1 - 2 * core})
    for which in range(2):
        for k in range(2):
            z_pair.forward(which, k)
    swapped.wait_recv()
    half = width // 2
    ours = pl.ds(pl.multiple_of(core * half, half), half)
    rest = pl.ds(pl.multiple_of((1 - core) * half, half), half)
    a, b = mine[:, ours].astype(f32), theirs[:, ours].astype(f32)
    head = core == 0
    early, late = jnp.where(head, a, b), jnp.where(head, b, a)
    early_decay, late_decay = decay_of(early[N:N + 16]), decay_of(late[N:N + 16])
    agg[0:N, :] = (late_decay * early[0:N] + late[0:N]).astype(bf)
    agg[N:N + 16, :] = three_terms(jnp.broadcast_to(early_decay * late_decay, (16, half)))
    chip = pair * 4 + ring
    chips = Gather(lambda pair, ring, core, piece: aggs.at[pair * 4 + ring, piece], lambda piece: agg.at[piece], seq_names,
                   pair, ring, core, gs, gr, 0, [pl.ds(0, 80), pl.ds(80, N + 16 - 80)], False)
    chips.begin()
    o_ring.begin()
    o_pair.begin()
    z_ring.last()
    chips.second(0)
    chips.second(1)
    z_pair.last()
    o_pair.second(0)
    o_pair.second(1)
    for which in range(2):
        for k in range(2):
            chips.forward(which, k)
    z_ring.pairs()
    o_ring.forward(0)
    o_ring.forward(1)
    z_pair.finish()
    z_ring.finish()
    at_home[4].wait()

    def open_gate(part):
        lanes = slice(part * 256, (part + 1) * 256)
        gate[:, lanes] = jnp.dot(normed[0:n, :], wza[:, lanes], preferred_element_type=f32)

    open_gate(0)
    o_pair.forward(0, 0)
    o_pair.forward(0, 1)
    open_gate(1)
    chips.last()
    half_out[...] = jnp.zeros_like(half_out)

    def add(k, _):
        half_out[...] = decay_of(aggs[k, N:N + 16, :]) * half_out[...] + aggs[k, 0:N, :].astype(f32)
        return 0

    lax.fori_loop(0, chip, add, 0)
    turn[...] = half_out[...].astype(bf)
    given = to_device(turn, half_in, 2, {"seq": place + 1 - 2 * core})
    o_pair.forward(1, 0)
    o_pair.forward(1, 1)
    open_gate(2)
    o_ring.last()
    open_gate(3)
    given.wait_recv()
    incoming[:, ours] = half_out[...]
    incoming[:, rest] = half_in[...].astype(f32)
    keep = jnp.where(head, 0.0, 1.0)
    before = theirs[N:N + 16, :].astype(f32)
    before_decay = jnp.where(head, 1.0, before[0:1] + (before[1:2] + before[2:3]))
    incoming[...] = before_decay * incoming[...] + keep * theirs[0:N, :].astype(f32)
    low_rows = low

    def close(c, _):
        here = pl.ds(pl.multiple_of(c * QB, QB), QB)
        cv = cc[here, :]
        cum = cumul[here, :]
        square = jnp.zeros((QB, 128), f32)
        for p in range(width // 128):
            lanes = slice(p * 128, (p + 1) * 128)
            ct = jnp.where(low_rows, jnp.broadcast_to(cum[:, 2 * p:2 * p + 1], (QB, 128)),
                           jnp.broadcast_to(cum[:, 2 * p + 1:2 * p + 2], (QB, 128)))
            carried = jnp.dot(cv, incoming[:, lanes].astype(bf), preferred_element_type=f32)
            g = gate[here, lanes]
            value = (y[here, lanes] + jnp.exp(ct) * carried) * (g / (1.0 + jnp.exp(-g)))
            gate[here, lanes] = value
            square = square + value * value
        scale = lax.rsqrt(jnp.sum(square, axis=1, keepdims=True) / width + 1e-05)
        out_ref[here, :] = (gate[here, :] * scale * gain_ref[...]).astype(bf)
        return 0

    lax.fori_loop(0, count, close, 0)
    o_pair.last()
    o_ring.pairs()
    for g in (o_pair, o_ring, hidden, edge, chips):
        g.finish()
    at_home[5].wait()
    for copy in (shifted, swapped, given):
        copy.wait_send()


def run_mixer(x, wx, wb, wc, wdt, wz, wo, norm_gain, conv_x, conv_b, conv_c, bias, rate, skip, gain, cid):
    n, w = x.shape
    depth, width = wx.shape
    tall, cols = wo.shape
    D, V = pltpu.SemaphoreType.DMA, pltpu.VMEM
    bf, f32 = jnp.bfloat16, jnp.float32
    fan2, plain2 = copies_of(2, True), copies_of(2, False)
    pairs = []
    for size in (3, plain2, copies_of(1, False), copies_of(1, True), fan2, fan2, 2 * fan2, 2 * fan2, plain2):
        pairs += [D((size,)), D((size,))]
    return pl.pallas_call(
        mixer_kernel,
        out_shape=(jax.ShapeDtypeStruct((n, width), bf), jax.ShapeDtypeStruct((16, tall, cols // 2), bf)),
        in_specs=[VM] * 15, out_specs=(VM, VM),
        scratch_shapes=[V((depth, 2 * N), bf), V((8, 128), f32), V((16, 16 * depth), bf),
                        V((8, n + 16, w), bf), V((n + 16, 8 * w), bf), V((16 * depth, width), bf), V((16 * depth, 2 * N), bf),
                        V((16 * depth, width), bf), V((n + 8, width), f32), V((n + 8, 2 * N), f32), V((n, N), f32),
                        V((n, width), f32), V((n, width), f32), V((N, width), f32), V((n, N), bf), V((n, 128), f32),
                        V((16, w), bf), V((N + 16, width), bf), V((N + 16, width), bf), V((N + 16, width // 2), bf),
                        V((8, N + 16, width // 2), bf), V((N, width // 2), bf), V((N, width // 2), bf), V((N, width // 2), f32), V((N, width), f32),
                        D((9,))] + pairs,
        compiler_params=pltpu.CompilerParams(collective_id=cid, has_side_effects=True, vmem_limit_bytes=63 << 20),
    )(x, wx, wb, wc, wdt, wz, wo, norm_gain, conv_x, conv_b, conv_c, bias, rate, skip, gain)


def mix_kernel(y_hbm, w_hbm, wo_ref, hidden_hbm, gain_hbm, mixed_ref, normed_ref, y_ref, gain_ref, hidden_ref, w, p, tmp, d1, d2, ysrc, ydst, yb, joint, tmpb, d1b, d2b, whole,
               wsem, s1, r1, s2, r2, sraw, rraw, sy, ry, syb, ryb, s1b, r1b, s2b, r2b, srb, rrb, gs, gr, ls, lr, local):
    high, low = mp_place()
    right, left, far = (low + 1) % 4, (low + 3) % 4, (low + 2) % 4
    me = high * 4 + low
    order = (1 - high, high)
    sides = ((right, left), (left, right))
    n = y_ref.shape[0]
    cols = w_hbm.shape[2]
    place = lax.axis_index("seq")
    spair, sring, score = seq_place()
    na, nb = ydst.shape[1], yb.shape[2]
    ha, hb = na // 2, nb // 2
    f32 = jnp.float32
    rings = (far, right, left, low)
    blocks = [pair * 4 + ring for ring in rings for pair in order]
    loads = [pltpu.make_async_copy(w_hbm.at[pl.ds(2 * b, 2)], w.at[0, pl.ds(2 * b, 2)], wsem.at[i]) for i, b in enumerate(blocks)]
    arriving = pltpu.make_async_copy(y_hbm, y_ref, local.at[2])
    arriving.start()
    for load in loads:
        load.start()
    greet(neighbours(mp_names, high, low, 0, False) + neighbours(seq_names, spair, sring, score, True))
    trail = wo_ref.at[:, pl.ds(cols, cols)]
    later = Gather(lambda pair, ring, core, piece: w.at[1, (pair * 4 + ring) * 2 + core, piece], lambda piece: trail.at[piece],
                   seq_names, spair, sring, score, ls, lr, 0, cut(wo_ref.shape[0], 2), True)
    later.begin()
    home = pltpu.make_async_copy(trail, w.at[1, place], local.at[0])
    home.start()
    fetched = [pltpu.make_async_copy(hidden_hbm, hidden_ref, local.at[1]), pltpu.make_async_copy(gain_hbm, gain_ref, local.at[3])]
    for copy in fetched:
        copy.start()
    arriving.wait()

    def send(src, dst, pair, ring, ssem, rsem):
        copy = pltpu.make_async_remote_copy(src_ref=src, dst_ref=dst, send_sem=ssem, recv_sem=rsem,
                                            device_id=mp_names(pair, ring, 0), device_id_type=MESH)
        copy.start()
        sent.append(copy)
        return copy

    def product(h, b):
        both = jnp.concatenate([w[h, 2 * b], w[h, 2 * b + 1]], axis=1)
        p[h, b] = jnp.dot(y_ref[...], both, preferred_element_type=f32).astype(p.dtype)

    def start_first(h, k):
        first[h][k] = [send(p.at[h, order[k] * 4 + far, rows(d * ha, ha)], d1.at[h, k, d], high, sides[d][0],
                            s1.at[h, k, d], r1.at[h, k, d]) for d in range(2)]

    def start_raw(h, k, d):
        raw[h][k][d] = send(p.at[h, order[k] * 4 + sides[d][0], rows((1 - d) * ha, ha)],
                            d2.at[h, k, d, rows((1 - d) * ha, ha)], high, sides[d][0], sraw.at[h, k, d], rraw.at[h, k, d])

    def pass_on(h, k):
        result = []
        for d in range(2):
            first[h][k][d].wait_recv()
            here = slice(d * ha, (d + 1) * ha)
            tmp[h, k, d] = (d1[h, k, d].astype(f32) + p[h, order[k] * 4 + sides[d][0], here, :].astype(f32)).astype(tmp.dtype)
            result.append(send(tmp.at[h, k, d], d2.at[h, k, d, rows(d * ha, ha)], high, sides[d][0],
                               s2.at[h, k, d], r2.at[h, k, d]))
        second[h][k] = result

    def total(h, k):
        for d in range(2):
            raw[h][k][d].wait_recv()
            second[h][k][d].wait_recv()
        return p[h, order[k] * 4 + low, 0:na, :].astype(f32) + d2[h, k, 0].astype(f32) + d2[h, k, 1].astype(f32)

    def give(h):
        ysrc[h] = total(h, 0).astype(ysrc.dtype)
        across[h] = send(ysrc.at[h], ydst.at[h], 1 - high, low, sy.at[h], ry.at[h])

    def start_pair(h, i):
        open_pair[h][i] = send(p.at[h, (1 - high) * 4 + rings[i], rows(na, nb)], yb.at[h, i], 1 - high, low,
                               syb.at[h, i], ryb.at[h, i])

    def join(h, i):
        open_pair[h][i].wait_recv()
        value = p[h, high * 4 + rings[i], na:n, :].astype(f32) + yb[h, i].astype(f32)
        if i < 3:
            joint[h, i] = value.astype(joint.dtype)
        return value

    def start_ring(h):
        join(h, 0)
        first_b[h] = [send(joint.at[h, 0, rows(d * hb, hb)], d1b.at[h, d], high, sides[d][0], s1b.at[h, d], r1b.at[h, d])
                      for d in range(2)]
        for d in range(2):
            join(h, 1 + d)
            raw_b[h][d] = send(joint.at[h, 1 + d, rows((1 - d) * hb, hb)], d2b.at[h, d, rows((1 - d) * hb, hb)], high, sides[d][0],
                               srb.at[h, d], rrb.at[h, d])

    def pass_ring(h):
        for d in range(2):
            first_b[h][d].wait_recv()
            tmpb[h, d] = (d1b[h, d].astype(f32) + joint[h, 1 + d, d * hb:(d + 1) * hb, :].astype(f32)).astype(tmpb.dtype)
            second_b[h][d] = send(tmpb.at[h, d], d2b.at[h, d, rows(d * hb, hb)], high, sides[d][0], s2b.at[h, d], r2b.at[h, d])

    def keep(h, start, result):
        here = slice(start, start + result.shape[0])
        for c in range(2):
            lanes = slice((2 * c + h) * cols, (2 * c + h + 1) * cols)
            value = hidden_ref[here, lanes].astype(f32) + result[:, c * cols:(c + 1) * cols]
            mixed_ref[here, lanes] = value
            whole[h, me, here, c * cols:(c + 1) * cols] = value.astype(whole.dtype)

    def close(h):
        own = total(h, 1)
        across[h].wait_recv()
        keep(h, 0, own + ydst[h].astype(f32))
        pair_first[h].begin()

    def close_ring(h):
        own = join(h, 3)
        for d in range(2):
            raw_b[h][d].wait_recv()
            second_b[h][d].wait_recv()
            own = own + d2b[h, d].astype(f32)
        keep(h, na, own)
        ring_first[h].begin()

    sent = []
    first, second = [[None, None] for _ in range(2)], [[None, None] for _ in range(2)]
    raw = [[[None, None], [None, None]] for _ in range(2)]
    across = [None, None]
    open_pair = [[None] * 4 for _ in range(2)]
    first_b, raw_b, second_b = [None, None], [[None, None] for _ in range(2)], [[None, None] for _ in range(2)]

    def gather(kind, index, h, start, size):
        return kind(lambda pair, ring, core, piece: whole.at[h, pair * 4 + ring, piece], lambda piece: whole.at[h, me, piece],
                    mp_names, high, low, 0, gs, gr, index * copies_of(2, False),
                    [pl.ds(start, size), pl.ds(start + size, size)], False)

    pair_first = [gather(Gather, h, h, 0, ha) for h in range(2)]
    ring_first = [gather(RingFirst, 2 + h, h, na, hb) for h in range(2)]
    def issue(h):
        for i, b in enumerate(blocks):
            if h == 0:
                loads[i].wait()
            product(h, b)
            if i % 2 == 0:
                start_pair(h, i // 2)
            if i < 2:
                start_first(h, i)
            elif i < 6:
                start_raw(h, i % 2, i // 2 - 1)

    issue(0)
    pass_on(0, 0)
    later.second(0)
    later.second(1)
    later.forward(0, 0)
    later.forward(0, 1)
    start_ring(0)
    pass_on(0, 1)
    pass_ring(0)
    give(0)
    later.forward(1, 0)
    later.forward(1, 1)
    for copy in fetched:
        copy.wait()
    close_ring(0)
    close(0)
    later.last()
    ring_first[0].forward(0)
    ring_first[0].forward(1)
    for copy in later.across:
        copy.wait_recv()
    home.wait()
    issue(1)
    for k in range(2):
        pair_first[0].second(k)
    pass_on(1, 0)
    start_ring(1)
    pass_on(1, 1)
    pass_ring(1)
    for k in range(2):
        pair_first[0].forward(0, k)
    ring_first[0].last()
    give(1)
    close_ring(1)
    for k in range(2):
        pair_first[0].forward(1, k)
    close(1)
    ring_first[1].forward(0)
    ring_first[1].forward(1)
    for k in range(2):
        pair_first[1].second(k)
    for k in range(2):
        pair_first[1].forward(0, k)
    ring_first[1].last()
    pair_first[0].last()
    ring_first[0].pairs()
    for k in range(2):
        pair_first[1].forward(1, k)
    pair_first[1].last()
    ring_first[1].pairs()
    wide = whole.shape[3]

    def norm(c, _):
        piece = rows(pl.multiple_of(c * 32, 32), 32)
        square = jnp.zeros((32, wide), f32)
        for b in range(8):
            for h in range(2):
                value = whole[h, b, piece, :].astype(f32)
                square = square + value * value
        scale = lax.rsqrt(jnp.sum(square, axis=1, keepdims=True) / (16 * wide) + 1e-05)
        for b in range(8):
            for h in range(2):
                for q in range(2):
                    start = b * 2 * wide + (2 * q + h) * cols
                    normed_ref[piece, start:start + cols] = (
                        whole[h, b, piece, q * cols:(q + 1) * cols].astype(f32) * scale
                        * gain_ref[:, start:start + cols]).astype(normed_ref.dtype)
        return 0

    lax.fori_loop(0, n // 32, norm, 0)
    for g in pair_first + ring_first:
        g.finish()
    for copy in sent + later.started:
        copy.wait_send()


def run_mix(y, w, wo, hidden, gain, cid):
    n, width = hidden.shape
    D = pltpu.SemaphoreType.DMA
    bf = jnp.bfloat16
    V = pltpu.VMEM
    na = n // 8 * 5
    nb = n - na
    lanes = width // 2
    few = 4 * copies_of(2, False)
    fan2 = copies_of(2, True)
    return pl.pallas_call(
        mix_kernel,
        out_shape=(jax.ShapeDtypeStruct((n, width), jnp.float32), jax.ShapeDtypeStruct((n, 8 * width), bf)),
        in_specs=[ANY] * 5, out_specs=(VM, VM),
        scratch_shapes=[V(y.shape, bf), V(gain.shape, jnp.float32), V((n, width), bf), V((2,) + w.shape, bf), V((2, 8, n, lanes), bf), V((2, 2, 2, na // 2, lanes), bf),
                        V((2, 2, 2, na // 2, lanes), bf), V((2, 2, 2, na, lanes), bf), V((2, na, lanes), bf), V((2, na, lanes), bf),
                        V((2, 4, nb, lanes), bf), V((2, 3, nb, lanes), bf), V((2, 2, nb // 2, lanes), bf),
                        V((2, 2, nb // 2, lanes), bf), V((2, 2, nb, lanes), bf), V((2, 8, n, lanes), bf), D((8,))]
        + [D((2, 2, 2))] * 6 + [D((2,))] * 2 + [D((2, 4))] * 2 + [D((2, 2))] * 6 + [D((few,))] * 2 + [D((fan2,))] * 2 + [D((4,))],
        compiler_params=pltpu.CompilerParams(collective_id=cid, has_side_effects=True, vmem_limit_bytes=63 << 20),
    )(y, w, wo, hidden, gain)


def attention_kernel(x_hbm, wq_hbm, wk_hbm, wv_hbm, out_ref, x_ref, wq_ref, wk_ref, wv_ref, wsem, own, kv, q, peak, total, local, ss, sr):
    place = lax.axis_index("seq")
    pair, ring, core = seq_place()
    loads = [pltpu.make_async_copy(src, dst, wsem.at[i])
             for i, (src, dst) in enumerate(((x_hbm, x_ref), (wk_hbm, wk_ref), (wv_hbm, wv_ref), (wq_hbm, wq_ref)))]
    for load in loads:
        load.start()
    greet(neighbours(seq_names, pair, ring, core, True))
    n = x_ref.shape[0]
    heads = q.shape[0]
    bf, f32 = jnp.bfloat16, jnp.float32
    scale = HD ** -0.5 * 1.4426950408889634
    loads[0].wait()
    loads[1].wait()
    own[:, 0:HD] = jnp.dot(x_ref[...], wk_ref[...], preferred_element_type=f32).astype(bf)
    loads[2].wait()
    own[:, HD:2 * HD] = jnp.dot(x_ref[...], wv_ref[...], preferred_element_type=f32).astype(bf)
    every = Gather(lambda pair, ring, core, piece: kv.at[(pair * 4 + ring) * 2 + core, piece], lambda piece: own.at[piece],
                   seq_names, pair, ring, core, ss, sr, 0, cut(n, 2), True)
    every.begin()
    mine = pltpu.make_async_copy(own, kv.at[place], local)
    mine.start()
    loads[3].wait()
    for h in range(0, heads, 2):
        both = jnp.dot(x_ref[...], wq_ref[:, h * HD:(h + 2) * HD], preferred_element_type=f32) * scale
        q[h] = both[:, 0:HD].astype(bf)
        q[h + 1] = both[:, HD:2 * HD].astype(bf)
    peak[...] = jnp.full_like(peak, -1e30)
    total[...] = jnp.zeros_like(total)

    def work(block, bounds):
        keys = block[:, 0:HD]
        both = jnp.concatenate([block[:, HD:2 * HD], jnp.ones((n, HD), bf)], axis=1)
        if bounds is not None:
            away = lax.broadcasted_iota(jnp.int32, (n, n), 1) - lax.broadcasted_iota(jnp.int32, (n, n), 0)
            allowed = (away > bounds[0]) & (away <= bounds[1])
        for h in range(heads):
            scores = lax.dot_general(q[h], keys, (((1,), (1,)), ((), ())), preferred_element_type=f32)
            if bounds is not None:
                scores = jnp.where(allowed, scores, -1e30)
            old = peak[h]
            new = jnp.maximum(old, jnp.max(scores, axis=1, keepdims=True))
            weights = jnp.exp2(scores - new[:, 0:1])
            if bounds is not None:
                weights = jnp.where(allowed, weights, 0.0)
            shrink = jnp.exp2(old - new)
            peak[h] = new
            total[h] = jnp.concatenate([shrink, shrink], axis=1) * total[h] + jnp.dot(
                weights.astype(bf), both, preferred_element_type=f32)

    def visit(count, chip):
        def one(j, _):
            other_pair, other_ring = chip(j // 2)
            which = (other_pair * 4 + other_ring) * 2 + j % 2
            away = place - which

            @pl.when((away >= 1) & (away < WINDOW // n))
            def _():
                work(kv.at[which], None)
            return 0

        lax.fori_loop(0, count, one, 0)

    every.second(0)
    every.second(1)
    every.forward(0, 0)
    every.forward(0, 1)
    mine.wait()

    for copy in every.across[0:4]:
        copy.wait_recv()

    def rim(j, _):
        other_core = jnp.where(j % 2 == 0, core, 1 - core)
        which = (jnp.where(j < 2, pair, 1 - pair) * 4 + ring) * 2 + other_core
        away = place - which

        @pl.when((away >= 0) & (away <= WINDOW // n))
        def _():
            work(kv.at[which], (jnp.where(away == WINDOW // n, 0, -n), jnp.where(away == 0, 0, n)))
        return 0

    lax.fori_loop(0, 4, rim, 0)
    every.forward(1, 0)
    every.forward(1, 1)
    for copy in every.across[4:12]:
        copy.wait_recv()
    visit(8, lambda g: (jnp.where(g % 2 == 0, pair, 1 - pair), (ring + jnp.where(g < 2, 1, 3)) % 4))
    every.last()
    for copy in every.across[12:]:
        copy.wait_recv()
    visit(4, lambda g: (jnp.where(g == 0, pair, 1 - pair), (ring + 2) % 4))
    for copy in every.started:
        copy.wait_send()
    for h in range(heads):
        out_ref[:, h * HD:(h + 1) * HD] = total[h, :, 0:HD] / total[h, :, HD:2 * HD]


def run_attention(x, wq, wk, wv, cid):
    n = x.shape[0]
    width = wq.shape[1]
    heads = width // HD
    D = pltpu.SemaphoreType.DMA
    many = copies_of(2, True)
    bf, f32 = jnp.bfloat16, jnp.float32
    return pl.pallas_call(
        attention_kernel,
        out_shape=jax.ShapeDtypeStruct((n, width), f32),
        in_specs=[ANY] * 4, out_specs=VM,
        scratch_shapes=[pltpu.VMEM(x.shape, bf), pltpu.VMEM(wq.shape, bf), pltpu.VMEM(wk.shape, bf), pltpu.VMEM(wv.shape, bf), D((4,)),
                        pltpu.VMEM((n, 2 * HD), bf), pltpu.VMEM((16, n, 2 * HD), bf), pltpu.VMEM((heads, n, HD), bf),
                        pltpu.VMEM((heads, n, HD), f32), pltpu.VMEM((heads, n, 2 * HD), f32), D, D((many,)), D((many,))],
        compiler_params=pltpu.CompilerParams(collective_id=cid, has_side_effects=True, vmem_limit_bytes=63 << 20),
    )(x, wq, wk, wv)


def on_device(hidden_in, norm_gain, w_z, w_x, w_b, w_c, w_dt, conv_x, conv_b, conv_c, dt_bias, a_rate,
              skip_gain, group_gain, w_out, attn_gain, w_q, w_k, w_v):
    y_normed, w_out_half = run_mixer(
        hidden_in, w_x, w_b, w_c, w_dt.T, w_z, w_out, norm_gain[None, :], conv_x, conv_b, conv_c,
        dt_bias[None, :], a_rate[None, :], skip_gain[None, :], group_gain[None, :], 0)
    mixed, normed_two = run_mix(y_normed, w_out_half, w_out, hidden_in, attn_gain[None, :], 1)
    return (mixed, run_attention(normed_two, w_q, w_k, w_v, 2))


def solution(mesh):
    tile, cols = P("seq", "mp"), P(None, "mp")
    placed = (tile, P(), tile, tile, tile, tile, tile, cols, cols, cols, P("mp"), P("mp"), P("mp"), P("mp"),
              P("mp", "seq"), P(), cols, cols, cols)
    return jax.shard_map(on_device, mesh=mesh, in_specs=placed, out_specs=(tile, tile), check_vma=False)
```

```python
import jax
import jax.numpy as jnp
from jax import lax
from jax.experimental import pallas as pl
from jax.experimental.pallas import tpu as pltpu
from jax.sharding import PartitionSpec as P

MESH = pl.DeviceIdType.MESH
VM = pl.BlockSpec(memory_space=pltpu.VMEM)
FAR = pl.BlockSpec(memory_space=pltpu.HBM)
P_SIZE = 64
N = 128
HD = 128
WINDOW = 4096
QB = 128


def rows(start, size):
    return pl.ds(start, size)


class Gather:
    def __init__(self, view, own, names, pair, ring, core, sends, recvs, base, pieces, fan):
        self.view, self.own, self.names = view, own, names
        self.pair, self.ring, self.core = pair, ring, core
        self.sends, self.recvs, self.next, self.pieces, self.fan = sends, recvs, base, pieces, fan
        self.right, self.left, self.far = (ring + 1) % 4, (ring + 3) % 4, (ring + 2) % 4
        self.started, self.across = [], []
        self.y, self.a, self.b, self.f = {}, {}, {}, []

    def send(self, src, block, piece, pair, ring, core):
        copy = pltpu.make_async_remote_copy(
            src_ref=src, dst_ref=self.view(*block, piece), send_sem=self.sends.at[self.next], recv_sem=self.recvs.at[self.next],
            device_id=self.names(pair, ring, core), device_id_type=MESH)
        self.next += 1
        copy.start()
        self.started.append(copy)
        return copy

    def over(self, src, block, piece):
        if self.fan:
            self.across.append(self.send(src, block, piece, self.pair, self.ring, 1 - self.core))

    def begin_piece(self, k):
        me, piece = (self.pair, self.ring, self.core), self.pieces[k]
        src = self.own(piece)
        self.y[k] = self.send(src, me, piece, 1 - self.pair, self.ring, self.core)
        self.a[k] = [self.send(src, me, piece, self.pair, to, self.core) for to in (self.right, self.left)]
        self.over(src, me, piece)

    def begin(self):
        for k in range(len(self.pieces)):
            self.begin_piece(k)

    def second(self, k):
        piece, block = self.pieces[k], (1 - self.pair, self.ring, self.core)
        self.y[k].wait_recv()
        src = self.view(*block, piece)
        self.b[k] = [self.send(src, block, piece, self.pair, to, self.core) for to in (self.right, self.left)]
        self.over(src, block, piece)

    def forward(self, which, k):
        pair = self.pair if which == 0 else 1 - self.pair
        piece, first = self.pieces[k], k < len(self.pieces) // 2
        for d, (to, origin) in enumerate(((self.right, self.left), (self.left, self.right))):
            (self.a, self.b)[which][k][d].wait_recv()
            block = (pair, origin, self.core)
            src = self.view(*block, piece)
            if first == (d == 0):
                self.f.append((self.send(src, block, piece, self.pair, to, self.core), (pair, self.far, self.core), piece))
            self.over(src, block, piece)

    def last(self):
        for copy, block, piece in self.f:
            copy.wait_recv()
            self.over(self.view(*block, piece), block, piece)

    def finish(self):
        for copy in self.across:
            copy.wait_recv()
        for copy in self.started:
            copy.wait_send()


def copies_of(pieces, fan):
    return pieces * (7 + (8 if fan else 0))


def seq_names(pair, ring, core):
    return {"seq": (pair * 4 + ring) * 2 + core}


def mp_names(pair, ring, core):
    return {"mp": pair * 4 + ring}


def greet(ids):
    barrier = pltpu.get_barrier_semaphore()
    for other in ids:
        pl.semaphore_signal(barrier, inc=1, device_id=other, device_id_type=MESH)
    pl.semaphore_wait(barrier, len(ids))


def seq_place():
    me = lax.axis_index("seq")
    return me // 8, (me // 2) % 4, me % 2


def mp_place():
    me = lax.axis_index("mp")
    return me // 4, me % 4


def neighbours(names, pair, ring, core, fan):
    ids = [names(1 - pair, ring, core), names(pair, (ring + 1) % 4, core), names(pair, (ring + 3) % 4, core)]
    return ids + ([names(pair, ring, 1 - core)] if fan else [])


def cut(total, count):
    return [pl.ds(k * (total // count), total // count) for k in range(count)]


def write_normed(whole, gain_ref, normed_ref, start, count, size):
    blocks, _, wide = whole.shape

    def norm(c, _):
        piece = rows(pl.multiple_of(start + c * size, 16), size)
        square = jnp.zeros((size, wide), jnp.float32)
        for b in range(blocks):
            value = whole[b, piece, :].astype(jnp.float32)
            square = square + value * value
        scale = lax.rsqrt(jnp.sum(square, axis=1, keepdims=True) / (blocks * wide) + 1e-05)
        for b in range(blocks):
            lanes = slice(b * wide, (b + 1) * wide)
            normed_ref[piece, lanes] = (whole[b, piece, :].astype(jnp.float32) * scale * gain_ref[:, lanes]).astype(normed_ref.dtype)
        return 0

    lax.fori_loop(0, count // size, norm, 0)


class RingFirst(Gather):
    def begin(self):
        me = (self.pair, self.ring, self.core)
        self.pairs_open = []
        for k, piece in enumerate(self.pieces):
            src = self.own(piece)
            self.a[k] = [self.send(src, me, piece, self.pair, to, self.core) for to in (self.right, self.left)]
            self.pairs_open.append((self.send(src, me, piece, 1 - self.pair, self.ring, self.core), self.ring, piece))
            self.over(src, me, piece)

    def beside(self, src, block, piece):
        self.pairs_open.append((self.send(src, block, piece, 1 - self.pair, self.ring, self.core), block[1], piece))
        self.over(src, block, piece)

    def forward(self, k):
        piece, first = self.pieces[k], k < len(self.pieces) // 2
        for d, (to, origin) in enumerate(((self.right, self.left), (self.left, self.right))):
            self.a[k][d].wait_recv()
            block = (self.pair, origin, self.core)
            src = self.view(*block, piece)
            if first == (d == 0):
                self.f.append((self.send(src, block, piece, self.pair, to, self.core), (self.pair, self.far, self.core), piece))
            self.beside(src, block, piece)

    def last(self):
        for copy, block, piece in self.f:
            copy.wait_recv()
            self.beside(self.view(*block, piece), block, piece)

    def pairs(self):
        for copy, ring, piece in self.pairs_open:
            copy.wait_recv()
            block = (1 - self.pair, ring, self.core)
            self.over(self.view(*block, piece), block, piece)


def three_terms(decay):
    bf, f32 = jnp.bfloat16, jnp.float32
    big = decay.astype(bf).astype(f32)
    middle = (decay - big).astype(bf).astype(f32)
    small = (decay - big - middle).astype(bf).astype(f32)
    which = lax.broadcasted_iota(jnp.int32, decay.shape, 0)
    return jnp.where(which == 0, big, jnp.where(which == 1, middle, small)).astype(bf)


def decay_of(block):
    tail = block.astype(jnp.float32)
    return tail[0:1] + (tail[1:2] + tail[2:3])


def mixer_kernel(x_ref, wx_ref, wb_ref, wc_ref, wdt_ref, wz_ref, wo_ref, norm_ref, cx_ref, cb_ref, cc_ref, bias_ref, rate_ref,
                 skip_ref, gain_ref,
                 out_ref, woa, wbc, vectors, wda, whole, normed, wxa, wba, wza, padx, padbc, bcd, y, gate, state, cc, cumul, tail, mine, theirs,
                 agg, aggs, turn, half_in, half_out, incoming, local, ts, tr, hs, hr, es, er, ds, dr, bs, br, xs, xr, zs, zr, os, orr, gs, gr):
    bf, f32 = jnp.bfloat16, jnp.float32
    mpair, mring = mp_place()
    pair, ring, core = seq_place()
    place = lax.axis_index("seq")
    following, previous = (place + 1) % 16, (place + 15) % 16
    joined = [pltpu.make_async_copy(wb_ref, wbc.at[:, pl.ds(0, N)], local.at[6]),
              pltpu.make_async_copy(wc_ref, wbc.at[:, pl.ds(N, N)], local.at[7])]
    for copy in joined:
        copy.start()
    greet(neighbours(mp_names, mpair, mring, 0, False) + neighbours(seq_names, pair, ring, core, True)
          + [{"seq": following}, {"seq": previous}])
    n = x_ref.shape[0]
    depth, tall = wx_ref.shape[0], wo_ref.shape[0]
    count = n // QB
    width = wx_ref.shape[1]

    def wide_view(ref):
        return lambda pair, ring, core, piece: ref.at[pl.ds(((pair * 4 + ring) * 2 + core) * depth + piece.start, piece.size), :]

    def seq_gather(kind, view, own, sends, recvs, base, pieces, fan=True):
        return kind(view, lambda piece: own.at[piece], seq_names, pair, ring, core, sends, recvs, base, pieces, fan)

    def mp_view(pair, ring, core, piece):
        return whole.at[pair * 4 + ring, piece]

    hidden = Gather(mp_view, lambda piece: x_ref.at[piece], mp_names, mpair, mring, 0, hs, hr, 0, cut(n, 2), False)
    edge = Gather(mp_view, lambda piece: tail, mp_names, mpair, mring, 0, es, er, 0, [pl.ds(n, 16)], False)
    small = seq_gather(Gather, wide_view(wba), wbc, bs, br, 0, cut(depth, 2))

    def step_view(pair, ring, core, piece):
        return wda.at[:, pl.ds(((pair * 4 + ring) * 2 + core) * depth, depth)]

    steps = Gather(step_view, lambda piece: wdt_ref, seq_names, pair, ring, core, ds, dr, 0, [None], True)
    big = seq_gather(Gather, wide_view(wxa), wx_ref, xs, xr, 0, cut(depth, 2))
    fan2 = copies_of(2, True)
    quarters, parts = cut(depth, 4), cut(tall, 4)
    z_pair = seq_gather(Gather, wide_view(wza), wz_ref, zs, zr, 0, quarters[0:2])
    z_ring = seq_gather(RingFirst, wide_view(wza), wz_ref, zs, zr, fan2, quarters[2:4])

    def out_view(pair, ring, core, piece):
        return woa.at[(pair * 4 + ring) * 2 + core, piece]

    lead = wo_ref.at[:, pl.ds(0, wo_ref.shape[1] // 2)]
    o_pair = seq_gather(Gather, out_view, lead, os, orr, 0, parts[0:2])
    o_ring = seq_gather(RingFirst, out_view, lead, os, orr, fan2, parts[2:4])
    own_rows = pl.ds(place * depth, depth)
    at_home = [pltpu.make_async_copy(x_ref, whole.at[mpair * 4 + mring, pl.ds(0, n)], local.at[0]),
               pltpu.make_async_copy(wx_ref, wxa.at[own_rows, :], local.at[1]),
               pltpu.make_async_copy(wbc, wba.at[own_rows, :], local.at[2]),
               pltpu.make_async_copy(wdt_ref, wda.at[:, own_rows], local.at[8]),
               pltpu.make_async_copy(wz_ref, wza.at[own_rows, :], local.at[3]),
               pltpu.make_async_copy(lead, woa.at[place], local.at[4])]

    def to_device(src, dst, index, device):
        copy = pltpu.make_async_remote_copy(src_ref=src, dst_ref=dst, send_sem=ts.at[index], recv_sem=tr.at[index],
                                            device_id=device, device_id_type=MESH)
        copy.start()
        return copy

    shifted = to_device(x_ref.at[pl.ds(n - 16, 16)], tail, 0, {"seq": following})
    for copy in joined:
        copy.wait()
    steps.begin()
    small.begin()
    for k in range(2):
        big.begin_piece(k)
        hidden.begin_piece(k)
    for copy in at_home:
        copy.start()
    shifted.wait_recv()
    edge.begin()
    home_tail = pltpu.make_async_copy(tail, whole.at[mpair * 4 + mring, pl.ds(n, 16)], local.at[5])
    home_tail.start()
    steps.second(0)
    small.second(0)
    small.second(1)
    for k in range(2):
        big.second(k)
        small.forward(0, k)
        hidden.forward(0, k)
        big.forward(0, k)
        hidden.second(k)
    steps.forward(0, 0)
    steps.forward(1, 0)
    edge.second(0)
    edge.forward(0, 0)
    small.forward(1, 0)
    small.forward(1, 1)
    for k in range(2):
        hidden.forward(1, k)
        big.forward(1, k)
    edge.forward(1, 0)
    z_ring.begin()
    z_pair.begin()
    hidden.last()
    edge.last()
    at_home[0].wait()
    home_tail.wait()
    write_normed(whole, norm_ref, normed, 0, n, 32)
    write_normed(whole, norm_ref, normed, n, 16, 16)
    vectors[...] = jnp.zeros_like(vectors)
    vectors[0:1, 0:bias_ref.shape[1]] = bias_ref[...]
    vectors[1:2, 0:rate_ref.shape[1]] = rate_ref[...]
    bcd[...] = jnp.zeros_like(bcd)
    small.last()
    steps.last()
    small.finish()
    steps.finish()
    at_home[2].wait()
    at_home[3].wait()
    inside = jnp.where(place > 0, 1.0, 0.0)
    product = jnp.dot(normed[...], wba[...], preferred_element_type=f32)
    bcd[:, 0:bias_ref.shape[1]] = lax.dot_general(
        normed[0:n, :], wda[...], (((1,), (1,)), ((), ())), preferred_element_type=f32)
    padbc[pl.ds(8, n), :] = product[0:n]
    padbc[pl.ds(0, 8), :] = product[n + 8:n + 16] * inside
    z_pair.second(0)
    z_pair.second(1)
    big.last()
    big.finish()
    at_home[1].wait()
    for part in range(4):
        lanes = slice(part * 256, (part + 1) * 256)
        product = jnp.dot(normed[...], wxa[:, lanes], preferred_element_type=f32)
        padx[pl.ds(8, n), lanes] = product[0:n]
        padx[pl.ds(0, 8), lanes] = product[n + 8:n + 16] * inside
    z_ring.forward(0)
    z_ring.forward(1)

    state[...] = jnp.zeros_like(state)
    row = lax.broadcasted_iota(jnp.int32, (QB, QB), 0)
    col = lax.broadcasted_iota(jnp.int32, (QB, QB), 1)
    causal = row >= col
    tri = jnp.where(causal, 1.0, 0.0).astype(f32)
    low = col < P_SIZE

    def conv(pad, taps, start, lanes, tap_lanes):
        whole_rows = pad[pl.ds(start, QB + 8), lanes]
        total = taps[0:1, tap_lanes] * whole_rows[5:5 + QB]
        for j in range(1, 4):
            total = total + taps[j:j + 1, tap_lanes] * whole_rows[5 + j:5 + j + QB]
        return total / (1.0 + jnp.exp(-total))

    def one(c, before):
        start = pl.multiple_of(c * QB, QB)
        here = pl.ds(start, QB)
        bv = conv(padbc, cb_ref, start, slice(0, N), slice(0, N))
        cv = conv(padbc, cc_ref, start, slice(N, 2 * N), slice(0, N)).astype(bf)
        cc[here, :] = cv
        raw = bcd[here, :] + vectors[0:1, :]
        step = jnp.maximum(raw, 0.0) + jnp.log1p(jnp.exp(-jnp.abs(raw)))
        decay = -vectors[1:2, :] * step
        cum = jnp.dot(tri, decay, precision=lax.Precision.HIGHEST, preferred_element_type=f32)
        cumul[here, :] = cum + before
        cum_t, step_t = cum.T, step.T
        last = cum[QB - 1:QB, :]
        bt = bv.T.astype(bf)
        affinity = jnp.dot(cv, bt, preferred_element_type=f32)
        for p in range(width // 128):
            lanes = slice(p * 128, (p + 1) * 128)
            xv = conv(padx, cx_ref, start, lanes, lanes)
            mixes, grown, tails, ends = [], [], [], []
            for h in (2 * p, 2 * p + 1):
                ct = jnp.broadcast_to(cum[:, h:h + 1], (QB, QB))
                st = jnp.broadcast_to(step[:, h:h + 1], (QB, QB))
                end = jnp.broadcast_to(last[:, h:h + 1], (1, QB))
                spread = jnp.where(causal, ct - cum_t[h:h + 1, :], -jnp.inf)
                mixes.append((affinity * jnp.exp(spread) * step_t[h:h + 1, :]).astype(bf))
                grown.append(ct)
                tails.append(jnp.exp(end - ct) * st)
                ends.append(end)
            mixed = jnp.concatenate(mixes, axis=1)
            xs2 = jnp.concatenate([jnp.where(low, xv, 0.0).astype(bf), jnp.where(low, 0.0, xv).astype(bf)], axis=0)
            out = jnp.dot(mixed, xs2, preferred_element_type=f32)
            old = state[:, lanes]
            carried = jnp.dot(cv, old.astype(bf), preferred_element_type=f32)
            out = out + jnp.exp(jnp.where(low, grown[0], grown[1])) * carried
            skips = [jnp.broadcast_to(skip_ref[:, h:h + 1], (1, QB)) for h in (2 * p, 2 * p + 1)]
            y[here, lanes] = out + jnp.where(low[0:1], skips[0], skips[1]) * xv
            weighted = (xv * jnp.where(low, tails[0], tails[1])).astype(bf)
            fresh = jnp.dot(bt, weighted, preferred_element_type=f32)
            state[:, lanes] = jnp.exp(jnp.where(low[0:1], ends[0], ends[1])) * old + fresh
        return before + last

    total = lax.fori_loop(0, count, one, jnp.zeros((1, 128), f32))
    mine[0:N, :] = state[...].astype(bf)
    for p in range(width // 128):
        lanes = slice(p * 128, (p + 1) * 128)
        ends = [jnp.broadcast_to(total[:, h:h + 1], (16, 128)) for h in (2 * p, 2 * p + 1)]
        mine[N:N + 16, lanes] = three_terms(jnp.exp(jnp.where(low[0:16], ends[0], ends[1])))
    swapped = to_device(mine, theirs, 1, {"seq": place + 1 - 2 * core})
    for which in range(2):
        for k in range(2):
            z_pair.forward(which, k)
    swapped.wait_recv()
    half = width // 2
    ours = pl.ds(pl.multiple_of(core * half, half), half)
    rest = pl.ds(pl.multiple_of((1 - core) * half, half), half)
    a, b = mine[:, ours].astype(f32), theirs[:, ours].astype(f32)
    head = core == 0
    early, late = jnp.where(head, a, b), jnp.where(head, b, a)
    early_decay, late_decay = decay_of(early[N:N + 16]), decay_of(late[N:N + 16])
    agg[0:N, :] = (late_decay * early[0:N] + late[0:N]).astype(bf)
    agg[N:N + 16, :] = three_terms(jnp.broadcast_to(early_decay * late_decay, (16, half)))
    chip = pair * 4 + ring
    chips = Gather(lambda pair, ring, core, piece: aggs.at[pair * 4 + ring, piece], lambda piece: agg.at[piece], seq_names,
                   pair, ring, core, gs, gr, 0, [pl.ds(0, 80), pl.ds(80, N + 16 - 80)], False)
    chips.begin()
    o_ring.begin()
    o_pair.begin()
    z_ring.last()
    chips.second(0)
    chips.second(1)
    z_pair.last()
    o_pair.second(0)
    o_pair.second(1)
    for which in range(2):
        for k in range(2):
            chips.forward(which, k)
    z_ring.pairs()
    o_ring.forward(0)
    o_ring.forward(1)
    z_pair.finish()
    z_ring.finish()
    at_home[4].wait()

    def open_gate(part):
        lanes = slice(part * 256, (part + 1) * 256)
        gate[:, lanes] = jnp.dot(normed[0:n, :], wza[:, lanes], preferred_element_type=f32)

    open_gate(0)
    o_pair.forward(0, 0)
    o_pair.forward(0, 1)
    open_gate(1)
    chips.last()
    half_out[...] = jnp.zeros_like(half_out)

    def add(k, _):
        half_out[...] = decay_of(aggs[k, N:N + 16, :]) * half_out[...] + aggs[k, 0:N, :].astype(f32)
        return 0

    lax.fori_loop(0, chip, add, 0)
    turn[...] = half_out[...].astype(bf)
    given = to_device(turn, half_in, 2, {"seq": place + 1 - 2 * core})
    o_pair.forward(1, 0)
    o_pair.forward(1, 1)
    open_gate(2)
    o_ring.last()
    open_gate(3)
    given.wait_recv()
    incoming[:, ours] = half_out[...]
    incoming[:, rest] = half_in[...].astype(f32)
    keep = jnp.where(head, 0.0, 1.0)
    before = theirs[N:N + 16, :].astype(f32)
    before_decay = jnp.where(head, 1.0, before[0:1] + (before[1:2] + before[2:3]))
    incoming[...] = before_decay * incoming[...] + keep * theirs[0:N, :].astype(f32)
    low_rows = low

    def close(c, _):
        here = pl.ds(pl.multiple_of(c * QB, QB), QB)
        cv = cc[here, :]
        cum = cumul[here, :]
        square = jnp.zeros((QB, 128), f32)
        for p in range(width // 128):
            lanes = slice(p * 128, (p + 1) * 128)
            ct = jnp.where(low_rows, jnp.broadcast_to(cum[:, 2 * p:2 * p + 1], (QB, 128)),
                           jnp.broadcast_to(cum[:, 2 * p + 1:2 * p + 2], (QB, 128)))
            carried = jnp.dot(cv, incoming[:, lanes].astype(bf), preferred_element_type=f32)
            g = gate[here, lanes]
            value = (y[here, lanes] + jnp.exp(ct) * carried) * (g / (1.0 + jnp.exp(-g)))
            gate[here, lanes] = value
            square = square + value * value
        scale = lax.rsqrt(jnp.sum(square, axis=1, keepdims=True) / width + 1e-05)
        out_ref[here, :] = (gate[here, :] * scale * gain_ref[...]).astype(bf)
        return 0

    lax.fori_loop(0, count, close, 0)
    o_pair.last()
    o_ring.pairs()
    for g in (o_pair, o_ring, hidden, edge, chips):
        g.finish()
    at_home[5].wait()
    for copy in (shifted, swapped, given):
        copy.wait_send()


def run_mixer(x, wx, wb, wc, wdt, wz, wo, norm_gain, conv_x, conv_b, conv_c, bias, rate, skip, gain, cid):
    n, w = x.shape
    depth, width = wx.shape
    tall, cols = wo.shape
    D, V = pltpu.SemaphoreType.DMA, pltpu.VMEM
    bf, f32 = jnp.bfloat16, jnp.float32
    fan2, plain2 = copies_of(2, True), copies_of(2, False)
    pairs = []
    for size in (3, plain2, copies_of(1, False), copies_of(1, True), fan2, fan2, 2 * fan2, 2 * fan2, plain2):
        pairs += [D((size,)), D((size,))]
    return pl.pallas_call(
        mixer_kernel,
        out_shape=(jax.ShapeDtypeStruct((n, width), bf), jax.ShapeDtypeStruct((16, tall, cols // 2), bf)),
        in_specs=[VM] * 15, out_specs=(VM, VM),
        scratch_shapes=[V((depth, 2 * N), bf), V((8, 128), f32), V((16, 16 * depth), bf),
                        V((8, n + 16, w), bf), V((n + 16, 8 * w), bf), V((16 * depth, width), bf), V((16 * depth, 2 * N), bf),
                        V((16 * depth, width), bf), V((n + 8, width), f32), V((n + 8, 2 * N), f32), V((n, N), f32),
                        V((n, width), f32), V((n, width), f32), V((N, width), f32), V((n, N), bf), V((n, 128), f32),
                        V((16, w), bf), V((N + 16, width), bf), V((N + 16, width), bf), V((N + 16, width // 2), bf),
                        V((8, N + 16, width // 2), bf), V((N, width // 2), bf), V((N, width // 2), bf), V((N, width // 2), f32), V((N, width), f32),
                        D((9,))] + pairs,
        compiler_params=pltpu.CompilerParams(collective_id=cid, has_side_effects=True, vmem_limit_bytes=63 << 20),
    )(x, wx, wb, wc, wdt, wz, wo, norm_gain, conv_x, conv_b, conv_c, bias, rate, skip, gain)


def mix_kernel(y_hbm, w_hbm, wo_ref, hidden_hbm, gain_hbm, mixed_ref, normed_ref, y_ref, gain_ref, hidden_ref, w, p, tmp, d1, d2, ysrc, ydst, yb, joint, tmpb, d1b, d2b, whole,
               wsem, s1, r1, s2, r2, sraw, rraw, sy, ry, syb, ryb, s1b, r1b, s2b, r2b, srb, rrb, gs, gr, ls, lr, local):
    high, low = mp_place()
    right, left, far = (low + 1) % 4, (low + 3) % 4, (low + 2) % 4
    me = high * 4 + low
    order = (1 - high, high)
    sides = ((right, left), (left, right))
    n = y_ref.shape[0]
    cols = w_hbm.shape[2]
    place = lax.axis_index("seq")
    spair, sring, score = seq_place()
    na, nb = ydst.shape[1], yb.shape[2]
    ha, hb = na // 2, nb // 2
    f32 = jnp.float32
    rings = (far, right, left, low)
    blocks = [pair * 4 + ring for ring in rings for pair in order]
    loads = [pltpu.make_async_copy(w_hbm.at[pl.ds(2 * b, 2)], w.at[0, pl.ds(2 * b, 2)], wsem.at[i]) for i, b in enumerate(blocks)]
    arriving = pltpu.make_async_copy(y_hbm, y_ref, local.at[2])
    arriving.start()
    for load in loads:
        load.start()
    greet(neighbours(mp_names, high, low, 0, False) + neighbours(seq_names, spair, sring, score, True))
    trail = wo_ref.at[:, pl.ds(cols, cols)]
    later = Gather(lambda pair, ring, core, piece: w.at[1, (pair * 4 + ring) * 2 + core, piece], lambda piece: trail.at[piece],
                   seq_names, spair, sring, score, ls, lr, 0, cut(wo_ref.shape[0], 2), True)
    later.begin()
    home = pltpu.make_async_copy(trail, w.at[1, place], local.at[0])
    home.start()
    fetched = [pltpu.make_async_copy(hidden_hbm, hidden_ref, local.at[1]), pltpu.make_async_copy(gain_hbm, gain_ref, local.at[3])]
    for copy in fetched:
        copy.start()
    arriving.wait()

    def send(src, dst, pair, ring, ssem, rsem):
        copy = pltpu.make_async_remote_copy(src_ref=src, dst_ref=dst, send_sem=ssem, recv_sem=rsem,
                                            device_id=mp_names(pair, ring, 0), device_id_type=MESH)
        copy.start()
        sent.append(copy)
        return copy

    def product(h, b):
        both = jnp.concatenate([w[h, 2 * b], w[h, 2 * b + 1]], axis=1)
        p[h, b] = jnp.dot(y_ref[...], both, preferred_element_type=f32).astype(p.dtype)

    def start_first(h, k):
        first[h][k] = [send(p.at[h, order[k] * 4 + far, rows(d * ha, ha)], d1.at[h, k, d], high, sides[d][0],
                            s1.at[h, k, d], r1.at[h, k, d]) for d in range(2)]

    def start_raw(h, k, d):
        raw[h][k][d] = send(p.at[h, order[k] * 4 + sides[d][0], rows((1 - d) * ha, ha)],
                            d2.at[h, k, d, rows((1 - d) * ha, ha)], high, sides[d][0], sraw.at[h, k, d], rraw.at[h, k, d])

    def pass_on(h, k):
        result = []
        for d in range(2):
            first[h][k][d].wait_recv()
            here = slice(d * ha, (d + 1) * ha)
            tmp[h, k, d] = (d1[h, k, d].astype(f32) + p[h, order[k] * 4 + sides[d][0], here, :].astype(f32)).astype(tmp.dtype)
            result.append(send(tmp.at[h, k, d], d2.at[h, k, d, rows(d * ha, ha)], high, sides[d][0],
                               s2.at[h, k, d], r2.at[h, k, d]))
        second[h][k] = result

    def total(h, k):
        for d in range(2):
            raw[h][k][d].wait_recv()
            second[h][k][d].wait_recv()
        return p[h, order[k] * 4 + low, 0:na, :].astype(f32) + d2[h, k, 0].astype(f32) + d2[h, k, 1].astype(f32)

    def give(h):
        ysrc[h] = total(h, 0).astype(ysrc.dtype)
        across[h] = send(ysrc.at[h], ydst.at[h], 1 - high, low, sy.at[h], ry.at[h])

    def start_pair(h, i):
        open_pair[h][i] = send(p.at[h, (1 - high) * 4 + rings[i], rows(na, nb)], yb.at[h, i], 1 - high, low,
                               syb.at[h, i], ryb.at[h, i])

    def join(h, i):
        open_pair[h][i].wait_recv()
        value = p[h, high * 4 + rings[i], na:n, :].astype(f32) + yb[h, i].astype(f32)
        if i < 3:
            joint[h, i] = value.astype(joint.dtype)
        return value

    def start_ring(h):
        join(h, 0)
        first_b[h] = [send(joint.at[h, 0, rows(d * hb, hb)], d1b.at[h, d], high, sides[d][0], s1b.at[h, d], r1b.at[h, d])
                      for d in range(2)]
        for d in range(2):
            join(h, 1 + d)
            raw_b[h][d] = send(joint.at[h, 1 + d, rows((1 - d) * hb, hb)], d2b.at[h, d, rows((1 - d) * hb, hb)], high, sides[d][0],
                               srb.at[h, d], rrb.at[h, d])

    def pass_ring(h):
        for d in range(2):
            first_b[h][d].wait_recv()
            tmpb[h, d] = (d1b[h, d].astype(f32) + joint[h, 1 + d, d * hb:(d + 1) * hb, :].astype(f32)).astype(tmpb.dtype)
            second_b[h][d] = send(tmpb.at[h, d], d2b.at[h, d, rows(d * hb, hb)], high, sides[d][0], s2b.at[h, d], r2b.at[h, d])

    def keep(h, start, result):
        here = slice(start, start + result.shape[0])
        for c in range(2):
            lanes = slice((2 * c + h) * cols, (2 * c + h + 1) * cols)
            value = hidden_ref[here, lanes].astype(f32) + result[:, c * cols:(c + 1) * cols]
            mixed_ref[here, lanes] = value
            whole[h, me, here, c * cols:(c + 1) * cols] = value.astype(whole.dtype)

    def close(h):
        own = total(h, 1)
        across[h].wait_recv()
        keep(h, 0, own + ydst[h].astype(f32))
        pair_first[h].begin()

    def close_ring(h):
        own = join(h, 3)
        for d in range(2):
            raw_b[h][d].wait_recv()
            second_b[h][d].wait_recv()
            own = own + d2b[h, d].astype(f32)
        keep(h, na, own)
        ring_first[h].begin()

    sent = []
    first, second = [[None, None] for _ in range(2)], [[None, None] for _ in range(2)]
    raw = [[[None, None], [None, None]] for _ in range(2)]
    across = [None, None]
    open_pair = [[None] * 4 for _ in range(2)]
    first_b, raw_b, second_b = [None, None], [[None, None] for _ in range(2)], [[None, None] for _ in range(2)]

    def gather(kind, index, h, start, size):
        return kind(lambda pair, ring, core, piece: whole.at[h, pair * 4 + ring, piece], lambda piece: whole.at[h, me, piece],
                    mp_names, high, low, 0, gs, gr, index * copies_of(2, False),
                    [pl.ds(start, size), pl.ds(start + size, size)], False)

    pair_first = [gather(Gather, h, h, 0, ha) for h in range(2)]
    ring_first = [gather(RingFirst, 2 + h, h, na, hb) for h in range(2)]
    def issue(h):
        for i, b in enumerate(blocks):
            if h == 0:
                loads[i].wait()
            product(h, b)
            if i % 2 == 0:
                start_pair(h, i // 2)
            if i < 2:
                start_first(h, i)
            elif i < 6:
                start_raw(h, i % 2, i // 2 - 1)

    issue(0)
    pass_on(0, 0)
    later.second(0)
    later.second(1)
    later.forward(0, 0)
    later.forward(0, 1)
    start_ring(0)
    pass_on(0, 1)
    pass_ring(0)
    give(0)
    later.forward(1, 0)
    later.forward(1, 1)
    for copy in fetched:
        copy.wait()
    close_ring(0)
    close(0)
    later.last()
    ring_first[0].forward(0)
    ring_first[0].forward(1)
    for copy in later.across:
        copy.wait_recv()
    home.wait()
    issue(1)
    for k in range(2):
        pair_first[0].second(k)
    pass_on(1, 0)
    start_ring(1)
    pass_on(1, 1)
    pass_ring(1)
    for k in range(2):
        pair_first[0].forward(0, k)
    ring_first[0].last()
    give(1)
    close_ring(1)
    for k in range(2):
        pair_first[0].forward(1, k)
    close(1)
    ring_first[1].forward(0)
    ring_first[1].forward(1)
    for k in range(2):
        pair_first[1].second(k)
    for k in range(2):
        pair_first[1].forward(0, k)
    ring_first[1].last()
    pair_first[0].last()
    ring_first[0].pairs()
    for k in range(2):
        pair_first[1].forward(1, k)
    pair_first[1].last()
    ring_first[1].pairs()
    wide = whole.shape[3]

    def norm(c, _):
        piece = rows(pl.multiple_of(c * 32, 32), 32)
        square = jnp.zeros((32, wide), f32)
        for b in range(8):
            for h in range(2):
                value = whole[h, b, piece, :].astype(f32)
                square = square + value * value
        scale = lax.rsqrt(jnp.sum(square, axis=1, keepdims=True) / (16 * wide) + 1e-05)
        for b in range(8):
            for h in range(2):
                for q in range(2):
                    start = b * 2 * wide + (2 * q + h) * cols
                    normed_ref[piece, start:start + cols] = (
                        whole[h, b, piece, q * cols:(q + 1) * cols].astype(f32) * scale
                        * gain_ref[:, start:start + cols]).astype(normed_ref.dtype)
        return 0

    lax.fori_loop(0, n // 32, norm, 0)
    for g in pair_first + ring_first:
        g.finish()
    for copy in sent + later.started:
        copy.wait_send()


def run_mix(y, w, wo, hidden, gain, cid):
    n, width = hidden.shape
    D = pltpu.SemaphoreType.DMA
    bf = jnp.bfloat16
    V = pltpu.VMEM
    na = n // 8 * 5
    nb = n - na
    lanes = width // 2
    few = 4 * copies_of(2, False)
    fan2 = copies_of(2, True)
    return pl.pallas_call(
        mix_kernel,
        out_shape=(jax.ShapeDtypeStruct((n, width), jnp.float32), jax.ShapeDtypeStruct((n, 8 * width), bf)),
        in_specs=[FAR] * 5, out_specs=(VM, VM),
        scratch_shapes=[V(y.shape, bf), V(gain.shape, jnp.float32), V((n, width), bf), V((2,) + w.shape, bf), V((2, 8, n, lanes), bf), V((2, 2, 2, na // 2, lanes), bf),
                        V((2, 2, 2, na // 2, lanes), bf), V((2, 2, 2, na, lanes), bf), V((2, na, lanes), bf), V((2, na, lanes), bf),
                        V((2, 4, nb, lanes), bf), V((2, 3, nb, lanes), bf), V((2, 2, nb // 2, lanes), bf),
                        V((2, 2, nb // 2, lanes), bf), V((2, 2, nb, lanes), bf), V((2, 8, n, lanes), bf), D((8,))]
        + [D((2, 2, 2))] * 6 + [D((2,))] * 2 + [D((2, 4))] * 2 + [D((2, 2))] * 6 + [D((few,))] * 2 + [D((fan2,))] * 2 + [D((4,))],
        compiler_params=pltpu.CompilerParams(collective_id=cid, has_side_effects=True, vmem_limit_bytes=44 << 20),
    )(y, w, wo, hidden, gain)


def attention_kernel(x_hbm, wq_ref, wk_ref, wv_ref, out_ref, x_ref, xsem, own, kv, q, peak, total, local, ss, sr):
    place = lax.axis_index("seq")
    pair, ring, core = seq_place()
    load = pltpu.make_async_copy(x_hbm, x_ref, xsem)
    load.start()
    greet(neighbours(seq_names, pair, ring, core, True))
    n = x_ref.shape[0]
    heads = q.shape[0]
    bf, f32 = jnp.bfloat16, jnp.float32
    scale = HD ** -0.5 * 1.4426950408889634
    load.wait()
    own[:, 0:HD] = jnp.dot(x_ref[...], wk_ref[...], preferred_element_type=f32).astype(bf)
    own[:, HD:2 * HD] = jnp.dot(x_ref[...], wv_ref[...], preferred_element_type=f32).astype(bf)
    every = Gather(lambda pair, ring, core, piece: kv.at[(pair * 4 + ring) * 2 + core, piece], lambda piece: own.at[piece],
                   seq_names, pair, ring, core, ss, sr, 0, cut(n, 2), True)
    every.begin()
    mine = pltpu.make_async_copy(own, kv.at[place], local)
    mine.start()
    for h in range(0, heads, 2):
        both = jnp.dot(x_ref[...], wq_ref[:, h * HD:(h + 2) * HD], preferred_element_type=f32) * scale
        q[h] = both[:, 0:HD].astype(bf)
        q[h + 1] = both[:, HD:2 * HD].astype(bf)
    peak[...] = jnp.full_like(peak, -1e30)
    total[...] = jnp.zeros_like(total)

    def work(block, bounds):
        keys = block[:, 0:HD]
        both = jnp.concatenate([block[:, HD:2 * HD], jnp.ones((n, HD), bf)], axis=1)
        if bounds is not None:
            away = lax.broadcasted_iota(jnp.int32, (n, n), 1) - lax.broadcasted_iota(jnp.int32, (n, n), 0)
            allowed = (away > bounds[0]) & (away <= bounds[1])
        for h in range(heads):
            scores = lax.dot_general(q[h], keys, (((1,), (1,)), ((), ())), preferred_element_type=f32)
            if bounds is not None:
                scores = jnp.where(allowed, scores, -1e30)
            old = peak[h]
            new = jnp.maximum(old, jnp.max(scores, axis=1, keepdims=True))
            weights = jnp.exp2(scores - new[:, 0:1])
            if bounds is not None:
                weights = jnp.where(allowed, weights, 0.0)
            shrink = jnp.exp2(old - new)
            peak[h] = new
            total[h] = jnp.concatenate([shrink, shrink], axis=1) * total[h] + jnp.dot(
                weights.astype(bf), both, preferred_element_type=f32)

    def visit(count, chip):
        def one(j, _):
            other_pair, other_ring = chip(j // 2)
            which = (other_pair * 4 + other_ring) * 2 + j % 2
            away = place - which

            @pl.when((away >= 1) & (away < WINDOW // n))
            def _():
                work(kv.at[which], None)
            return 0

        lax.fori_loop(0, count, one, 0)

    every.second(0)
    every.second(1)
    every.forward(0, 0)
    every.forward(0, 1)
    mine.wait()

    for copy in every.across[0:4]:
        copy.wait_recv()

    def rim(j, _):
        other_core = jnp.where(j % 2 == 0, core, 1 - core)
        which = (jnp.where(j < 2, pair, 1 - pair) * 4 + ring) * 2 + other_core
        away = place - which

        @pl.when((away >= 0) & (away <= WINDOW // n))
        def _():
            work(kv.at[which], (jnp.where(away == WINDOW // n, 0, -n), jnp.where(away == 0, 0, n)))
        return 0

    lax.fori_loop(0, 4, rim, 0)
    every.forward(1, 0)
    every.forward(1, 1)
    for copy in every.across[4:12]:
        copy.wait_recv()
    visit(8, lambda g: (jnp.where(g % 2 == 0, pair, 1 - pair), (ring + jnp.where(g < 2, 1, 3)) % 4))
    every.last()
    for copy in every.across[12:]:
        copy.wait_recv()
    visit(4, lambda g: (jnp.where(g == 0, pair, 1 - pair), (ring + 2) % 4))
    for copy in every.started:
        copy.wait_send()
    for h in range(heads):
        out_ref[:, h * HD:(h + 1) * HD] = total[h, :, 0:HD] / total[h, :, HD:2 * HD]


def run_attention(x, wq, wk, wv, cid):
    n = x.shape[0]
    width = wq.shape[1]
    heads = width // HD
    D = pltpu.SemaphoreType.DMA
    many = copies_of(2, True)
    bf, f32 = jnp.bfloat16, jnp.float32
    return pl.pallas_call(
        attention_kernel,
        out_shape=jax.ShapeDtypeStruct((n, width), f32),
        in_specs=[FAR, VM, VM, VM], out_specs=VM,
        scratch_shapes=[pltpu.VMEM(x.shape, bf), D,
                        pltpu.VMEM((n, 2 * HD), bf), pltpu.VMEM((16, n, 2 * HD), bf), pltpu.VMEM((heads, n, HD), bf),
                        pltpu.VMEM((heads, n, HD), f32), pltpu.VMEM((heads, n, 2 * HD), f32), D, D((many,)), D((many,))],
        compiler_params=pltpu.CompilerParams(collective_id=cid, has_side_effects=True, vmem_limit_bytes=40 << 20),
    )(x, wq, wk, wv)


def on_device(hidden_in, norm_gain, w_z, w_x, w_b, w_c, w_dt, conv_x, conv_b, conv_c, dt_bias, a_rate,
              skip_gain, group_gain, w_out, attn_gain, w_q, w_k, w_v):
    y_normed, w_out_half = run_mixer(
        hidden_in, w_x, w_b, w_c, w_dt.T, w_z, w_out, norm_gain[None, :], conv_x, conv_b, conv_c,
        dt_bias[None, :], a_rate[None, :], skip_gain[None, :], group_gain[None, :], 0)
    mixed, normed_two = run_mix(y_normed, w_out_half, w_out, hidden_in, attn_gain[None, :], 1)
    return (mixed, run_attention(normed_two, w_q, w_k, w_v, 2))


def solution(mesh):
    tile, cols = P("seq", "mp"), P(None, "mp")
    placed = (tile, P(), tile, tile, tile, tile, tile, cols, cols, cols, P("mp"), P("mp"), P("mp"), P("mp"),
              P("mp", "seq"), P(), cols, cols, cols)
    return jax.shard_map(on_device, mesh=mesh, in_specs=placed, out_specs=(tile, tile), check_vma=False)
```
